32 devices in a mesh: tiles: 16 (over z, x, core), strip: 2 (over y).
Axes of the slice: x: 2, y: 2, z: 4, core: 2. Of those that a mesh axis runs over, the one named last changes fastest.
Arguments:
- fields: float32 [16, 2, 3, 3, 4, 8100], P('tiles', 'strip'), may hold values from -6 to 6
- wet_land: int32 [16, 2, 3, 8100], P('tiles', 'strip'), may hold values from 0 to 1, as said below
- links: int32 [16, 2, 3, 4, 4], P('tiles', 'strip'), may hold values from -1 to 3, as said below
- surface_diagonal: float32 [16, 2, 3, 8100], P('tiles', 'strip'), may hold values from 0.25 to 2
- spread: float32 [3, 4], replicated, may hold values from 0.02 to 0.2
- mixing: float32 [4], replicated, may hold values from 0.02 to 0.2
- thickness: float32 [4], replicated, may hold values from 0.5 to 2
Outputs:
- adjoint_fields: float32 [16, 2, 3, 3, 4, 8100], P('tiles', 'strip')
- surface_solution: float32 [16, 2, 3, 8100], P('tiles', 'strip')
- surface_residual: float32 [16, 2, 3, 8100], P('tiles', 'strip')
The draws below stay inside these ranges and needn't reach their ends.
Inputs may be any that keep to these rules, and one draw needn't show every extreme that they name: wet_land is 1 on most cells of the first 1 to 3 slots of each device and 0 on all cells of its other slots. Offsets dt and ds are -1, 0 or 1; on the west and east sides dt is -1 and 1, on the south and north sides ds is -1 and 1; a partner slot is -1 or a slot that holds wet cells; links are mutual: side e of slot k pairs with side e XOR 1 of its partner, whose entry points back with opposite offsets and rotation code (4 - code) mod 4; an empty slot has no links; rotation codes are 0 to 3.
All inputs are finite; a program needn't handle non-finite values.
Results may differ from the reference program's by a relative error of at most 0.00027.
Values sent between devices are 32-bit elements; how exact they have to be, the bound alone decides.
A program may use at most 64 MiB of HBM per device.

```python
import math
import jax
import jax.numpy as jnp
import numpy as np
from jax import lax

TILE = 90
SLOTS = 3
FIELDS = 3
LEVELS = 4
ITERS = 2
CELLS = 8100
TILE_GROUPS = 16
STRIP_GROUPS = 2


def wet_counts(key):
    return jax.random.randint(jax.random.fold_in(key, 11), (TILE_GROUPS, STRIP_GROUPS), 1, SLOTS + 1)


def live_slots(key):
    counts = wet_counts(key)
    return jnp.arange(SLOTS, dtype=jnp.int32)[None, None, :] < counts[:, :, None]


def draw_wet_land(key, part):
    live = live_slots(key)
    ocean = jax.random.randint(jax.random.fold_in(key, 13), (TILE_GROUPS, STRIP_GROUPS, SLOTS, CELLS), 0, 8) != 0
    return (live[..., None] & ocean).astype(jnp.int32)


def slot_orders(key):
    scores = jax.random.randint(key, (TILE_GROUPS, STRIP_GROUPS, SLOTS), 0, 1 << 20) * SLOTS
    scores = scores + jnp.arange(SLOTS, dtype=jnp.int32)[None, None, :]
    order = jnp.argsort(scores, axis=-1).astype(jnp.int32)
    inverse = jnp.argsort(order, axis=-1).astype(jnp.int32)
    return (order, inverse)


def entry_table(group_shift, strip_shift, partner, code):
    shape = (TILE_GROUPS, STRIP_GROUPS, SLOTS)
    return jnp.stack([jnp.broadcast_to(group_shift, shape), jnp.broadcast_to(strip_shift, shape), jnp.broadcast_to(partner, shape), jnp.broadcast_to(code, shape)], axis=-1).astype(jnp.int32)


def draw_links(key, part):
    live = live_slots(key)
    shape = (TILE_GROUPS, STRIP_GROUPS, SLOTS)
    group_ids = jnp.arange(TILE_GROUPS, dtype=jnp.int32)[:, None, None]
    strip_ids = jnp.arange(STRIP_GROUPS, dtype=jnp.int32)[None, :, None]
    slot_ids = jnp.arange(SLOTS, dtype=jnp.int32)[None, None, :]
    east_shift = jax.random.randint(jax.random.fold_in(key, 21), (TILE_GROUPS,), -1, 2)
    east_order, east_inverse = slot_orders(jax.random.fold_in(key, 22))
    east_code = jax.random.randint(jax.random.fold_in(key, 23), shape, 0, 4)
    east_cut = jax.random.randint(jax.random.fold_in(key, 24), shape, 0, 8) == 0
    east_group = (group_ids + 1) % TILE_GROUPS
    east_strip = (strip_ids + east_shift[:, None, None]) % STRIP_GROUPS
    east_live = live & live[east_group, east_strip, east_order] & jnp.logical_not(east_cut)
    east_entry = entry_table(1, east_shift[:, None, None], jnp.where(east_live, east_order, -1), east_code)
    from_group = (group_ids - 1) % TILE_GROUPS
    west_shift = east_shift[from_group]
    from_strip = (strip_ids - west_shift) % STRIP_GROUPS
    from_slot = east_inverse[from_group, from_strip, slot_ids]
    west_live = east_live[from_group, from_strip, from_slot]
    west_code = (4 - east_code[from_group, from_strip, from_slot]) % 4
    west_entry = entry_table(-1, -west_shift, jnp.where(west_live, from_slot, -1), west_code)
    north_shift = jax.random.randint(jax.random.fold_in(key, 31), (STRIP_GROUPS,), -1, 2)
    north_order, north_inverse = slot_orders(jax.random.fold_in(key, 32))
    north_code = jax.random.randint(jax.random.fold_in(key, 33), shape, 0, 4)
    north_cut = jax.random.randint(jax.random.fold_in(key, 34), shape, 0, 8) == 0
    north_group = (group_ids + north_shift[None, :, None]) % TILE_GROUPS
    north_strip = (strip_ids + 1) % STRIP_GROUPS
    north_live = live & live[north_group, north_strip, north_order] & jnp.logical_not(north_cut)
    north_entry = entry_table(north_shift[None, :, None], 1, jnp.where(north_live, north_order, -1), north_code)
    below_strip = (strip_ids - 1) % STRIP_GROUPS
    south_shift = north_shift[below_strip]
    below_group = (group_ids - south_shift) % TILE_GROUPS
    below_slot = north_inverse[below_group, below_strip, slot_ids]
    south_live = north_live[below_group, below_strip, below_slot]
    south_code = (4 - north_code[below_group, below_strip, below_slot]) % 4
    south_entry = entry_table(-south_shift, -1, jnp.where(south_live, below_slot, -1), south_code)
    return jnp.stack([west_entry, east_entry, south_entry, north_entry], axis=3)


def steps_of(stream_key, dims, cuts, low, largest):
    def one(position, blocks):
        draws = jax.random.uniform(jax.random.fold_in(jax.random.fold_in(stream_key, 6), position), (blocks,), jnp.float32, low / len(cuts), largest / len(cuts))
        return jnp.repeat(jnp.exp(draws), dims[position] // blocks).reshape((-1,) + (1,) * (len(dims) - position - 1))

    level = one(*cuts[0])
    for cut in cuts[1:]:
        level = level * one(*cut)
    return level


def scatter_about(key, extent, scale, bound, cuts=(), kind=jnp.bfloat16):
    gain = steps_of(key, extent, cuts, -0.22, 0.18) if cuts else 1.0
    values = jax.random.normal(key, extent, jnp.float32) * scale * gain
    return jnp.minimum(jnp.maximum(values, -bound), bound).astype(kind)


def setup_inputs(seed: int = 0) -> dict:
    key_list = jax.random.split(jax.random.key(seed), 8)
    return {
        "fields": scatter_about(key_list[0], (TILE_GROUPS, STRIP_GROUPS, SLOTS, FIELDS, LEVELS, CELLS), 1.0, 6.0, ((0, 16), (1, 2)), jnp.float32),
        "wet_land": draw_wet_land(jax.random.fold_in(key_list[7], 71), 0),
        "links": draw_links(jax.random.fold_in(key_list[7], 71), 0),
        "surface_diagonal": jnp.clip(0.25 + 1.75 * jax.random.uniform(key_list[3], (TILE_GROUPS, STRIP_GROUPS, SLOTS, CELLS), jnp.float32) ** steps_of(key_list[3], (TILE_GROUPS, STRIP_GROUPS, SLOTS, CELLS), ((0, 16), (1, 2)), -0.2, 0.2), 0.25, 2.0),
        "spread": jnp.clip(jnp.exp(jax.random.uniform(key_list[4], (FIELDS, LEVELS), jnp.float32, math.log(0.02), math.log(0.2))), 0.02, 0.2),
        "mixing": jnp.clip(jnp.exp(jax.random.uniform(key_list[5], (LEVELS,), jnp.float32, math.log(0.02), math.log(0.2))), 0.02, 0.2),
        "thickness": jnp.clip(jnp.exp(jax.random.uniform(key_list[6], (LEVELS,), jnp.float32, math.log(0.5), math.log(2.0))), 0.5, 2.0),
    }


OPPOSITE = np.array([1, 0, 3, 2], np.int32)


def rim_rows(values, width):
    west_rim = values[..., ::width]
    east_rim = values[..., width - 1::width]
    south_rim = values[..., :width]
    north_rim = values[..., -width:]
    return jnp.concatenate([west_rim, east_rim, south_rim, north_rim], axis=-1)


def beside_values(values, rims, width):
    cells_total = values.shape[-1]
    leading = values.shape[:-1]
    places = jnp.arange(cells_total, dtype=jnp.int32)
    column_index = places % width
    row_index = places // width
    west_full = jnp.broadcast_to(rims[..., 0, :, None], leading + (width, width)).reshape(leading + (cells_total,))
    east_full = jnp.broadcast_to(rims[..., 1, :, None], leading + (width, width)).reshape(leading + (cells_total,))
    south_full = jnp.broadcast_to(rims[..., 2, None, :], leading + (width, width)).reshape(leading + (cells_total,))
    north_full = jnp.broadcast_to(rims[..., 3, None, :], leading + (width, width)).reshape(leading + (cells_total,))
    zero_cell = jnp.zeros(leading + (1,), jnp.float32)
    zero_line = jnp.zeros(leading + (width,), jnp.float32)
    west_side = jnp.where(column_index == 0, west_full, jnp.concatenate([zero_cell, values[..., :-1]], -1))
    east_side = jnp.where(column_index == width - 1, east_full, jnp.concatenate([values[..., 1:], zero_cell], -1))
    south_side = jnp.where(row_index == 0, south_full, jnp.concatenate([zero_line, values[..., :-width]], -1))
    north_side = jnp.where(row_index == width - 1, north_full, jnp.concatenate([values[..., width:], zero_line], -1))
    return west_side, east_side, south_side, north_side


def orient(picked, links, vector):
    code = links[..., 3]
    partner = links[..., 2]
    lead = code.ndim
    extra = picked.ndim - lead
    tail_shape = code.shape + (1,) * extra
    flipped = jnp.where((code != 0).reshape(tail_shape), jnp.flip(picked, -1), picked)
    flipped = flipped * (partner >= 0).astype(jnp.float32).reshape(tail_shape)
    if vector:
        turn_shape = code.shape + (1,) * (extra - 1)
        cosine_part = ((code == 0).astype(jnp.float32) - (code == 2).astype(jnp.float32)).reshape(turn_shape)
        sine_part = ((code == 1).astype(jnp.float32) - (code == 3).astype(jnp.float32)).reshape(turn_shape)
        eastward = jnp.take(flipped, 0, axis=lead)
        northward = jnp.take(flipped, 1, axis=lead)
        scalar_part = jnp.take(flipped, 2, axis=lead)
        flipped = jnp.stack([cosine_part * eastward + sine_part * northward,
                             cosine_part * northward - sine_part * eastward, scalar_part], axis=lead)
    return jnp.moveaxis(flipped, lead - 1, -2)


def slab_step(fields, wet, rims, spread, mixing, thickness, width):
    wet_cells = wet[..., None, None, :]
    masked = fields * wet_cells
    west_side, east_side, south_side, north_side = beside_values(masked, rims, width)
    flat_term = west_side + east_side + south_side + north_side - 4.0 * masked
    above = jnp.concatenate([masked[..., 1:, :], masked[..., -1:, :]], axis=-2)
    below = jnp.concatenate([masked[..., :1, :], masked[..., :-1, :]], axis=-2)
    column_term = above + below - 2.0 * masked
    updated = wet_cells * (masked + spread[:, :, None] * flat_term + mixing[:, None] * column_term)
    flux = 0.5 * (east_side[..., 0, :, :] - west_side[..., 0, :, :] + north_side[..., 1, :, :] - south_side[..., 1, :, :])
    source = wet * jnp.sum(thickness[:, None] * flux, axis=-2)
    return updated, source


def surface_apply(values, wet, rims, diagonal, width):
    west_side, east_side, south_side, north_side = beside_values(values, rims, width)
    return wet * ((4.0 + diagonal) * values - (west_side + east_side + south_side + north_side))


def pick_global(packs, links):
    group_shift = links[..., 0]
    strip_shift = links[..., 1]
    partner = jnp.maximum(links[..., 2], 0)
    group_index = (jnp.arange(TILE_GROUPS, dtype=jnp.int32)[:, None, None, None] + group_shift) % TILE_GROUPS
    strip_index = (jnp.arange(STRIP_GROUPS, dtype=jnp.int32)[None, :, None, None] + strip_shift) % STRIP_GROUPS
    opposite = jnp.broadcast_to(jnp.asarray(OPPOSITE)[None, None, None, :], partner.shape)
    return packs[group_index, strip_index, partner, ..., opposite, :]


def reference(fields, wet_land, links, surface_diagonal, spread, mixing, thickness):
    wet = wet_land.astype(jnp.float32)
    masked = fields * wet[:, :, :, None, None, :]
    slab_packs = rim_rows(masked, TILE).reshape(masked.shape[:-1] + (4, TILE))
    slab_rims = orient(pick_global(slab_packs, links), links, True)

    def one_group(items):
        group_fields, group_wet, group_rims = items
        return slab_step(group_fields, group_wet, group_rims, spread, mixing, thickness, TILE)

    updated, source = lax.map(one_group, (fields, wet, slab_rims))

    def surface_image(values):
        packs = rim_rows(values, TILE).reshape(values.shape[:-1] + (4, TILE))
        rims = orient(pick_global(packs, links), links, False)
        return surface_apply(values, wet, rims, surface_diagonal, TILE)

    solution = jnp.zeros_like(source)
    residual = source
    direction = source
    norm_now = jnp.sum(residual * residual)
    for iteration in range(ITERS):
        image = surface_image(direction)
        alpha = norm_now / jnp.sum(direction * image)
        solution = solution + alpha * direction
        residual = residual - alpha * image
        if iteration + 1 < ITERS:
            norm_next = jnp.sum(residual * residual)
            direction = residual + (norm_next / norm_now) * direction
            norm_now = norm_next
    return updated, solution, residual
```

```python
import math

import jax
import jax.numpy as jnp
from jax import lax
from jax.experimental import pallas as pl
from jax.experimental.pallas import tpu as pltpu
from jax.sharding import PartitionSpec as P

LANES = 128
CHUNK = 1024
POS = (0, 3, 1, 2)
GROUP = 16


def offsets(size):
    return (-1, 0, 1) if size >= 3 else tuple(range(size))


def place(offset, size):
    if size >= 3:
        return offset + 1
    return offset * offset if size == 2 else 0 * offset


def roll(value, shift, axis=1):
    size = value.shape[axis]
    shift = shift % size
    return pltpu.roll(value, shift, axis) if shift else value


def window(size):
    return (-3, 3) if size >= 7 else (0, size - 1)


def slot_of(offset, size):
    return offset + 3 if size >= 7 else offset % size


def build(tiles, strips, slots, fields_n, levels, cells):
    width = math.isqrt(cells)
    n_tiles = -(-cells // CHUNK) * CHUNK // LANES
    wide = n_tiles * LANES
    padded = wide + 2 * LANES
    chunks = wide // CHUNK
    steps_t, steps_s = offsets(tiles), offsets(strips)
    n_s = len(steps_s)
    n_dirs = len(steps_t) * n_s
    low = min(GROUP, tiles)
    high = tiles // low
    first = low * strips
    half = 4
    span_t = window(tiles)
    span_s = window(strips)
    far_t = span_t[1] - span_t[0] + 1
    far_s = span_s[1] - span_s[0] + 1
    n_far = far_t * far_s
    n_far_even = n_far + n_far % 2
    directions = []
    for dt in steps_t:
        for ds in steps_s:
            if dt == 0 and ds == 0:
                continue
            sides = []
            if dt == -1 or (tiles == 2 and dt):
                sides.append(0)
            if ds == -1 or (strips == 2 and ds):
                sides.append(1)
            if ds == 1:
                sides.append(2)
            if dt == 1:
                sides.append(3)
            here = place(dt, tiles) * n_s + place(ds, strips)
            back = place(-dt if tiles >= 3 else dt, tiles) * n_s + place(-ds if strips >= 3 else ds, strips)
            directions.append((dt, ds, here, back, min(sides), max(sides) + 1))
    directions.sort(key=lambda d: -abs(d[0]) - abs(d[1]))
    around = []
    for dt in range(span_t[0], span_t[1] + 1):
        for ds in range(span_s[0], span_s[1] + 1):
            here = slot_of(dt, tiles) * far_s + slot_of(ds, strips)
            back = slot_of(-dt, tiles) * far_s + slot_of(-ds, strips)
            around.append((dt, ds, here, back))
    self_far = slot_of(0, tiles) * far_s + slot_of(0, strips)
    around = [a for a in around if a[2] != self_far]
    around.sort(key=lambda a: -abs(a[0]))

    def reach(steps):
        if tiles < 7:
            return list(range(n_far))
        return [n for n in range(n_far) if abs(n // far_s - 3) <= steps]

    def kernel(
        fields, wet_in, links_in, diag_in, spread_in, mixing_in, thick_in, out_f, out_x, out_r,
        links, spread, mixing, thick, fbuf, wbuf, dbuf, m_ref, w_ref, d_ref, nw_ref, ne_ref, uv_ref, s_ref, u_ref, v_ref, eba_ref, ebb_ref, ebs_ref,
        got_ref, rima_ref, rimb_ref, rims_ref, pack1, near1, packb, nearb, cpack, cnear, row_ref, red_ref, red2_ref,
        in_sem, send1, recv1, sendb, recvb, sendc, recvc, sendr, recvr, sendq, recvq,
    ):
        t = lax.axis_index("tiles")
        s = lax.axis_index("strip")
        copies = [
            pltpu.make_async_copy(wet_in.at[0], wbuf, in_sem.at[0]),
            pltpu.make_async_copy(diag_in.at[0], dbuf, in_sem.at[1]),
        ] + [pltpu.make_async_copy(fields.at[0, 0, k], fbuf.at[k], in_sem.at[2 + k]) for k in range(slots)]
        small = [
            pltpu.make_async_copy(thick_in, thick, in_sem.at[2 + slots]),
            pltpu.make_async_copy(mixing_in, mixing, in_sem.at[3 + slots]),
            pltpu.make_async_copy(spread_in, spread, in_sem.at[4 + slots]),
            pltpu.make_async_copy(links_in.at[0, 0], links, in_sem.at[5 + slots]),
        ]
        for copy in copies[:3] + small + copies[3:]:
            copy.start()

        barrier = pltpu.get_barrier_semaphore()
        base = (t // low) * low
        place_t = t % low
        me_first = place_t * strips + s
        peers = 0
        for j in range(1, first):
            other = lax.rem(me_first + j, first)
            pl.semaphore_signal(
                barrier, inc=1, device_id=(base + other // strips, other % strips),
                device_id_type=pl.DeviceIdType.MESH,
            )
            peers += 1
        for j in range(1, high):
            other = lax.rem(t // low + j, high)
            pl.semaphore_signal(
                barrier, inc=1, device_id=(other * low + place_t, s), device_id_type=pl.DeviceIdType.MESH
            )
            peers += 1
        if high > 1:
            for dt, ds, here, back in around:
                pl.semaphore_signal(
                    barrier, inc=1,
                    device_id=(lax.rem(t + dt + tiles, tiles), lax.rem(s + ds + strips, strips)),
                    device_id_type=pl.DeviceIdType.MESH,
                )
                peers += 1

        def exchange(pack, near, send_sem, recv_sem):
            out = []
            for dt, ds, here, back, lo, hi in directions:
                copy = pltpu.make_async_remote_copy(
                    src_ref=pack.at[pl.ds(lo, hi - lo)],
                    dst_ref=near.at[back, pl.ds(lo, hi - lo)],
                    send_sem=send_sem.at[here],
                    recv_sem=recv_sem.at[back],
                    device_id=(lax.rem(t + dt + tiles, tiles), lax.rem(s + ds + strips, strips)),
                    device_id_type=pl.DeviceIdType.MESH,
                )
                copy.start()
                out.append(copy)
            return out

        lane = lax.broadcasted_iota(jnp.int32, (1, LANES), 1)
        flip_at = jnp.where(lane < width, width - 1 - lane, lane)

        def flip(value):
            rows = value.shape[0]
            if rows < 8:
                value = jnp.concatenate([value, jnp.zeros((8 - rows, LANES), jnp.float32)], 0)
            at = jnp.broadcast_to(flip_at, value.shape)
            return jnp.take_along_axis(value, at, axis=1)[:rows]

        def spread_corners():
            out = []
            for dt, ds, here, back in around:
                copy = pltpu.make_async_remote_copy(
                    src_ref=cpack,
                    dst_ref=cnear.at[back],
                    send_sem=sendc.at[here],
                    recv_sem=recvc.at[back],
                    device_id=(lax.rem(t + dt + tiles, tiles), lax.rem(s + ds + strips, strips)),
                    device_id_type=pl.DeviceIdType.MESH,
                )
                copy.start()
                out.append(copy)
            return out

        def pick(value, at):
            rows = value.shape[0]
            if rows < 8:
                value = jnp.concatenate([value, jnp.zeros((8 - rows, LANES), jnp.float32)], 0)
            return jnp.take_along_axis(value, jnp.broadcast_to(at, value.shape), axis=1)

        def extract(tile, rows, depth):
            blank = jnp.zeros((rows, LANES), jnp.float32)
            period = 2 * depth
            parts = [blank] * period
            loaded = {}

            def at(n):
                if n not in loaded:
                    loaded[n] = tile(n)
                return loaded[n]

            for i in range(-1, width):
                pe = width * i + width - 1
                shift = (i - pe) % LANES
                reach_lo = pe - depth + 1 if i >= 0 else pe + 1
                reach_hi = pe + depth if i + 1 < width else pe
                for n in range(reach_lo // LANES, reach_hi // LANES + 1):
                    lo, hi = max(reach_lo, n * LANES), min(reach_hi, n * LANES + LANES - 1)
                    begin = (i + lo - pe) % LANES
                    mask = ((lane - begin) & (LANES - 1)) <= hi - lo if hi > lo else lane == begin
                    parts[i % period] = jnp.where(mask, roll(at(n), shift), parts[i % period])
            signed = jnp.where(lane >= LANES - depth, lane - LANES + period * LANES, lane)
            rest = signed - period * ((signed * ((1 << 12) // period + 1)) >> 12)

            def gather(offset, turn_by):
                total = parts[(0 + offset) % period]
                for m in range(1, period):
                    total = jnp.where(rest == m, parts[(m + offset) % period], total)
                total = roll(total, turn_by)
                return jnp.where(lane < width, total, 0.0)

            def line(start):
                a, n = start % LANES, start // LANES
                if a == 0:
                    return jnp.where(lane < width, at(n), 0.0)
                head = roll(at(n), -a)
                if a + width <= LANES:
                    return jnp.where(lane < width, head, 0.0)
                tail = roll(at(n + 1), -a)
                return jnp.where(lane < LANES - a, head, jnp.where(lane < width, tail, 0.0))

            west = [gather(-d - 1, -d) for d in range(depth)]
            east = [gather(d, d) for d in range(depth)]
            south = [line(width * d) for d in range(depth)]
            north = [line(width * (width - 1 - d)) for d in range(depth)]
            return west, east, south, north

        def insert(west, east, south, north, store):
            even = (lane & 1) == 0
            mixed = (jnp.where(even, east, west), jnp.where(even, west, east))
            tiles_of = {}

            def add(n, mask, value):
                tiles_of.setdefault(n, []).append((mask, value))

            for i in range(-1, width):
                pe = width * i + width - 1
                pw = pe + 1
                turned = roll(mixed[i % 2], (pe - i) % LANES)
                if i >= 0 and i + 1 < width and pe // LANES == pw // LANES:
                    mask = (lane == pe % LANES) | (lane == pw % LANES)
                    add(pe // LANES, mask, turned)
                else:
                    if i >= 0:
                        add(pe // LANES, lane == pe % LANES, turned)
                    if i + 1 < width:
                        add(pw // LANES, lane == pw % LANES, turned)
            extra = {}
            for start, rim in ((0, south), (width * (width - 1), north)):
                a, n = start % LANES, start // LANES
                turned = roll(rim, a)
                extra.setdefault(n, []).append(jnp.where(lane >= a, turned, 0.0) if a else turned)
                if a + width > LANES:
                    extra.setdefault(n + 1, []).append(jnp.where(lane < a + width - LANES, turned, 0.0))
            blank = jnp.zeros(west.shape, jnp.float32)
            for n in range(n_tiles):
                total = blank
                for mask, value in tiles_of.get(n, ()):
                    total = jnp.where(mask, value, total)
                for value in extra.get(n, ()):
                    total = total + value
                store(n, total)

        shift_bits = 22
        factor = (1 << shift_bits) // width + 1
        for c in range(chunks):
            index = lax.broadcasted_iota(jnp.int32, (1, CHUNK), 1) + c * CHUNK
            column = index - width * ((index * factor) >> shift_bits)
            nw_ref[:, pl.ds(c * CHUNK, CHUNK)] = jnp.where(column == 0, 0.0, 1.0)
            ne_ref[:, pl.ds(c * CHUNK, CHUNK)] = jnp.where(column == width - 1, 0.0, 1.0)
        tail = wide - LANES
        m_ref[:, :, :LANES] = jnp.zeros((slots * fields_n, levels, LANES), jnp.float32)
        m_ref[:, :, tail + LANES :] = jnp.zeros((slots * fields_n, levels, 2 * LANES), jnp.float32)
        uv_ref[:, :LANES] = jnp.zeros((2 * half, LANES), jnp.float32)
        uv_ref[:, tail + LANES :] = jnp.zeros((2 * half, 2 * LANES), jnp.float32)
        for f in range(2):
            for k in range(slots, half):
                uv_ref[f * half + k : f * half + k + 1, :] = jnp.zeros((1, padded), jnp.float32)
        for ref in (s_ref, u_ref):
            ref[:, :LANES] = jnp.zeros((slots, LANES), jnp.float32)
            ref[:, wide + LANES :] = jnp.zeros((slots, LANES), jnp.float32)
        w_ref[:, tail:] = jnp.zeros((slots, LANES), jnp.float32)
        d_ref[:, tail:] = jnp.zeros((slots, LANES), jnp.float32)
        rima_ref[...] = jnp.zeros(rima_ref.shape, jnp.float32)

        def per_level(read):
            level = lax.broadcasted_iota(jnp.int32, (levels, 1), 0)
            value = jnp.zeros((levels, 1), jnp.float32)
            for n in range(levels):
                value = jnp.where(level == n, read(n), value)
            return value

        for copy in small:
            copy.wait()
        thick_col = per_level(lambda n: thick[n])
        mix_col = per_level(lambda n: mixing[n])

        def choose(number, test, yes, no):
            return jnp.where(test(jnp.full(yes.shape, number, jnp.int32)), yes, no)

        sub = lax.broadcasted_iota(jnp.int32, (slots, LANES), 0)
        sub8 = lax.broadcasted_iota(jnp.int32, (8, LANES), 0)
        group, lane32 = lane >> 5, lane & 31
        own_k, own_e, own_n = lane32 >> 3, (lane32 >> 1) & 3, lane32 & 1

        def code_rows(e):
            value = jnp.zeros((slots, LANES), jnp.int32)
            for k in range(slots):
                value = jnp.where(sub == k, jnp.full(value.shape, links[k, e, 3], jnp.int32), value)
            return value

        codes = [code_rows(e) for e in range(4)]

        def turn(code):
            a = jnp.where(code == 0, 1.0, jnp.where(code == 2, -1.0, 0.0))
            b = jnp.where(code == 1, 1.0, jnp.where(code == 3, -1.0, 0.0))
            return a, b

        own_links = []
        for n in range(4):
            value = jnp.zeros((1, LANES), jnp.int32)
            for k in range(slots):
                for e in range(4):
                    value = jnp.where((lane32 >> 1) == 4 * k + e, jnp.full(value.shape, links[k, e, n], jnp.int32), value)
            own_links.append(value)

        copies[0].wait()
        copies[1].wait()
        spans = [(c * CHUNK, min(CHUNK, cells - c * CHUNK)) for c in range(chunks)]
        for k in range(slots):
            for at, size in spans:
                w_ref[k : k + 1, pl.ds(at, size)] = wbuf[k, :, pl.ds(at, size)].astype(jnp.float32)
                d_ref[k : k + 1, pl.ds(at, size)] = dbuf[k, :, pl.ds(at, size)] + 4.0

        q_rims = extract(
            lambda n: w_ref[:, pl.ds(LANES * n, LANES)] * d_ref[:, pl.ds(LANES * n, LANES)], slots, 2
        )
        w_rims = [[jnp.where(x > 0.0, 1.0, 0.0) for x in side] for side in q_rims]

        def pre_flip(e, value):
            return jnp.where(codes[e] != 0, flip(value), value)

        for e in range(4):
            value = pre_flip(e, q_rims[e][0])
            for k in range(slots):
                pack1[POS[e], k, 3:4, :] = value[k : k + 1]

        cpack[0:1, :] = jnp.where(
            group == 0, own_links[0],
            jnp.where(group == 1, own_links[1], jnp.where(group == 2, own_links[2], own_links[3])),
        ).astype(jnp.float32)
        cpack[3:4, :] = jnp.zeros((1, LANES), jnp.float32)
        step = jnp.where(group >= 2, 1, 0)
        ends_at = jnp.where(own_n == 0, step, width - 1 - step)
        step2 = jnp.where(group == 2, 1, 0)
        ends_at2 = jnp.where(own_n == 0, step2, width - 1 - step2)

        for k in range(slots):
            copies[2 + k].wait()
            for f in range(fields_n):
                for at, size in spans:
                    masked = fbuf[k, f, :, pl.ds(at, size)] * w_ref[k : k + 1, pl.ds(at, size)]
                    m_ref[k * fields_n + f, :, pl.ds(LANES + at, size)] = masked
                    if f < 2:
                        uv_ref[f * half + k : f * half + k + 1, pl.ds(LANES + at, size)] = jnp.sum(
                            masked * thick_col, axis=0, keepdims=True
                        )

        uv_rims = extract(lambda n: uv_ref[:, pl.ds(LANES * (n + 1), LANES)], 2 * half, 3)
        sent_rims, s_local = [], []
        ends_uv = jnp.zeros((8, LANES), jnp.float32)
        ends_s = jnp.zeros((8, LANES), jnp.float32)
        for e in range(4):
            us = [x[0:slots] for x in uv_rims[e]]
            vs = [x[half : half + slots] for x in uv_rims[e]]
            normal, along = (us, vs) if e < 2 else (vs, us)
            sign = 0.5 if e in (0, 2) else -0.5
            w0, w1, q0 = w_rims[e][0], w_rims[e][1], q_rims[e][0]

            def slope(x):
                return 0.5 * (roll(x, -1) - roll(x, 1))

            s0 = w0 * (sign * normal[1] + slope(along[0]))
            s1 = w1 * (sign * (normal[2] - normal[0]) + slope(along[1]))
            u0 = q0 * s0 - w0 * (s1 + (roll(s0, -1) + roll(s0, 1)))
            a, b = turn(codes[e])
            rim = a * us[0] - b * vs[0] if e < 2 else a * vs[0] + b * us[0]
            for r, value in enumerate((rim, s0, u0)):
                value = pre_flip(e, value)
                for k in range(slots):
                    pack1[POS[e], k, r : r + 1, :] = value[k : k + 1]
            sent_rims.append(rim)
            s_local.append(s0)
            mine = own_e == e
            ends_uv = jnp.where(
                mine & ((sub8 & 3) == own_k) & ((sub8 >> 2) == (group & 1)), pick(uv_rims[e][0], ends_at), ends_uv
            )
            mine = mine & (sub8 == own_k)
            ends_s = jnp.where(mine & (group == 0), pick(s0, jnp.broadcast_to(ends_at2, (8, LANES))), ends_s)
            ends_s = jnp.where(mine & ((group == 1) | (group == 2)), pick(w0, ends_at2), ends_s)
        cpack[1:2, :] = jnp.sum(ends_uv, axis=0, keepdims=True)
        cpack[2:3, :] = jnp.sum(ends_s, axis=0, keepdims=True)

        pl.semaphore_wait(barrier, peers)
        sent1 = exchange(pack1, near1, send1, recv1)
        sentc = spread_corners()
        cnear[self_far] = cpack[...]
        if n_far_even > n_far:
            cnear[n_far] = jnp.zeros((4, LANES), jnp.float32)

        def slab_pack(kf, carry):
            rims = extract(lambda n: m_ref[kf, :, pl.ds(LANES * (n + 1), LANES)], levels, 1)
            for e, rim in enumerate(rims):
                packb[POS[e], kf] = rim[0]
            return carry

        lax.fori_loop(0, slots * fields_n, slab_pack, 0)
        sentb = exchange(packb, nearb, sendb, recvb)

        def entry(k, e):
            dt, ds, p, code = (links[k, e, n] for n in range(4))
            source = place(dt, tiles) * n_s + place(ds, strips)
            return source, jnp.maximum(p, 0), p, code

        inner = slice(LANES, LANES + CHUNK)

        def image(x_ref, at):
            span = pl.ds(at, CHUNK)
            win = x_ref[:, pl.ds(at, CHUNK + 2 * LANES)]
            near = ne_ref[:, span] * roll(win, -1)[:, inner] + nw_ref[:, span] * roll(win, 1)[:, inner]
            near = near + (roll(win, -width)[:, inner] + roll(win, width)[:, inner])
            return w_ref[:, span] * (d_ref[:, span] * win[:, inner] - near)

        def whole(value):
            return jnp.sum(jnp.sum(value, axis=1, keepdims=True), axis=0, keepdims=True)

        for c in range(chunks):
            at = c * CHUNK
            span = pl.ds(at, CHUNK)
            u_win = uv_ref[0:slots, pl.ds(at, CHUNK + 2 * LANES)]
            v_win = uv_ref[half : half + slots, pl.ds(at, CHUNK + 2 * LANES)]
            flux = ne_ref[:, span] * roll(u_win, -1)[:, inner] - nw_ref[:, span] * roll(u_win, 1)[:, inner]
            flux = flux + (roll(v_win, -width)[:, inner] - roll(v_win, width)[:, inner])
            s_ref[:, pl.ds(LANES + at, CHUNK)] = w_ref[:, span] * (0.5 * flux)
        blank = jnp.zeros((slots, CHUNK), jnp.float32)
        ss = su = blank
        for c in range(chunks):
            x = s_ref[:, pl.ds(LANES + c * CHUNK, CHUNK)]
            y = image(s_ref, c * CHUNK)
            ss, su = ss + x * x, su + x * y
        ss, su = whole(ss), whole(su)
        ratio = jnp.where(su > 0.0, ss / su, 0.0)

        def slab_inner(k):
            def one(f, carry):
                spread_col = per_level(lambda n: spread[f, n])
                for at, size in spans:
                    span = pl.ds(at, CHUNK)
                    win = m_ref[k * fields_n + f, :, pl.ds(at, CHUNK + 2 * LANES)]
                    mid = win[:, inner]
                    flat = ne_ref[:, span] * roll(win, -1)[:, inner] + nw_ref[:, span] * roll(win, 1)[:, inner]
                    flat = flat + (roll(win, -width)[:, inner] + roll(win, width)[:, inner])
                    flat = flat - 4.0 * mid
                    above = jnp.concatenate([mid[1:], mid[-1:]], 0)
                    below = jnp.concatenate([mid[:1], mid[:-1]], 0)
                    column = above + below - 2.0 * mid
                    new = w_ref[k : k + 1, span] * (mid + spread_col * flat + mix_col * column)
                    out_f[0, 0, k, f, :, pl.ds(at, size)] = new[:, :size]
                return carry

            lax.fori_loop(0, fields_n, one, 0)

        def slab_rims(k):
            for e in range(4):
                source, slot, p, code = entry(k, e)
                a, b = turn(code)
                got = []
                for f in range(fields_n):
                    rim = nearb[source, POS[e ^ 1], slot * fields_n + f]
                    rim = choose(code, lambda x: x != 0, flip(rim), rim)
                    got.append(choose(p, lambda x: x >= 0, rim, jnp.zeros_like(rim)))
                rims_ref[e, 0] = a * got[0] + b * got[1]
                rims_ref[e, 1] = a * got[1] - b * got[0]
                for f in range(2, fields_n):
                    rims_ref[e, f] = got[f]

            def one(f, carry):
                def store(n, value):
                    ebs_ref[:, pl.ds(n * LANES, LANES)] = value

                insert(rims_ref[0, f], rims_ref[1, f], rims_ref[2, f], rims_ref[3, f], store)
                spread_col = per_level(lambda n: spread[f, n])
                for at, size in spans:
                    wet = w_ref[k : k + 1, pl.ds(at, size)]
                    old = out_f[0, 0, k, f, :, pl.ds(at, size)]
                    out_f[0, 0, k, f, :, pl.ds(at, size)] = old + wet * (spread_col * ebs_ref[:, pl.ds(at, size)])
                return carry

            lax.fori_loop(0, fields_n, one, 0)

        for k in range(slots):
            slab_inner(k)

        for copy in sent1:
            copy.wait_recv()
        for e in range(4):
            for k in range(slots):
                source, slot, p, code = entry(k, e)
                got = near1[source, POS[e ^ 1], slot]
                got = choose(p, lambda x: x >= 0, got, jnp.zeros_like(got))
                for r in range(4):
                    got_ref[r, e, k : k + 1, :] = got[r : r + 1]
        for copy in sentc:
            copy.wait_recv()

        def lookup(steps, at, target):
            at = 32 * group + at
            total = jnp.zeros((8, LANES), jnp.float32)
            wanted = target - (sub8 >> 2)
            near = reach(steps)
            for n in range(near[0] - near[0] % 2, near[-1] + 1, 2):
                pair = jnp.concatenate([cnear[n], cnear[n + 1]], 0)
                found = jnp.take_along_axis(pair, jnp.broadcast_to(at, pair.shape), axis=1)
                total = jnp.where(wanted == n, found, total)
            return total + roll(total, 4, 0)

        apart = lane32 + 32 * (sub8 & 3)

        def quantities(found, r):
            value = jnp.take_along_axis(jnp.broadcast_to(found[r : r + 1], (8, LANES)), apart, axis=1)
            return [value[n : n + 1] for n in range(4)]

        def far(dt, ds):
            if tiles >= 7:
                at_t = dt + 3
            else:
                at_t = dt - tiles * jnp.floor(dt * (1.0 / tiles) + 1e-3)
            if strips >= 7:
                at_s = ds + 3
            else:
                at_s = ds - strips * jnp.floor(ds * (1.0 / strips) + 1e-3)
            return at_t * far_s + at_s

        dt1, ds1, p1, c1 = (x.astype(jnp.float32) for x in own_links)
        one_if = lambda test: jnp.where(test, 1, 0)
        end1 = own_n ^ one_if(c1 != 0.0)
        side_f = jnp.where(own_e < 2, 2, 0) + end1
        end_f = 1 - (own_e & 1)
        lane1 = jnp.maximum(p1, 0.0).astype(jnp.int32) * 8 + side_f * 2 + end_f
        found1 = lookup(1, lane1, far(dt1, ds1).astype(jnp.int32))
        dt2, ds2, p2, c2 = quantities(found1, 0)
        u_c, v_c, _, _ = quantities(found1, 1)
        _, w_c, w_n, _ = quantities(found1, 2)
        side_g = side_f ^ 1
        end2 = end_f ^ one_if(c2 != 0.0)
        side_h = jnp.where(side_g < 2, 2, 0) + end2
        end_h = side_g & 1
        slot2 = jnp.maximum(p2, 0.0).astype(jnp.int32) * 8
        dt12, ds12 = dt1 + dt2, ds1 + ds2
        lane2 = slot2 + side_g * 2 + end2
        lane2h = slot2 + side_h * 2 + end_h
        found2 = lookup(2, jnp.where((sub8 & 3) == 0, lane2h, lane2), far(dt12, ds12).astype(jnp.int32))
        dt3, ds3, p3, c3 = quantities(found2, 0)
        u_g, v_g, u_g1, v_g1 = quantities(found2, 1)
        s_g, w_g, _, _ = quantities(found2, 2)
        lane3 = jnp.maximum(p3, 0.0).astype(jnp.int32) * 8 + (side_h ^ 1) * 2 + (end_h ^ one_if(c3 != 0.0))
        found3 = lookup(3, lane3, far(dt12 + dt3, ds12 + ds3).astype(jnp.int32))
        u_h, v_h, _, _ = quantities(found3, 1)

        def arriving(a, b, u, v, side):
            value = jnp.where(side < 2, a * u + b * v, a * v - b * u)
            return jnp.where((side & 1) == 0, -0.5, 0.5) * value

        a2, b2 = turn(c2)
        a3, b3 = turn(c3)
        live2 = (p1 >= 0.0) & (p2 >= 0.0)
        first_in = jnp.where(live2, w_c * arriving(a2, b2, u_g, v_g, side_f), 0.0)
        next_in = jnp.where(live2, w_n * arriving(a2, b2, u_g1, v_g1, side_f), 0.0)
        beyond = arriving(a2, -b2, u_c, v_c, side_g)
        beyond = beyond + jnp.where(p3 >= 0.0, arriving(a3, b3, u_h, v_h, side_h), 0.0)
        beyond = jnp.where(live2, s_g + w_g * beyond, 0.0)
        next_in = next_in + beyond
        first_in = jnp.broadcast_to(first_in, (8, LANES))
        next_in = jnp.broadcast_to(next_in, (8, LANES))

        rho = [(0.5 if e in (1, 3) else -0.5) * got_ref[0, e] for e in range(4)]

        def side_totals(west, east, south, north):
            end = slice(width - 1, width)

            def ends(at_first, at_last):
                return jnp.where(lane == 0, at_first, jnp.where(lane == width - 1, at_last, 0.0))

            return (
                west + ends(south[:, :1], north[:, :1]),
                east + ends(south[:, end], north[:, end]),
                south + ends(west[:, :1], east[:, :1]),
                north + ends(west[:, end], east[:, end]),
            )

        totals = side_totals(*rho)
        at_end = (lane == 0) | (lane == width - 1)
        by_end = (lane == 1) | (lane == width - 2)
        for e in range(4):
            mine = s_local[e] + w_rims[e][0] * totals[e]
            q = got_ref[3, e]
            wet = jnp.where(q > 0.0, 1.0, 0.0)
            delta = wet * ((-0.5 if e in (1, 3) else 0.5) * sent_rims[e])
            at = (sub8 & 3) * 8 + 2 * e + jnp.where(lane >= width // 2, 1, 0)
            at_first = jnp.take_along_axis(first_in, at, axis=1)[:slots]
            at_next = jnp.take_along_axis(next_in, at, axis=1)[:slots]
            delta = delta + jnp.where(at_end, at_first, 0.0)
            there = got_ref[1, e] + delta
            beside = (roll(delta, -1) + roll(delta, 1)) + mine
            beside = beside + jnp.where(at_end, at_next, 0.0)
            image_there = got_ref[2, e] + q * delta - wet * beside
            rima_ref[e, 0:slots, :] = rho[e]
            rima_ref[e, half : half + slots, :] = there
            rimb_ref[e] = image_there

        def store_a(n, value):
            eba_ref[:, pl.ds(n * LANES, LANES)] = value

        def store_b(n, value):
            ebb_ref[:, pl.ds(n * LANES, LANES)] = value

        insert(rima_ref[0], rima_ref[1], rima_ref[2], rima_ref[3], store_a)
        insert(rimb_ref[0], rimb_ref[1], rimb_ref[2], rimb_ref[3], store_b)
        for c in range(chunks):
            span, shifted = pl.ds(c * CHUNK, CHUNK), pl.ds(LANES + c * CHUNK, CHUNK)
            s_ref[:, shifted] = s_ref[:, shifted] + w_ref[:, span] * eba_ref[0:slots, span]
        for c in range(chunks):
            span = pl.ds(c * CHUNK, CHUNK)
            u_ref[:, pl.ds(LANES + c * CHUNK, CHUNK)] = (
                image(s_ref, c * CHUNK) - w_ref[:, span] * eba_ref[half : half + slots, span]
            )
        ss = su = uu = uv = ee = eu = ef = uf = blank
        for c in range(chunks):
            span = pl.ds(c * CHUNK, CHUNK)
            x = s_ref[:, pl.ds(LANES + c * CHUNK, CHUNK)]
            y = u_ref[:, pl.ds(LANES + c * CHUNK, CHUNK)]
            z = image(u_ref, c * CHUNK) - w_ref[:, span] * ebb_ref[:, span]
            v_ref[:, span] = z
            left = x - ratio * y
            left_image = y - ratio * z
            ss, su, uu, uv = ss + x * x, su + x * y, uu + y * y, uv + y * z
            ee, eu, ef = ee + left * left, eu + left * y, ef + left * left_image
            uf = uf + (y * left_image + left * z)
        row = jnp.zeros((1, LANES), jnp.float32)
        for n, value in enumerate((ss, su, None, ee, eu, uu, ef, uf, uv)):
            row = jnp.where(lane == n, ratio if value is None else whole(value), row)
        row_ref[...] = row
        red_ref[me_first] = row

        def first_copy(j):
            other = lax.rem(me_first + j, first)
            return pltpu.make_async_remote_copy(
                src_ref=row_ref,
                dst_ref=red_ref.at[me_first],
                send_sem=sendr.at[j],
                recv_sem=recvr.at[me_first],
                device_id=(base + other // strips, other % strips),
                device_id_type=pl.DeviceIdType.MESH,
            )

        def first_arrival(j):
            other = lax.rem(me_first + j, first)
            return pltpu.make_async_remote_copy(
                src_ref=row_ref,
                dst_ref=red_ref.at[other],
                send_sem=sendr.at[j],
                recv_sem=recvr.at[other],
                device_id=(base + other // strips, other % strips),
                device_id_type=pl.DeviceIdType.MESH,
            )

        for j in sorted(range(1, first), key=lambda j: abs(2 * j - first)):
            first_copy(j).start()
        for copy in sentb:
            copy.wait_recv()
        for k in range(slots):
            slab_rims(k)
        for j in range(1, first):
            first_arrival(j).wait_recv()

        if high > 1:
            mine = t // low
            copies2 = []
            for j in range(1, high):
                other = lax.rem(mine + j, high)
                copy = pltpu.make_async_remote_copy(
                    src_ref=red_ref,
                    dst_ref=red2_ref.at[mine],
                    send_sem=sendq.at[j],
                    recv_sem=recvq.at[mine],
                    device_id=(other * low + place_t, s),
                    device_id_type=pl.DeviceIdType.MESH,
                )
                copy.start()
                copies2.append(copy)
            red2_ref[mine] = red_ref[...]
            for j in range(1, high):
                other = lax.rem(mine + j, high)
                pltpu.make_async_remote_copy(
                    src_ref=red_ref,
                    dst_ref=red2_ref.at[other],
                    send_sem=sendq.at[j],
                    recv_sem=recvq.at[other],
                    device_id=(other * low + place_t, s),
                    device_id_type=pl.DeviceIdType.MESH,
                ).wait_recv()
            for copy in copies2:
                copy.wait_send()
            rows = [red2_ref[n] for n in range(high)]
        else:
            rows = [red_ref[...]]

        total = sum(jnp.sum(x, axis=0) for x in rows)
        rr0, sas = total[:, 0:1], total[:, 1:2]
        alpha0 = rr0 / sas
        moved = jnp.zeros((1, LANES), jnp.float32)
        lane3 = lax.broadcasted_iota(jnp.int32, (1, 1, LANES), 2)
        for x in rows:
            delta = jnp.broadcast_to(x[:, :, 2:3], x.shape) - alpha0[None]
            weight = jnp.where(
                (lane3 == 3) | (lane3 == 6), 1.0,
                jnp.where(lane3 == 4, 2.0 * delta, jnp.where(lane3 == 7, delta, delta * delta)),
            )
            moved = moved + jnp.sum(x * weight, axis=0)
        rr1 = jnp.sum(jnp.where((lane >= 3) & (lane <= 5), moved, 0.0), axis=1, keepdims=True)
        rar = jnp.sum(jnp.where((lane >= 6) & (lane <= 8), moved, 0.0), axis=1, keepdims=True)
        beta = rr1 / rr0
        alpha1 = rr1 / (rar - beta * rr1 / alpha0)
        for at, size in spans:
            x = s_ref[:, pl.ds(LANES + at, CHUNK)]
            y = u_ref[:, pl.ds(LANES + at, CHUNK)]
            z = v_ref[:, pl.ds(at, CHUNK)]
            r1 = x - alpha0 * y
            direction = r1 + beta * x
            direction_image = (y - alpha0 * z) + beta * y
            answer = alpha0 * x + alpha1 * direction
            left = r1 - alpha1 * direction_image
            for k in range(slots):
                out_x[0, k, :, pl.ds(at, size)] = answer[k : k + 1, :size]
                out_r[0, k, :, pl.ds(at, size)] = left[k : k + 1, :size]

        for copy in sent1 + sentc + sentb:
            copy.wait_send()
        for j in range(1, first):
            first_copy(j).wait_send()

    f32 = jnp.float32
    any_space = pl.BlockSpec(memory_space=pl.ANY)
    hbm = pl.BlockSpec(memory_space=pltpu.HBM)
    vmem = pl.BlockSpec(memory_space=pltpu.VMEM)
    kf = slots * fields_n
    dma = pltpu.SemaphoreType.DMA
    return pl.pallas_call(
        kernel,
        out_shape=(
            pltpu.VMEM((1, 1, slots, fields_n, levels, cells), f32),
            pltpu.VMEM((1, slots, 1, cells), f32),
            pltpu.VMEM((1, slots, 1, cells), f32),
        ),
        in_specs=[hbm] * 7,
        out_specs=(vmem, vmem, vmem),
        scratch_shapes=[
            pltpu.SMEM((slots, 4, 4), jnp.int32),
            pltpu.SMEM((fields_n, levels), f32),
            pltpu.SMEM((levels,), f32),
            pltpu.SMEM((levels,), f32),
            pltpu.VMEM((slots, fields_n, levels, cells), f32),
            pltpu.VMEM((slots, 1, cells), jnp.int32),
            pltpu.VMEM((slots, 1, cells), f32),
            pltpu.VMEM((kf, levels, padded), f32),
            pltpu.VMEM((slots, wide), f32),
            pltpu.VMEM((slots, wide), f32),
            pltpu.VMEM((1, wide), f32),
            pltpu.VMEM((1, wide), f32),
            pltpu.VMEM((2 * half, padded), f32),
            pltpu.VMEM((slots, padded), f32),
            pltpu.VMEM((slots, padded), f32),
            pltpu.VMEM((slots, wide), f32),
            pltpu.VMEM((2 * half, wide), f32),
            pltpu.VMEM((slots, wide), f32),
            pltpu.VMEM((levels, wide), f32),
            pltpu.VMEM((4, 4, slots, LANES), f32),
            pltpu.VMEM((4, 2 * half, LANES), f32),
            pltpu.VMEM((4, slots, LANES), f32),
            pltpu.VMEM((4, fields_n, levels, LANES), f32),
            pltpu.VMEM((4, slots, 4, LANES), f32),
            pltpu.VMEM((n_dirs, 4, slots, 4, LANES), f32),
            pltpu.VMEM((4, kf, levels, LANES), f32),
            pltpu.VMEM((n_dirs, 4, kf, levels, LANES), f32),
            pltpu.VMEM((4, LANES), f32),
            pltpu.VMEM((n_far_even, 4, LANES), f32),
            pltpu.VMEM((1, LANES), f32),
            pltpu.VMEM((first, 1, LANES), f32),
            pltpu.VMEM((high, first, 1, LANES) if high > 1 else (1, 1, 1, LANES), f32),
            dma((6 + slots,)),
            dma((n_dirs,)), dma((n_dirs,)), dma((n_dirs,)), dma((n_dirs,)),
            dma((n_far,)), dma((n_far,)),
            dma((first,)), dma((first,)), dma((high,)), dma((high,)),
        ],
        compiler_params=pltpu.CompilerParams(
            collective_id=0, has_side_effects=True, vmem_limit_bytes=58 << 20
        ),
    )


def put(*arrays):
    def kernel(*refs):
        count = len(arrays)
        sems = refs[-1]
        copies = [pltpu.make_async_copy(refs[n], refs[count + n], sems.at[n]) for n in range(count)]
        for copy in copies:
            copy.start()
        for copy in copies:
            copy.wait()

    return pl.pallas_call(
        kernel,
        out_shape=tuple(jax.ShapeDtypeStruct(x.shape, x.dtype) for x in arrays),
        in_specs=[pl.BlockSpec(memory_space=pl.ANY)] * len(arrays),
        out_specs=tuple(pl.BlockSpec(memory_space=pltpu.HBM) for _ in arrays),
        scratch_shapes=[pltpu.SemaphoreType.DMA((len(arrays),))],
        compiler_params=pltpu.CompilerParams(vmem_limit_bytes=1 << 20),
    )(*arrays)


def solution(mesh):
    tiles, strips = mesh.shape["tiles"], mesh.shape["strip"]

    def on_device(fields, wet_land, links, surface_diagonal, spread, mixing, thickness):
        slots, fields_n, levels, cells = fields.shape[2:]
        call = build(tiles, strips, slots, fields_n, levels, cells)
        wet_land, surface_diagonal = (jnp.swapaxes(x, 1, 2) for x in (wet_land, surface_diagonal))
        new, answer, left = call(fields, wet_land, links, surface_diagonal, spread, mixing, thickness)
        new, answer, left = put(new, answer, left)
        return new, jnp.swapaxes(answer, 1, 2), jnp.swapaxes(left, 1, 2)

    placed = (
        P("tiles", "strip", None, None, None, None),
        P("tiles", "strip", None, None),
        P("tiles", "strip", None, None, None),
        P("tiles", "strip", None, None),
        P(),
        P(),
        P(),
    )
    return jax.shard_map(
        on_device,
        mesh=mesh,
        in_specs=placed,
        out_specs=(
            P("tiles", "strip", None, None, None, None),
            P("tiles", "strip", None, None),
            P("tiles", "strip", None, None),
        ),
        check_vma=False,
    )
```

```python
import math

import jax
import jax.numpy as jnp
from jax import lax
from jax.experimental import pallas as pl
from jax.experimental.pallas import tpu as pltpu
from jax.sharding import PartitionSpec as P

LANES = 128
CHUNK = 1024
POS = (0, 3, 1, 2)
GROUP = 16


def offsets(size):
    return (-1, 0, 1) if size >= 3 else tuple(range(size))


def place(offset, size):
    if size >= 3:
        return offset + 1
    return offset * offset if size == 2 else 0 * offset


def roll(value, shift, axis=1):
    size = value.shape[axis]
    shift = shift % size
    return pltpu.roll(value, shift, axis) if shift else value


def window(size):
    return (-3, 3) if size >= 7 else (0, size - 1)


def slot_of(offset, size):
    return offset + 3 if size >= 7 else offset % size


def build(tiles, strips, slots, fields_n, levels, cells):
    width = math.isqrt(cells)
    n_tiles = -(-cells // CHUNK) * CHUNK // LANES
    wide = n_tiles * LANES
    padded = wide + 2 * LANES
    chunks = wide // CHUNK
    steps_t, steps_s = offsets(tiles), offsets(strips)
    n_s = len(steps_s)
    n_dirs = len(steps_t) * n_s
    low = min(GROUP, tiles)
    high = tiles // low
    first = low * strips
    half = 4
    span_t = window(tiles)
    span_s = window(strips)
    far_t = span_t[1] - span_t[0] + 1
    far_s = span_s[1] - span_s[0] + 1
    n_far = far_t * far_s
    n_far_even = n_far + n_far % 2
    directions = []
    for dt in steps_t:
        for ds in steps_s:
            if dt == 0 and ds == 0:
                continue
            sides = []
            if dt == -1 or (tiles == 2 and dt):
                sides.append(0)
            if ds == -1 or (strips == 2 and ds):
                sides.append(1)
            if ds == 1:
                sides.append(2)
            if dt == 1:
                sides.append(3)
            here = place(dt, tiles) * n_s + place(ds, strips)
            back = place(-dt if tiles >= 3 else dt, tiles) * n_s + place(-ds if strips >= 3 else ds, strips)
            directions.append((dt, ds, here, back, min(sides), max(sides) + 1))
    directions.sort(key=lambda d: -abs(d[0]) - abs(d[1]))
    self_far = slot_of(0, tiles) * far_s + slot_of(0, strips)
    beside_me = {slot_of(d[0], tiles) * far_s + slot_of(d[1], strips) for d in directions}
    around = []
    for dt in range(span_t[0], span_t[1] + 1):
        for ds in range(span_s[0], span_s[1] + 1):
            here = slot_of(dt, tiles) * far_s + slot_of(ds, strips)
            if here != self_far and here not in beside_me:
                around.append((dt, ds))
    around.sort(key=lambda a: -abs(a[0]))
    bits = first.bit_length() - 1
    paired = first == 1 << bits

    def hops(j):
        upper = j >> max(bits - 2, 0) if bits > 2 else j
        return upper + bin(j % (1 << max(bits - 2, 0))).count("1")

    relay = strips == 2 and high == 1 and tiles % 4 == 0 and tiles >= 12
    edge = 3
    relays = (tiles // 2 + 1, tiles // 2 + 3)
    centre = tiles // 2 - 1
    peer_order = sorted(range(1, first), key=lambda j: (-hops(j), -j))

    def reach(steps):
        if tiles < 7:
            return list(range(n_far))
        return [n for n in range(n_far) if abs(n // far_s - 3) <= steps]

    def kernel(
        fields, wet_in, links_in, diag_in, spread_in, mixing_in, thick_in, out_f, out_x, out_r,
        links, spread, mixing, thick, fbuf, wbuf, dbuf, m_ref, w_ref, d_ref, nw_ref, ne_ref, uv_ref, s_ref, u_ref, v_ref, eba_ref, ebr_ref, ebs_ref,
        got_ref, rima_ref, rims_ref, pack1, near1, packb, nearb, cpack, cnear, relay_rim, relay_c, row_ref, red_ref, red2_ref,
        in_sem, send1, recv1, sendb, recvb, sendc, recvc, sendm, recvm, sendf, far_sem, sendr, recvr, sendq, recvq,
    ):
        t = lax.axis_index("tiles")
        s = lax.axis_index("strip")
        copies = [
            pltpu.make_async_copy(wet_in.at[0], wbuf, in_sem.at[0]),
            pltpu.make_async_copy(diag_in.at[0], dbuf, in_sem.at[1]),
        ] + [pltpu.make_async_copy(fields.at[0, 0, k], fbuf.at[k], in_sem.at[2 + k]) for k in range(slots)]
        small = [
            pltpu.make_async_copy(thick_in, thick, in_sem.at[2 + slots]),
            pltpu.make_async_copy(mixing_in, mixing, in_sem.at[3 + slots]),
            pltpu.make_async_copy(spread_in, spread, in_sem.at[4 + slots]),
            pltpu.make_async_copy(links_in.at[0, 0], links, in_sem.at[5 + slots]),
        ]
        for copy in copies[:3] + small + copies[3:]:
            copy.start()

        barrier = pltpu.get_barrier_semaphore()
        base = (t // low) * low
        place_t = t % low
        me_first = place_t * strips + s
        deltas = [(1 << b) * (1 - 2 * ((me_first // (1 << b)) % 2)) for b in range(bits)]

        def peer(j):
            if not paired:
                return lax.rem(me_first + j, first)
            return me_first + sum(deltas[b] for b in range(bits) if j >> b & 1)

        early = t < edge
        peers = 0

        def greet(tx, sx):
            pl.semaphore_signal(barrier, inc=1, device_id=(tx, sx), device_id_type=pl.DeviceIdType.MESH)

        def greet_if(wanted, *targets):
            @pl.when(wanted)
            def _():
                for tx, sx in targets:
                    greet(tx, sx)

        if relay:
            other_s = 1 - s
            greet_if(t >= tiles - edge, (relays[0], s), (relays[0], other_s))
            greet_if(t == tiles - 1, (relays[1], s), (relays[1], other_s))
            greet_if(t == relays[0], (0, s))
            greet_if(t == relays[1], (1, s), (2, s))
            for dt in (-1, -2, -3):
                tx = lax.rem(t + dt + tiles, tiles)
                greet(tx, s)
                greet(tx, other_s)
            greet(t, other_s)
            for dt in (1, 2, 3):
                greet_if(t + dt < tiles, (t + dt, s), (t + dt, other_s))
            greet_if((t < centre - edge) | (t > centre + edge), (centre, 0))
            peers = 4 * edge + 1
            peers = peers + jnp.where(t == relays[0], 2 * edge, jnp.where(t == relays[1], 2, 0))
            peers = jnp.where(early, 2 * (t + edge + 1), peers)
            peers = jnp.where((t == centre) & (s == 0), first - 1, peers)
        for j in () if relay else peer_order:
            other = peer(j)
            pl.semaphore_signal(
                barrier, inc=1, device_id=(base + other // strips, other % strips),
                device_id_type=pl.DeviceIdType.MESH,
            )
            peers += 1
        for j in range(1, high):
            other = lax.rem(t // low + j, high)
            pl.semaphore_signal(
                barrier, inc=1, device_id=(other * low + place_t, s), device_id_type=pl.DeviceIdType.MESH
            )
            peers += 1
        if high > 1:
            for dt, ds in around + [d[:2] for d in directions]:
                pl.semaphore_signal(
                    barrier, inc=1,
                    device_id=(lax.rem(t + dt + tiles, tiles), lax.rem(s + ds + strips, strips)),
                    device_id_type=pl.DeviceIdType.MESH,
                )
                peers += 1

        def exchange(pack, near, send_sem, recv_sem, wanted):
            out = []
            for dt, ds, here, back, lo, hi in directions:
                copy = pltpu.make_async_remote_copy(
                    src_ref=pack.at[pl.ds(lo, hi - lo)],
                    dst_ref=near.at[back, pl.ds(lo, hi - lo)],
                    send_sem=send_sem.at[here],
                    recv_sem=recv_sem.at[back],
                    device_id=(lax.rem(t + dt + tiles, tiles), lax.rem(s + ds + strips, strips)),
                    device_id_type=pl.DeviceIdType.MESH,
                )
                if wanted is None:
                    copy.start()
                out.append(copy)
            if wanted is not None:
                @pl.when(wanted)
                def _():
                    for copy in out:
                        copy.start()
            return out

        lane = lax.broadcasted_iota(jnp.int32, (1, LANES), 1)
        flip_at = jnp.where(lane < width, width - 1 - lane, lane)

        def flip(value):
            rows = value.shape[0]
            if rows < 8:
                value = jnp.concatenate([value, jnp.zeros((8 - rows, LANES), jnp.float32)], 0)
            at = jnp.broadcast_to(flip_at, value.shape)
            return jnp.take_along_axis(value, at, axis=1)[:rows]

        outward = 2 * (t // (tiles // 2)) - 1 if tiles >= 7 and tiles % 2 == 0 else 1

        def to(dt, ds):
            return lax.rem(t + dt + tiles, tiles), lax.rem(s + ds + strips, strips)

        def start(copy, dt):
            if not relay:
                copy.start()
            else:
                pl.when(t + dt >= 0)(copy.start)

        def sent(pair):
            if not relay:
                pair[0].wait_send()
            else:
                pl.when(t + pair[1] >= 0)(pair[0].wait_send)

        def send_rim(dt, ds, lo, count):
            copy = pltpu.make_async_remote_copy(
                src_ref=pack1.at[pl.ds(lo, count)],
                dst_ref=near1.at[place(-dt if tiles >= 3 else dt, tiles) * n_s + place(-ds if strips >= 3 else ds, strips), pl.ds(lo, count)],
                send_sem=send1.at[place(dt, tiles) * n_s + place(ds, strips)],
                recv_sem=recv1.at[place(-dt if tiles >= 3 else dt, tiles) * n_s + place(-ds if strips >= 3 else ds, strips)],
                device_id=to(dt, ds),
                device_id_type=pl.DeviceIdType.MESH,
            )
            start(copy, dt)
            return copy, dt

        def send_corners(dt, ds):
            if tiles >= 7:
                here, back = (dt + 3) * far_s, (3 - dt) * far_s
            else:
                here, back = slot_of(dt, tiles) * far_s, slot_of(-dt, tiles) * far_s
            here, back = here + slot_of(ds, strips), back + slot_of(-ds, strips)
            copy = pltpu.make_async_remote_copy(
                src_ref=cpack,
                dst_ref=cnear.at[back],
                send_sem=sendc.at[here],
                recv_sem=recvc.at[back],
                device_id=to(dt, ds),
                device_id_type=pl.DeviceIdType.MESH,
            )
            start(copy, dt)
            return copy, dt

        def by_relay(index):
            if index == 0:
                pair = (pack1.at[pl.ds(0, 3)], relay_rim)
            else:
                pair = (cpack, relay_c.at[index - 1])
            return pltpu.make_async_remote_copy(
                src_ref=pair[0], dst_ref=pair[1], send_sem=sendm.at[index], recv_sem=recvm.at[index],
                device_id=(relays[0] if index < 2 else relays[1], s), device_id_type=pl.DeviceIdType.MESH,
            )

        def forwards(which):
            out = []
            for ds in range(2):
                def onward(src, dst, sem, tx, n):
                    return pltpu.make_async_remote_copy(
                        src_ref=src, dst_ref=dst, send_sem=sendf.at[n], recv_sem=sem,
                        device_id=(tx, lax.rem(s + ds, 2)), device_id_type=pl.DeviceIdType.MESH,
                    )

                if which == 0:
                    at = 2 * n_s + ds
                    count = 3 if ds else 1
                    out.append(onward(
                        relay_rim.at[pl.ds(0, count)], near1.at[at, pl.ds(0, count)], recv1.at[at],
                        tiles - 1, len(out),
                    ))
                for index, tx, dt in ((1, 2, 2), (1, 3, 3)) if which == 0 else ((2, 1, 2), (2, 2, 3), (3, 1, 3)):
                    at = (3 + dt) * far_s + ds
                    out.append(onward(relay_c.at[index - 1], cnear.at[at], recvc.at[at], tiles - tx, len(out)))
            return out

        def relay_on():
            for which in range(2):
                @pl.when(t == relays[which])
                def _():
                    for index in (0, 1) if which == 0 else (2, 3):
                        by_relay(index).wait_recv()
                    for copy in forwards(which):
                        copy.start()

        def relay_end():
            @pl.when(t == 0)
            def _():
                by_relay(0).wait_send()

            for tx in range(edge):
                @pl.when(t == tx)
                def _():
                    by_relay(tx + 1).wait_send()

            for which in range(2):
                @pl.when(t == relays[which])
                def _():
                    for copy in forwards(which):
                        copy.wait_send()

        def send_all():
            rims, corners = [], []
            if relay:
                @pl.when(t == 0)
                def _():
                    by_relay(0).start()

                for tx in range(edge):
                    @pl.when(t == tx)
                    def _():
                        by_relay(tx + 1).start()

            if tiles < 7 or tiles % 2:
                for dt, ds, here, back, lo, hi in directions:
                    rims.append(send_rim(dt, ds, lo, hi - lo))
                for dt, ds in around:
                    corners.append(send_corners(dt, ds))
                return rims, corners
            for sign in (1, -1):
                way = outward * sign
                right = (way + 1) // 2
                for dt, ds in around:
                    if dt > 0:
                        corners.append(send_corners(way * dt, ds))
                    elif dt == 0 and sign < 0:
                        corners.append(send_corners(dt, ds))
                for ds in sorted(steps_s, key=lambda d: -abs(d)):
                    rims.append(send_rim(way, ds, right if ds else 3 * right, 3 if ds else 1))
                if sign < 0:
                    for dt, ds, here, back, lo, hi in directions:
                        if dt == 0:
                            rims.append(send_rim(dt, ds, lo, hi - lo))
            return rims, corners

        def pick(value, at):
            rows = value.shape[0]
            if rows < 8:
                value = jnp.concatenate([value, jnp.zeros((8 - rows, LANES), jnp.float32)], 0)
            return jnp.take_along_axis(value, jnp.broadcast_to(at, value.shape), axis=1)

        def extract(tile, rows, depth):
            blank = jnp.zeros((rows, LANES), jnp.float32)
            period = 2 * depth
            parts = [blank] * period
            loaded = {}

            def at(n):
                if n not in loaded:
                    loaded[n] = tile(n)
                return loaded[n]

            for i in range(-1, width):
                pe = width * i + width - 1
                shift = (i - pe) % LANES
                reach_lo = pe - depth + 1 if i >= 0 else pe + 1
                reach_hi = pe + depth if i + 1 < width else pe
                for n in range(reach_lo // LANES, reach_hi // LANES + 1):
                    lo, hi = max(reach_lo, n * LANES), min(reach_hi, n * LANES + LANES - 1)
                    begin = (i + lo - pe) % LANES
                    mask = ((lane - begin) & (LANES - 1)) <= hi - lo if hi > lo else lane == begin
                    parts[i % period] = jnp.where(mask, roll(at(n), shift), parts[i % period])
            signed = jnp.where(lane >= LANES - depth, lane - LANES + period * LANES, lane)
            rest = signed - period * ((signed * ((1 << 12) // period + 1)) >> 12)

            def gather(offset, turn_by):
                total = parts[(0 + offset) % period]
                for m in range(1, period):
                    total = jnp.where(rest == m, parts[(m + offset) % period], total)
                total = roll(total, turn_by)
                return jnp.where(lane < width, total, 0.0)

            def line(start):
                a, n = start % LANES, start // LANES
                if a == 0:
                    return jnp.where(lane < width, at(n), 0.0)
                head = roll(at(n), -a)
                if a + width <= LANES:
                    return jnp.where(lane < width, head, 0.0)
                tail = roll(at(n + 1), -a)
                return jnp.where(lane < LANES - a, head, jnp.where(lane < width, tail, 0.0))

            west = [gather(-d - 1, -d) for d in range(depth)]
            east = [gather(d, d) for d in range(depth)]
            south = [line(width * d) for d in range(depth)]
            north = [line(width * (width - 1 - d)) for d in range(depth)]
            return west, east, south, north

        def insert(west, east, south, north, store):
            even = (lane & 1) == 0
            mixed = (jnp.where(even, east, west), jnp.where(even, west, east))
            tiles_of = {}

            def add(n, mask, value):
                tiles_of.setdefault(n, []).append((mask, value))

            for i in range(-1, width):
                pe = width * i + width - 1
                pw = pe + 1
                turned = roll(mixed[i % 2], (pe - i) % LANES)
                if i >= 0 and i + 1 < width and pe // LANES == pw // LANES:
                    mask = (lane == pe % LANES) | (lane == pw % LANES)
                    add(pe // LANES, mask, turned)
                else:
                    if i >= 0:
                        add(pe // LANES, lane == pe % LANES, turned)
                    if i + 1 < width:
                        add(pw // LANES, lane == pw % LANES, turned)
            extra = {}
            for start, rim in ((0, south), (width * (width - 1), north)):
                a, n = start % LANES, start // LANES
                turned = roll(rim, a)
                extra.setdefault(n, []).append(jnp.where(lane >= a, turned, 0.0) if a else turned)
                if a + width > LANES:
                    extra.setdefault(n + 1, []).append(jnp.where(lane < a + width - LANES, turned, 0.0))
            blank = jnp.zeros(west.shape, jnp.float32)
            for n in range(n_tiles):
                total = blank
                for mask, value in tiles_of.get(n, ()):
                    total = jnp.where(mask, value, total)
                for value in extra.get(n, ()):
                    total = total + value
                store(n, total)

        shift_bits = 22
        factor = (1 << shift_bits) // width + 1
        for c in range(chunks):
            index = lax.broadcasted_iota(jnp.int32, (1, CHUNK), 1) + c * CHUNK
            column = index - width * ((index * factor) >> shift_bits)
            nw_ref[:, pl.ds(c * CHUNK, CHUNK)] = jnp.where(column == 0, 0.0, 1.0)
            ne_ref[:, pl.ds(c * CHUNK, CHUNK)] = jnp.where(column == width - 1, 0.0, 1.0)
        tail = wide - LANES
        m_ref[:, :, :LANES] = jnp.zeros((slots * fields_n, levels, LANES), jnp.float32)
        m_ref[:, :, tail + LANES :] = jnp.zeros((slots * fields_n, levels, 2 * LANES), jnp.float32)
        uv_ref[:, :LANES] = jnp.zeros((2 * half, LANES), jnp.float32)
        uv_ref[:, tail + LANES :] = jnp.zeros((2 * half, 2 * LANES), jnp.float32)
        for f in range(2):
            for k in range(slots, half):
                uv_ref[f * half + k : f * half + k + 1, :] = jnp.zeros((1, padded), jnp.float32)
        for ref in (s_ref, u_ref):
            ref[:, :LANES] = jnp.zeros((slots, LANES), jnp.float32)
            ref[:, wide + LANES :] = jnp.zeros((slots, LANES), jnp.float32)
        w_ref[:, tail:] = jnp.zeros((slots, LANES), jnp.float32)
        d_ref[:, tail:] = jnp.zeros((slots, LANES), jnp.float32)
        rima_ref[...] = jnp.zeros(rima_ref.shape, jnp.float32)

        def per_level(read):
            level = lax.broadcasted_iota(jnp.int32, (levels, 1), 0)
            value = jnp.zeros((levels, 1), jnp.float32)
            for n in range(levels):
                value = jnp.where(level == n, read(n), value)
            return value

        for copy in small:
            copy.wait()
        thick_col = per_level(lambda n: thick[n])
        mix_col = per_level(lambda n: mixing[n])

        def choose(number, test, yes, no):
            return jnp.where(test(jnp.full(yes.shape, number, jnp.int32)), yes, no)

        sub = lax.broadcasted_iota(jnp.int32, (slots, LANES), 0)
        sub8 = lax.broadcasted_iota(jnp.int32, (8, LANES), 0)
        group, lane32 = lane >> 5, lane & 31
        own_k, own_e, own_n = lane32 >> 3, (lane32 >> 1) & 3, lane32 & 1

        def code_rows(e):
            value = jnp.zeros((slots, LANES), jnp.int32)
            for k in range(slots):
                value = jnp.where(sub == k, jnp.full(value.shape, links[k, e, 3], jnp.int32), value)
            return value

        codes = [code_rows(e) for e in range(4)]

        def turn(code):
            a = jnp.where(code == 0, 1.0, jnp.where(code == 2, -1.0, 0.0))
            b = jnp.where(code == 1, 1.0, jnp.where(code == 3, -1.0, 0.0))
            return a, b

        own_links = []
        for n in range(4):
            value = jnp.zeros((1, LANES), jnp.int32)
            for k in range(slots):
                for e in range(4):
                    value = jnp.where((lane32 >> 1) == 4 * k + e, jnp.full(value.shape, links[k, e, n], jnp.int32), value)
            own_links.append(value)

        copies[0].wait()
        copies[1].wait()
        spans = [(c * CHUNK, min(CHUNK, cells - c * CHUNK)) for c in range(chunks)]
        for k in range(slots):
            for at, size in spans:
                w_ref[k : k + 1, pl.ds(at, size)] = wbuf[k, :, pl.ds(at, size)].astype(jnp.float32)
                d_ref[k : k + 1, pl.ds(at, size)] = dbuf[k, :, pl.ds(at, size)] + 4.0

        q_rims = extract(
            lambda n: w_ref[:, pl.ds(LANES * n, LANES)] * d_ref[:, pl.ds(LANES * n, LANES)], slots, 2
        )
        w_rims = [[jnp.where(x > 0.0, 1.0, 0.0) for x in side] for side in q_rims]

        def pre_flip(e, value):
            return jnp.where(codes[e] != 0, flip(value), value)

        for e in range(4):
            value = pre_flip(e, q_rims[e][0])
            for k in range(slots):
                pack1[POS[e], k, 3:4, :] = value[k : k + 1]

        link_f = [x.astype(jnp.float32) for x in own_links]
        nothing = jnp.zeros((1, LANES), jnp.float32)
        ends_at = [jnp.where(own_n == 0, m, width - 1 - m) for m in range(2)]
        ends_w = jnp.where(group == 2, ends_at[1], ends_at[0])

        for k in range(slots):
            copies[2 + k].wait()
            for f in range(fields_n):
                for at, size in spans:
                    masked = fbuf[k, f, :, pl.ds(at, size)] * w_ref[k : k + 1, pl.ds(at, size)]
                    m_ref[k * fields_n + f, :, pl.ds(LANES + at, size)] = masked
                    if f < 2:
                        uv_ref[f * half + k : f * half + k + 1, pl.ds(LANES + at, size)] = jnp.sum(
                            masked * thick_col, axis=0, keepdims=True
                        )

        uv_rims = extract(lambda n: uv_ref[:, pl.ds(LANES * (n + 1), LANES)], 2 * half, 3)
        sent_rims, s_local = [], []
        ends_uv = [jnp.zeros((8, LANES), jnp.float32)] * 2
        ends_s = jnp.zeros((8, LANES), jnp.float32)
        for e in range(4):
            us = [x[0:slots] for x in uv_rims[e]]
            vs = [x[half : half + slots] for x in uv_rims[e]]
            normal, along = (us, vs) if e < 2 else (vs, us)
            sign = 0.5 if e in (0, 2) else -0.5
            w0, w1, q0 = w_rims[e][0], w_rims[e][1], q_rims[e][0]

            def slope(x):
                return 0.5 * (roll(x, -1) - roll(x, 1))

            s0 = w0 * (sign * normal[1] + slope(along[0]))
            s1 = w1 * (sign * (normal[2] - normal[0]) + slope(along[1]))
            u0 = q0 * s0 - w0 * (s1 + (roll(s0, -1) + roll(s0, 1)))
            a, b = turn(codes[e])
            rim = a * us[0] - b * vs[0] if e < 2 else a * vs[0] + b * us[0]
            for r, value in enumerate((rim, s0, u0)):
                value = pre_flip(e, value)
                for k in range(slots):
                    pack1[POS[e], k, r : r + 1, :] = value[k : k + 1]
            sent_rims.append(rim)
            s_local.append(s0)
            mine = own_e == e
            for m in range(2):
                ends_uv[m] = jnp.where(
                    mine & ((sub8 & 3) == own_k) & ((sub8 >> 2) == group), pick(uv_rims[e][0], ends_at[m]), ends_uv[m]
                )
            mine = mine & (sub8 == own_k)
            ends_s = jnp.where(mine & (group == 0), pick(s0, ends_at[0]), ends_s)
            ends_s = jnp.where(mine & ((group == 1) | (group == 2)), pick(w0, ends_w), ends_s)
        ends_uv = [jnp.sum(x, axis=0, keepdims=True) for x in ends_uv]
        cpack[0:1, :] = jnp.where(
            group == 0, link_f[0], jnp.where(group == 1, link_f[1], jnp.where(group == 2, link_f[2], 0.0))
        )
        cpack[1:2, :] = jnp.where(group == 2, link_f[3], ends_uv[0])
        cpack[2:3, :] = jnp.sum(ends_s, axis=0, keepdims=True)
        cpack[3:4, :] = ends_uv[1]
        record = cpack[...]
        for k in range(slots):
            carried = jnp.where(lane >= 96, roll(record, 96 - 32 * k), 0.0)
            for e in range(4):
                pack1[e, k] = pack1[e, k] + carried

        pl.semaphore_wait(barrier, peers)
        sent1, sentc = send_all()
        if relay:
            @pl.when((t == centre) & (s == 0))
            def _():
                for x in range(first):
                    if x != 2 * centre:
                        pl.semaphore_signal(
                            far_sem, inc=1, device_id=(x // 2, x % 2), device_id_type=pl.DeviceIdType.MESH
                        )

        cnear[self_far] = record
        if n_far_even > n_far:
            cnear[n_far] = jnp.zeros((4, LANES), jnp.float32)

        def slab_pack(kf, carry):
            rims = extract(lambda n: m_ref[kf, :, pl.ds(LANES * (n + 1), LANES)], levels, 1)
            for e, rim in enumerate(rims):
                packb[POS[e], kf] = rim[0]
            return carry

        lax.fori_loop(0, slots * fields_n, slab_pack, 0)
        sentb = exchange(packb, nearb, sendb, recvb, t >= edge if relay else None)
        if relay:
            relay_on()

        def entry(k, e):
            dt, ds, p, code = (links[k, e, n] for n in range(4))
            source = place(dt, tiles) * n_s + place(ds, strips)
            return source, jnp.maximum(p, 0), p, code

        inner = slice(LANES, LANES + CHUNK)

        def image(x_ref, at):
            span = pl.ds(at, CHUNK)
            win = x_ref[:, pl.ds(at, CHUNK + 2 * LANES)]
            near = ne_ref[:, span] * roll(win, -1)[:, inner] + nw_ref[:, span] * roll(win, 1)[:, inner]
            near = near + (roll(win, -width)[:, inner] + roll(win, width)[:, inner])
            return w_ref[:, span] * (d_ref[:, span] * win[:, inner] - near)

        def whole(value):
            return jnp.sum(jnp.sum(value, axis=1, keepdims=True), axis=0, keepdims=True)

        for c in range(chunks):
            at = c * CHUNK
            span = pl.ds(at, CHUNK)
            u_win = uv_ref[0:slots, pl.ds(at, CHUNK + 2 * LANES)]
            v_win = uv_ref[half : half + slots, pl.ds(at, CHUNK + 2 * LANES)]
            flux = ne_ref[:, span] * roll(u_win, -1)[:, inner] - nw_ref[:, span] * roll(u_win, 1)[:, inner]
            flux = flux + (roll(v_win, -width)[:, inner] - roll(v_win, width)[:, inner])
            s_ref[:, pl.ds(LANES + at, CHUNK)] = w_ref[:, span] * (0.5 * flux)
        blank = jnp.zeros((slots, CHUNK), jnp.float32)
        ss = su = blank
        for c in range(chunks):
            x = s_ref[:, pl.ds(LANES + c * CHUNK, CHUNK)]
            y = image(s_ref, c * CHUNK)
            ss, su = ss + x * x, su + x * y
        ss, su = whole(ss), whole(su)
        ratio = jnp.where(su > 0.0, ss / su, 0.0)

        def slab_inner(k):
            def one(f, carry):
                spread_col = per_level(lambda n: spread[f, n])
                for at, size in spans:
                    span = pl.ds(at, CHUNK)
                    win = m_ref[k * fields_n + f, :, pl.ds(at, CHUNK + 2 * LANES)]
                    mid = win[:, inner]
                    flat = ne_ref[:, span] * roll(win, -1)[:, inner] + nw_ref[:, span] * roll(win, 1)[:, inner]
                    flat = flat + (roll(win, -width)[:, inner] + roll(win, width)[:, inner])
                    flat = flat - 4.0 * mid
                    above = jnp.concatenate([mid[1:], mid[-1:]], 0)
                    below = jnp.concatenate([mid[:1], mid[:-1]], 0)
                    column = above + below - 2.0 * mid
                    new = w_ref[k : k + 1, span] * (mid + spread_col * flat + mix_col * column)
                    out_f[0, 0, k, f, :, pl.ds(at, size)] = new[:, :size]
                return carry

            lax.fori_loop(0, fields_n, one, 0)

        def slab_rims(k):
            for e in range(4):
                source, slot, p, code = entry(k, e)
                a, b = turn(code)
                got = []
                for f in range(fields_n):
                    rim = nearb[source, POS[e ^ 1], slot * fields_n + f]
                    rim = choose(code, lambda x: x != 0, flip(rim), rim)
                    got.append(choose(p, lambda x: x >= 0, rim, jnp.zeros_like(rim)))
                rims_ref[e, 0] = a * got[0] + b * got[1]
                rims_ref[e, 1] = a * got[1] - b * got[0]
                for f in range(2, fields_n):
                    rims_ref[e, f] = got[f]

            def one(f, carry):
                def store(n, value):
                    ebs_ref[:, pl.ds(n * LANES, LANES)] = value

                insert(rims_ref[0, f], rims_ref[1, f], rims_ref[2, f], rims_ref[3, f], store)
                spread_col = per_level(lambda n: spread[f, n])
                for at, size in spans:
                    wet = w_ref[k : k + 1, pl.ds(at, size)]
                    old = out_f[0, 0, k, f, :, pl.ds(at, size)]
                    out_f[0, 0, k, f, :, pl.ds(at, size)] = old + wet * (spread_col * ebs_ref[:, pl.ds(at, size)])
                return carry

            lax.fori_loop(0, fields_n, one, 0)

        slab_inner(0)
        if relay:
            @pl.when(early)
            def _():
                pl.semaphore_wait(far_sem, 1)
                for copy in sentb:
                    copy.start()

        for copy, _ in sent1:
            copy.wait_recv()
        for e in range(4):
            for k in range(slots):
                source, slot, p, code = entry(k, e)
                got = near1[source, POS[e ^ 1], slot]
                got = choose(p, lambda x: (x >= 0) & (lane < width), got, jnp.zeros_like(got))
                for r in range(4):
                    got_ref[r, e, k : k + 1, :] = got[r : r + 1]
        rho = [(0.5 if e in (1, 3) else -0.5) * got_ref[0, e] for e in range(4)]

        def store_r(n, value):
            ebr_ref[:, pl.ds(n * LANES, LANES)] = value

        insert(rho[0], rho[1], rho[2], rho[3], store_r)
        for c in range(chunks):
            span, shifted = pl.ds(c * CHUNK, CHUNK), pl.ds(LANES + c * CHUNK, CHUNK)
            s_ref[:, shifted] = s_ref[:, shifted] + w_ref[:, span] * ebr_ref[:, span]
        for dt in steps_t:
            for ds in steps_s:
                if dt == 0 and ds == 0:
                    continue
                at_side = 1
                if ds == 0:
                    at_side = 3 if dt == -1 else 0
                elif dt == 0 and strips >= 3:
                    at_side = 1 if ds == 1 else 2
                total = jnp.zeros((4, LANES), jnp.float32)
                for k in range(slots):
                    found = near1[place(dt, tiles) * n_s + place(ds, strips), at_side, k]
                    total = jnp.where(group == k, roll(found, 32 * k - 96), total)
                cnear[slot_of(dt, tiles) * far_s + slot_of(ds, strips)] = total

        for copy, _ in sentc:
            copy.wait_recv()

        def lookup(steps, at, target):
            at = 32 * group + at
            total = jnp.zeros((8, LANES), jnp.float32)
            wanted = target - (sub8 >> 2)
            near = reach(steps)
            for n in range(near[0] - near[0] % 2, near[-1] + 1, 2):
                pair = jnp.concatenate([cnear[n], cnear[n + 1]], 0)
                found = jnp.take_along_axis(pair, jnp.broadcast_to(at, pair.shape), axis=1)
                total = jnp.where(wanted == n, found, total)
            return total + roll(total, 4, 0)

        apart = lane32 + 32 * (sub8 & 3)

        def quantities(found, r):
            value = jnp.take_along_axis(jnp.broadcast_to(found[r : r + 1], (8, LANES)), apart, axis=1)
            return [value[n : n + 1] for n in range(4)]

        def far(dt, ds):
            if tiles >= 7:
                at_t = dt + 3
            else:
                at_t = dt - tiles * jnp.floor(dt * (1.0 / tiles) + 1e-3)
            if strips >= 7:
                at_s = ds + 3
            else:
                at_s = ds - strips * jnp.floor(ds * (1.0 / strips) + 1e-3)
            return at_t * far_s + at_s

        dt1, ds1, p1, c1 = link_f
        one_if = lambda test: jnp.where(test, 1, 0)
        end1 = own_n ^ one_if(c1 != 0.0)
        side_f = jnp.where(own_e < 2, 2, 0) + end1
        end_f = 1 - (own_e & 1)
        lane1 = jnp.maximum(p1, 0.0).astype(jnp.int32) * 8 + side_f * 2 + end_f
        found1 = lookup(1, lane1, far(dt1, ds1).astype(jnp.int32))
        dt2, ds2, p2, _ = quantities(found1, 0)
        u_c, v_c, c2, _ = quantities(found1, 1)
        _, w_c, w_n, _ = quantities(found1, 2)
        side_g = side_f ^ 1
        end2 = end_f ^ one_if(c2 != 0.0)
        side_h = jnp.where(side_g < 2, 2, 0) + end2
        end_h = side_g & 1
        slot2 = jnp.maximum(p2, 0.0).astype(jnp.int32) * 8
        dt12, ds12 = dt1 + dt2, ds1 + ds2
        lane2 = slot2 + side_g * 2 + end2
        lane2h = slot2 + side_h * 2 + end_h
        for_h = ((sub8 & 3) == 0) | (((sub8 & 3) == 1) & (group == 2))
        found2 = lookup(2, jnp.where(for_h, lane2h, lane2), far(dt12, ds12).astype(jnp.int32))
        dt3, ds3, p3, _ = quantities(found2, 0)
        u_g, v_g, c3, _ = quantities(found2, 1)
        s_g, w_g, _, _ = quantities(found2, 2)
        u_g1, v_g1, _, _ = quantities(found2, 3)
        lane3 = jnp.maximum(p3, 0.0).astype(jnp.int32) * 8 + (side_h ^ 1) * 2 + (end_h ^ one_if(c3 != 0.0))
        found3 = lookup(3, lane3, far(dt12 + dt3, ds12 + ds3).astype(jnp.int32))
        u_h, v_h, _, _ = quantities(found3, 1)

        def arriving(a, b, u, v, side):
            value = jnp.where(side < 2, a * u + b * v, a * v - b * u)
            return jnp.where((side & 1) == 0, -0.5, 0.5) * value

        a2, b2 = turn(c2)
        a3, b3 = turn(c3)
        live2 = (p1 >= 0.0) & (p2 >= 0.0)
        first_in = jnp.where(live2, w_c * arriving(a2, b2, u_g, v_g, side_f), 0.0)
        next_in = jnp.where(live2, w_n * arriving(a2, b2, u_g1, v_g1, side_f), 0.0)
        beyond = arriving(a2, -b2, u_c, v_c, side_g)
        beyond = beyond + jnp.where(p3 >= 0.0, arriving(a3, b3, u_h, v_h, side_h), 0.0)
        beyond = jnp.where(live2, s_g + w_g * beyond, 0.0)
        next_in = next_in + beyond
        first_in = jnp.broadcast_to(first_in, (8, LANES))
        next_in = jnp.broadcast_to(next_in, (8, LANES))

        def side_totals(west, east, south, north):
            end = slice(width - 1, width)

            def ends(at_first, at_last):
                return jnp.where(lane == 0, at_first, jnp.where(lane == width - 1, at_last, 0.0))

            return (
                west + ends(south[:, :1], north[:, :1]),
                east + ends(south[:, end], north[:, end]),
                south + ends(west[:, :1], east[:, :1]),
                north + ends(west[:, end], east[:, end]),
            )

        totals = side_totals(*rho)
        at_end = (lane == 0) | (lane == width - 1)
        by_end = (lane == 1) | (lane == width - 2)
        for e in range(4):
            mine = s_local[e] + w_rims[e][0] * totals[e]
            q = got_ref[3, e]
            wet = jnp.where(q > 0.0, 1.0, 0.0)
            delta = wet * ((-0.5 if e in (1, 3) else 0.5) * sent_rims[e])
            at = (sub8 & 3) * 8 + 2 * e + jnp.where(lane >= width // 2, 1, 0)
            at_first = jnp.take_along_axis(first_in, at, axis=1)[:slots]
            at_next = jnp.take_along_axis(next_in, at, axis=1)[:slots]
            delta = delta + jnp.where(at_end, at_first, 0.0)
            there = got_ref[1, e] + delta
            beside = (roll(delta, -1) + roll(delta, 1)) + mine
            beside = beside + jnp.where(at_end, at_next, 0.0)
            image_there = got_ref[2, e] + q * delta - wet * beside
            rima_ref[e, 0:slots, :] = there
            rima_ref[e, half : half + slots, :] = image_there

        def store_a(n, value):
            eba_ref[:, pl.ds(n * LANES, LANES)] = value

        insert(rima_ref[0], rima_ref[1], rima_ref[2], rima_ref[3], store_a)
        for c in range(chunks):
            span = pl.ds(c * CHUNK, CHUNK)
            u_ref[:, pl.ds(LANES + c * CHUNK, CHUNK)] = (
                image(s_ref, c * CHUNK) - w_ref[:, span] * eba_ref[0:slots, span]
            )
        uu = uv = ee = eu = ez = blank
        for c in range(chunks):
            span = pl.ds(c * CHUNK, CHUNK)
            x = s_ref[:, pl.ds(LANES + c * CHUNK, CHUNK)]
            y = u_ref[:, pl.ds(LANES + c * CHUNK, CHUNK)]
            z = image(u_ref, c * CHUNK) - w_ref[:, span] * eba_ref[half : half + slots, span]
            v_ref[:, span] = z
            left = x - ratio * y
            uu, uv = uu + y * y, uv + y * z
            ee, eu, ez = ee + left * left, eu + left * y, ez + left * z
        uu, uv, ee, eu, ez = (whole(x) for x in (uu, uv, ee, eu, ez))
        su = eu + ratio * uu
        ss = ee + ratio * (eu + su)
        ef = eu - ratio * ez
        uf = uu - ratio * uv + ez
        row = jnp.zeros((1, LANES), jnp.float32)
        for n, value in enumerate((ss, su, None, ee, eu, uu, ef, uf, uv)):
            row = jnp.where(lane == n, ratio if value is None else value, row)
        row_ref[...] = row
        red_ref[me_first] = row

        def first_copy(j):
            other = peer(j)
            return pltpu.make_async_remote_copy(
                src_ref=row_ref,
                dst_ref=red_ref.at[me_first],
                send_sem=sendr.at[j],
                recv_sem=recvr.at[me_first],
                device_id=(base + other // strips, other % strips),
                device_id_type=pl.DeviceIdType.MESH,
            )

        def first_arrival(j):
            other = peer(j)
            return pltpu.make_async_remote_copy(
                src_ref=row_ref,
                dst_ref=red_ref.at[other],
                send_sem=sendr.at[j],
                recv_sem=recvr.at[other],
                device_id=(base + other // strips, other % strips),
                device_id_type=pl.DeviceIdType.MESH,
            )

        if relay:
            @pl.when((t >= edge) & ((t != centre) | (s != 0)))
            def _():
                pl.semaphore_wait(far_sem, 1)

        for j in peer_order:
            first_copy(j).start()
        for k in range(1, slots):
            slab_inner(k)

        for copy in sentb:
            copy.wait_recv()
        for k in range(slots):
            slab_rims(k)
        for j in range(1, first):
            first_arrival(j).wait_recv()

        if high > 1:
            mine = t // low
            copies2 = []
            for j in range(1, high):
                other = lax.rem(mine + j, high)
                copy = pltpu.make_async_remote_copy(
                    src_ref=red_ref,
                    dst_ref=red2_ref.at[mine],
                    send_sem=sendq.at[j],
                    recv_sem=recvq.at[mine],
                    device_id=(other * low + place_t, s),
                    device_id_type=pl.DeviceIdType.MESH,
                )
                copy.start()
                copies2.append(copy)
            red2_ref[mine] = red_ref[...]
            for j in range(1, high):
                other = lax.rem(mine + j, high)
                pltpu.make_async_remote_copy(
                    src_ref=red_ref,
                    dst_ref=red2_ref.at[other],
                    send_sem=sendq.at[j],
                    recv_sem=recvq.at[other],
                    device_id=(other * low + place_t, s),
                    device_id_type=pl.DeviceIdType.MESH,
                ).wait_recv()
            for copy in copies2:
                copy.wait_send()
            rows = [red2_ref[n] for n in range(high)]
        else:
            rows = [red_ref[...]]

        total = sum(jnp.sum(x, axis=0) for x in rows)
        rr0, sas = total[:, 0:1], total[:, 1:2]
        alpha0 = rr0 / sas
        moved = jnp.zeros((1, LANES), jnp.float32)
        lane3 = lax.broadcasted_iota(jnp.int32, (1, 1, LANES), 2)
        for x in rows:
            delta = jnp.broadcast_to(x[:, :, 2:3], x.shape) - alpha0[None]
            weight = jnp.where(
                (lane3 == 3) | (lane3 == 6), 1.0,
                jnp.where(lane3 == 4, 2.0 * delta, jnp.where(lane3 == 7, delta, delta * delta)),
            )
            moved = moved + jnp.sum(x * weight, axis=0)
        rr1 = jnp.sum(jnp.where((lane >= 3) & (lane <= 5), moved, 0.0), axis=1, keepdims=True)
        rar = jnp.sum(jnp.where((lane >= 6) & (lane <= 8), moved, 0.0), axis=1, keepdims=True)
        beta = rr1 / rr0
        alpha1 = rr1 / (rar - beta * rr1 / alpha0)
        for at, size in spans:
            x = s_ref[:, pl.ds(LANES + at, CHUNK)]
            y = u_ref[:, pl.ds(LANES + at, CHUNK)]
            z = v_ref[:, pl.ds(at, CHUNK)]
            r1 = x - alpha0 * y
            direction = r1 + beta * x
            direction_image = (y - alpha0 * z) + beta * y
            answer = alpha0 * x + alpha1 * direction
            left = r1 - alpha1 * direction_image
            for k in range(slots):
                out_x[0, k, :, pl.ds(at, size)] = answer[k : k + 1, :size]
                out_r[0, k, :, pl.ds(at, size)] = left[k : k + 1, :size]

        for pair in sent1 + sentc:
            sent(pair)
        if relay:
            relay_end()
        for copy in sentb:
            copy.wait_send()
        for j in range(1, first):
            first_copy(j).wait_send()

    f32 = jnp.float32
    any_space = pl.BlockSpec(memory_space=pl.ANY)
    hbm = pl.BlockSpec(memory_space=pltpu.HBM)
    vmem = pl.BlockSpec(memory_space=pltpu.VMEM)
    kf = slots * fields_n
    dma = pltpu.SemaphoreType.DMA
    return pl.pallas_call(
        kernel,
        out_shape=(
            pltpu.VMEM((1, 1, slots, fields_n, levels, cells), f32),
            pltpu.VMEM((1, slots, 1, cells), f32),
            pltpu.VMEM((1, slots, 1, cells), f32),
        ),
        in_specs=[hbm] * 7,
        out_specs=(vmem, vmem, vmem),
        scratch_shapes=[
            pltpu.SMEM((slots, 4, 4), jnp.int32),
            pltpu.SMEM((fields_n, levels), f32),
            pltpu.SMEM((levels,), f32),
            pltpu.SMEM((levels,), f32),
            pltpu.VMEM((slots, fields_n, levels, cells), f32),
            pltpu.VMEM((slots, 1, cells), jnp.int32),
            pltpu.VMEM((slots, 1, cells), f32),
            pltpu.VMEM((kf, levels, padded), f32),
            pltpu.VMEM((slots, wide), f32),
            pltpu.VMEM((slots, wide), f32),
            pltpu.VMEM((1, wide), f32),
            pltpu.VMEM((1, wide), f32),
            pltpu.VMEM((2 * half, padded), f32),
            pltpu.VMEM((slots, padded), f32),
            pltpu.VMEM((slots, padded), f32),
            pltpu.VMEM((slots, wide), f32),
            pltpu.VMEM((2 * half, wide), f32),
            pltpu.VMEM((slots, wide), f32),
            pltpu.VMEM((levels, wide), f32),
            pltpu.VMEM((4, 4, slots, LANES), f32),
            pltpu.VMEM((4, 2 * half, LANES), f32),
            pltpu.VMEM((4, fields_n, levels, LANES), f32),
            pltpu.VMEM((4, slots, 4, LANES), f32),
            pltpu.VMEM((n_dirs, 4, slots, 4, LANES), f32),
            pltpu.VMEM((4, kf, levels, LANES), f32),
            pltpu.VMEM((n_dirs, 4, kf, levels, LANES), f32),
            pltpu.VMEM((4, LANES), f32),
            pltpu.VMEM((n_far_even, 4, LANES), f32),
            pltpu.VMEM((3, slots, 4, LANES), f32),
            pltpu.VMEM((3, 4, LANES), f32),
            pltpu.VMEM((1, LANES), f32),
            pltpu.VMEM((first, 1, LANES), f32),
            pltpu.VMEM((high, first, 1, LANES) if high > 1 else (1, 1, 1, LANES), f32),
            dma((6 + slots,)),
            dma((n_dirs,)), dma((n_dirs,)), dma((n_dirs,)), dma((n_dirs,)),
            dma((n_far,)), dma((n_far,)), dma((4,)), dma((4,)), dma((8,)), pltpu.SemaphoreType.REGULAR,
            dma((first,)), dma((first,)), dma((high,)), dma((high,)),
        ],
        compiler_params=pltpu.CompilerParams(
            collective_id=0, has_side_effects=True, vmem_limit_bytes=58 << 20
        ),
    )


def put(*arrays):
    def kernel(*refs):
        count = len(arrays)
        sems = refs[-1]
        copies = [pltpu.make_async_copy(refs[n], refs[count + n], sems.at[n]) for n in range(count)]
        for copy in copies:
            copy.start()
        for copy in copies:
            copy.wait()

    return pl.pallas_call(
        kernel,
        out_shape=tuple(jax.ShapeDtypeStruct(x.shape, x.dtype) for x in arrays),
        in_specs=[pl.BlockSpec(memory_space=pl.ANY)] * len(arrays),
        out_specs=tuple(pl.BlockSpec(memory_space=pltpu.HBM) for _ in arrays),
        scratch_shapes=[pltpu.SemaphoreType.DMA((len(arrays),))],
        compiler_params=pltpu.CompilerParams(vmem_limit_bytes=1 << 20),
    )(*arrays)


def solution(mesh):
    tiles, strips = mesh.shape["tiles"], mesh.shape["strip"]

    def on_device(fields, wet_land, links, surface_diagonal, spread, mixing, thickness):
        slots, fields_n, levels, cells = fields.shape[2:]
        call = build(tiles, strips, slots, fields_n, levels, cells)
        wet_land, surface_diagonal = (jnp.swapaxes(x, 1, 2) for x in (wet_land, surface_diagonal))
        new, answer, left = call(fields, wet_land, links, surface_diagonal, spread, mixing, thickness)
        new, answer, left = put(new, answer, left)
        return new, jnp.swapaxes(answer, 1, 2), jnp.swapaxes(left, 1, 2)

    placed = (
        P("tiles", "strip", None, None, None, None),
        P("tiles", "strip", None, None),
        P("tiles", "strip", None, None, None),
        P("tiles", "strip", None, None),
        P(),
        P(),
        P(),
    )
    return jax.shard_map(
        on_device,
        mesh=mesh,
        in_specs=placed,
        out_specs=(
            P("tiles", "strip", None, None, None, None),
            P("tiles", "strip", None, None),
            P("tiles", "strip", None, None),
        ),
        check_vma=False,
    )
```

```python
import math

import jax
import jax.numpy as jnp
from jax import lax
from jax.experimental import pallas as pl
from jax.experimental.pallas import tpu as pltpu
from jax.sharding import PartitionSpec as P

LANES = 128
CHUNK = 1024
POS = (0, 3, 1, 2)
GROUP = 16


def offsets(size):
    return (-1, 0, 1) if size >= 3 else tuple(range(size))


def place(offset, size):
    if size >= 3:
        return offset + 1
    return offset * offset if size == 2 else 0 * offset


def roll(value, shift, axis=1):
    size = value.shape[axis]
    shift = shift % size
    return pltpu.roll(value, shift, axis) if shift else value


def window(size):
    return (-3, 3) if size >= 7 else (0, size - 1)


def slot_of(offset, size):
    return offset + 3 if size >= 7 else offset % size


def build(tiles, strips, slots, fields_n, levels, cells):
    width = math.isqrt(cells)
    n_tiles = -(-cells // CHUNK) * CHUNK // LANES
    wide = n_tiles * LANES
    padded = wide + 2 * LANES
    chunks = wide // CHUNK
    steps_t, steps_s = offsets(tiles), offsets(strips)
    n_s = len(steps_s)
    n_dirs = len(steps_t) * n_s
    low = min(GROUP, tiles)
    high = tiles // low
    first = low * strips
    half = 4
    span_t = window(tiles)
    span_s = window(strips)
    far_t = span_t[1] - span_t[0] + 1
    far_s = span_s[1] - span_s[0] + 1
    n_far = far_t * far_s
    n_far_even = n_far + n_far % 2
    directions = []
    for dt in steps_t:
        for ds in steps_s:
            if dt == 0 and ds == 0:
                continue
            sides = []
            if dt == -1 or (tiles == 2 and dt):
                sides.append(0)
            if ds == -1 or (strips == 2 and ds):
                sides.append(1)
            if ds == 1:
                sides.append(2)
            if dt == 1:
                sides.append(3)
            here = place(dt, tiles) * n_s + place(ds, strips)
            back = place(-dt if tiles >= 3 else dt, tiles) * n_s + place(-ds if strips >= 3 else ds, strips)
            directions.append((dt, ds, here, back, min(sides), max(sides) + 1))
    directions.sort(key=lambda d: -abs(d[0]) - abs(d[1]))
    self_far = slot_of(0, tiles) * far_s + slot_of(0, strips)
    beside_me = {slot_of(d[0], tiles) * far_s + slot_of(d[1], strips) for d in directions}
    around = []
    for dt in range(span_t[0], span_t[1] + 1):
        for ds in range(span_s[0], span_s[1] + 1):
            here = slot_of(dt, tiles) * far_s + slot_of(ds, strips)
            if here != self_far and here not in beside_me:
                around.append((dt, ds))
    around.sort(key=lambda a: -abs(a[0]))
    bits = first.bit_length() - 1
    paired = first == 1 << bits

    def hops(j):
        upper = j >> max(bits - 2, 0) if bits > 2 else j
        return upper + bin(j % (1 << max(bits - 2, 0))).count("1")

    relay = strips == 2 and high == 1 and tiles % 4 == 0 and tiles >= 12
    edge = 3
    relays = (tiles // 2 + 1, tiles // 2 + 3)
    centre = tiles // 2 - 1
    peer_order = sorted(range(1, first), key=lambda j: (-hops(j), -j))

    def reach(steps):
        if tiles < 7:
            return list(range(n_far))
        return [n for n in range(n_far) if abs(n // far_s - 3) <= steps]

    def kernel(
        fields, wet_in, links_in, diag_in, spread_in, mixing_in, thick_in, out_f, out_x, out_r,
        links, spread, mixing, thick, fbuf, wbuf, dbuf, m_ref, w_ref, d_ref, nw_ref, ne_ref, uv_ref, s_ref, u_ref, v_ref, eba_ref, ebr_ref, ebs_ref,
        got_ref, rima_ref, rims_ref, pack1, near1, packb, nearb, cpack, cnear, relay_rim, relay_c, row_ref, red_ref, red2_ref,
        in_sem, send1, recv1, sendb, recvb, sendc, recvc, sendm, recvm, sendf, far_sem, sendr, recvr, sendq, recvq,
    ):
        t = lax.axis_index("tiles")
        s = lax.axis_index("strip")
        copies = [
            pltpu.make_async_copy(wet_in.at[0], wbuf, in_sem.at[0]),
            pltpu.make_async_copy(diag_in.at[0], dbuf, in_sem.at[1]),
        ] + [
            pltpu.make_async_copy(fields.at[0, 0, k, pl.ds(0, 2)], fbuf.at[k, pl.ds(0, 2)], in_sem.at[2 + k])
            for k in range(slots)
        ]
        later = [
            pltpu.make_async_copy(
                fields.at[0, 0, k, pl.ds(2, fields_n - 2)], fbuf.at[k, pl.ds(2, fields_n - 2)], in_sem.at[6 + slots + k]
            )
            for k in range(slots)
        ]
        small = [
            pltpu.make_async_copy(thick_in, thick, in_sem.at[2 + slots]),
            pltpu.make_async_copy(mixing_in, mixing, in_sem.at[3 + slots]),
            pltpu.make_async_copy(spread_in, spread, in_sem.at[4 + slots]),
            pltpu.make_async_copy(links_in.at[0, 0], links, in_sem.at[5 + slots]),
        ]
        for copy in copies[:3] + small + copies[3:] + later:
            copy.start()

        barrier = pltpu.get_barrier_semaphore()
        base = (t // low) * low
        place_t = t % low
        me_first = place_t * strips + s
        deltas = [(1 << b) * (1 - 2 * ((me_first // (1 << b)) % 2)) for b in range(bits)]

        def peer(j):
            if not paired:
                return lax.rem(me_first + j, first)
            return me_first + sum(deltas[b] for b in range(bits) if j >> b & 1)

        early = t < edge
        peers = 0

        def greet(tx, sx):
            pl.semaphore_signal(barrier, inc=1, device_id=(tx, sx), device_id_type=pl.DeviceIdType.MESH)

        def greet_if(wanted, *targets):
            @pl.when(wanted)
            def _():
                for tx, sx in targets:
                    greet(tx, sx)

        if relay:
            other_s = 1 - s
            greet_if(t >= tiles - edge, (relays[0], s), (relays[0], other_s))
            greet_if(t == tiles - 1, (relays[1], s), (relays[1], other_s))
            greet_if(t == relays[0], (0, s))
            greet_if(t == relays[1], (1, s), (2, s))
            for dt in (-1, -2, -3):
                tx = lax.rem(t + dt + tiles, tiles)
                greet(tx, s)
                greet(tx, other_s)
            greet(t, other_s)
            for dt in (1, 2, 3):
                greet_if(t + dt < tiles, (t + dt, s), (t + dt, other_s))
            greet_if((t < centre - edge) | (t > centre + edge), (centre, 0))
            peers = 4 * edge + 1
            peers = peers + jnp.where(t == relays[0], 2 * edge, jnp.where(t == relays[1], 2, 0))
            peers = jnp.where(early, 2 * (t + edge + 1), peers)
            peers = jnp.where((t == centre) & (s == 0), first - 1, peers)
        for j in () if relay else peer_order:
            other = peer(j)
            pl.semaphore_signal(
                barrier, inc=1, device_id=(base + other // strips, other % strips),
                device_id_type=pl.DeviceIdType.MESH,
            )
            peers += 1
        for j in range(1, high):
            other = lax.rem(t // low + j, high)
            pl.semaphore_signal(
                barrier, inc=1, device_id=(other * low + place_t, s), device_id_type=pl.DeviceIdType.MESH
            )
            peers += 1
        if high > 1:
            for dt, ds in around + [d[:2] for d in directions]:
                pl.semaphore_signal(
                    barrier, inc=1,
                    device_id=(lax.rem(t + dt + tiles, tiles), lax.rem(s + ds + strips, strips)),
                    device_id_type=pl.DeviceIdType.MESH,
                )
                peers += 1

        def exchange(pack, near, send_sem, recv_sem, wanted):
            out = []
            for dt, ds, here, back, lo, hi in directions:
                copy = pltpu.make_async_remote_copy(
                    src_ref=pack.at[pl.ds(lo, hi - lo)],
                    dst_ref=near.at[back, pl.ds(lo, hi - lo)],
                    send_sem=send_sem.at[here],
                    recv_sem=recv_sem.at[back],
                    device_id=(lax.rem(t + dt + tiles, tiles), lax.rem(s + ds + strips, strips)),
                    device_id_type=pl.DeviceIdType.MESH,
                )
                if wanted is None:
                    copy.start()
                out.append(copy)
            if wanted is not None:
                @pl.when(wanted)
                def _():
                    for copy in out:
                        copy.start()
            return out

        lane = lax.broadcasted_iota(jnp.int32, (1, LANES), 1)
        flip_at = jnp.where(lane < width, width - 1 - lane, lane)

        def flip(value):
            rows = value.shape[0]
            if rows < 8:
                value = jnp.concatenate([value, jnp.zeros((8 - rows, LANES), jnp.float32)], 0)
            at = jnp.broadcast_to(flip_at, value.shape)
            return jnp.take_along_axis(value, at, axis=1)[:rows]

        outward = 2 * (t // (tiles // 2)) - 1 if tiles >= 7 and tiles % 2 == 0 else 1

        def to(dt, ds):
            return lax.rem(t + dt + tiles, tiles), lax.rem(s + ds + strips, strips)

        def start(copy, dt):
            if not relay:
                copy.start()
            else:
                pl.when(t + dt >= 0)(copy.start)

        def sent(pair):
            if not relay:
                pair[0].wait_send()
            else:
                pl.when(t + pair[1] >= 0)(pair[0].wait_send)

        def send_rim(dt, ds, lo, count):
            copy = pltpu.make_async_remote_copy(
                src_ref=pack1.at[pl.ds(lo, count)],
                dst_ref=near1.at[place(-dt if tiles >= 3 else dt, tiles) * n_s + place(-ds if strips >= 3 else ds, strips), pl.ds(lo, count)],
                send_sem=send1.at[place(dt, tiles) * n_s + place(ds, strips)],
                recv_sem=recv1.at[place(-dt if tiles >= 3 else dt, tiles) * n_s + place(-ds if strips >= 3 else ds, strips)],
                device_id=to(dt, ds),
                device_id_type=pl.DeviceIdType.MESH,
            )
            start(copy, dt)
            return copy, dt

        def send_corners(dt, ds):
            if tiles >= 7:
                here, back = (dt + 3) * far_s, (3 - dt) * far_s
            else:
                here, back = slot_of(dt, tiles) * far_s, slot_of(-dt, tiles) * far_s
            here, back = here + slot_of(ds, strips), back + slot_of(-ds, strips)
            copy = pltpu.make_async_remote_copy(
                src_ref=cpack,
                dst_ref=cnear.at[back],
                send_sem=sendc.at[here],
                recv_sem=recvc.at[back],
                device_id=to(dt, ds),
                device_id_type=pl.DeviceIdType.MESH,
            )
            start(copy, dt)
            return copy, dt

        def by_relay(index):
            if index == 0:
                pair = (pack1.at[pl.ds(0, 3)], relay_rim)
            else:
                pair = (cpack, relay_c.at[index - 1])
            return pltpu.make_async_remote_copy(
                src_ref=pair[0], dst_ref=pair[1], send_sem=sendm.at[index], recv_sem=recvm.at[index],
                device_id=(relays[0] if index < 2 else relays[1], s), device_id_type=pl.DeviceIdType.MESH,
            )

        def forwards(which):
            out = []
            for ds in range(2):
                def onward(src, dst, sem, tx, n):
                    return pltpu.make_async_remote_copy(
                        src_ref=src, dst_ref=dst, send_sem=sendf.at[n], recv_sem=sem,
                        device_id=(tx, lax.rem(s + ds, 2)), device_id_type=pl.DeviceIdType.MESH,
                    )

                if which == 0:
                    at = 2 * n_s + ds
                    count = 3 if ds else 1
                    out.append(onward(
                        relay_rim.at[pl.ds(0, count)], near1.at[at, pl.ds(0, count)], recv1.at[at],
                        tiles - 1, len(out),
                    ))
                for index, tx, dt in ((1, 2, 2), (1, 3, 3)) if which == 0 else ((2, 2, 3), (2, 1, 2), (3, 1, 3)):
                    at = (3 + dt) * far_s + ds
                    out.append(onward(relay_c.at[index - 1], cnear.at[at], recvc.at[at], tiles - tx, len(out)))
            return out

        def relay_on():
            for which in range(2):
                @pl.when(t == relays[which])
                def _():
                    for index in (0, 1) if which == 0 else (2, 3):
                        by_relay(index).wait_recv()
                    for copy in forwards(which):
                        copy.start()

        def relay_end():
            @pl.when(t == 0)
            def _():
                by_relay(0).wait_send()

            for tx in range(edge):
                @pl.when(t == tx)
                def _():
                    by_relay(tx + 1).wait_send()

            for which in range(2):
                @pl.when(t == relays[which])
                def _():
                    for copy in forwards(which):
                        copy.wait_send()

        def send_all():
            rims, corners = [], []
            if relay:
                @pl.when(t == 0)
                def _():
                    by_relay(0).start()

                for tx in range(edge):
                    @pl.when(t == tx)
                    def _():
                        by_relay(tx + 1).start()

            if tiles < 7 or tiles % 2:
                for dt, ds, here, back, lo, hi in directions:
                    rims.append(send_rim(dt, ds, lo, hi - lo))
                for dt, ds in around:
                    corners.append(send_corners(dt, ds))
                return rims, corners
            for sign in (1, -1):
                way = outward * sign
                right = (way + 1) // 2
                for dt, ds in around:
                    if dt > 0:
                        corners.append(send_corners(way * dt, ds))
                    elif dt == 0 and sign < 0:
                        corners.append(send_corners(dt, ds))
                for ds in sorted(steps_s, key=lambda d: -abs(d)):
                    rims.append(send_rim(way, ds, right if ds else 3 * right, 3 if ds else 1))
                if sign < 0:
                    for dt, ds, here, back, lo, hi in directions:
                        if dt == 0:
                            rims.append(send_rim(dt, ds, lo, hi - lo))
            return rims, corners

        def pick(value, at):
            rows = value.shape[0]
            if rows < 8:
                value = jnp.concatenate([value, jnp.zeros((8 - rows, LANES), jnp.float32)], 0)
            return jnp.take_along_axis(value, jnp.broadcast_to(at, value.shape), axis=1)

        def extract(tile, rows, depth):
            blank = jnp.zeros((rows, LANES), jnp.float32)
            period = 2 * depth
            parts = [blank] * period
            loaded = {}

            def at(n):
                if n not in loaded:
                    loaded[n] = tile(n)
                return loaded[n]

            for i in range(-1, width):
                pe = width * i + width - 1
                shift = (i - pe) % LANES
                reach_lo = pe - depth + 1 if i >= 0 else pe + 1
                reach_hi = pe + depth if i + 1 < width else pe
                for n in range(reach_lo // LANES, reach_hi // LANES + 1):
                    lo, hi = max(reach_lo, n * LANES), min(reach_hi, n * LANES + LANES - 1)
                    begin = (i + lo - pe) % LANES
                    mask = ((lane - begin) & (LANES - 1)) <= hi - lo if hi > lo else lane == begin
                    parts[i % period] = jnp.where(mask, roll(at(n), shift), parts[i % period])
            signed = jnp.where(lane >= LANES - depth, lane - LANES + period * LANES, lane)
            rest = signed - period * ((signed * ((1 << 12) // period + 1)) >> 12)

            def gather(offset, turn_by):
                total = parts[(0 + offset) % period]
                for m in range(1, period):
                    total = jnp.where(rest == m, parts[(m + offset) % period], total)
                total = roll(total, turn_by)
                return jnp.where(lane < width, total, 0.0)

            def line(start):
                a, n = start % LANES, start // LANES
                if a == 0:
                    return jnp.where(lane < width, at(n), 0.0)
                head = roll(at(n), -a)
                if a + width <= LANES:
                    return jnp.where(lane < width, head, 0.0)
                tail = roll(at(n + 1), -a)
                return jnp.where(lane < LANES - a, head, jnp.where(lane < width, tail, 0.0))

            west = [gather(-d - 1, -d) for d in range(depth)]
            east = [gather(d, d) for d in range(depth)]
            south = [line(width * d) for d in range(depth)]
            north = [line(width * (width - 1 - d)) for d in range(depth)]
            return west, east, south, north

        def insert(west, east, south, north, store):
            even = (lane & 1) == 0
            mixed = (jnp.where(even, east, west), jnp.where(even, west, east))
            tiles_of = {}

            def add(n, mask, value):
                tiles_of.setdefault(n, []).append((mask, value))

            for i in range(-1, width):
                pe = width * i + width - 1
                pw = pe + 1
                turned = roll(mixed[i % 2], (pe - i) % LANES)
                if i >= 0 and i + 1 < width and pe // LANES == pw // LANES:
                    mask = (lane == pe % LANES) | (lane == pw % LANES)
                    add(pe // LANES, mask, turned)
                else:
                    if i >= 0:
                        add(pe // LANES, lane == pe % LANES, turned)
                    if i + 1 < width:
                        add(pw // LANES, lane == pw % LANES, turned)
            extra = {}
            for start, rim in ((0, south), (width * (width - 1), north)):
                a, n = start % LANES, start // LANES
                turned = roll(rim, a)
                extra.setdefault(n, []).append(jnp.where(lane >= a, turned, 0.0) if a else turned)
                if a + width > LANES:
                    extra.setdefault(n + 1, []).append(jnp.where(lane < a + width - LANES, turned, 0.0))
            blank = jnp.zeros(west.shape, jnp.float32)
            for n in range(n_tiles):
                total = blank
                for mask, value in tiles_of.get(n, ()):
                    total = jnp.where(mask, value, total)
                for value in extra.get(n, ()):
                    total = total + value
                store(n, total)

        shift_bits = 22
        factor = (1 << shift_bits) // width + 1
        for c in range(chunks):
            index = lax.broadcasted_iota(jnp.int32, (1, CHUNK), 1) + c * CHUNK
            column = index - width * ((index * factor) >> shift_bits)
            nw_ref[:, pl.ds(c * CHUNK, CHUNK)] = jnp.where(column == 0, 0.0, 1.0)
            ne_ref[:, pl.ds(c * CHUNK, CHUNK)] = jnp.where(column == width - 1, 0.0, 1.0)
        tail = wide - LANES
        groups = -(-slots * fields_n // 2)
        m_ref[:, :, :LANES] = jnp.zeros((groups, 2 * levels, LANES), jnp.float32)
        m_ref[:, :, tail + LANES :] = jnp.zeros((groups, 2 * levels, 2 * LANES), jnp.float32)
        if (slots * fields_n) % 2:
            m_ref[groups - 1, levels:, :] = jnp.zeros((levels, padded), jnp.float32)
        uv_ref[:, :LANES] = jnp.zeros((2 * half, LANES), jnp.float32)
        uv_ref[:, tail + LANES :] = jnp.zeros((2 * half, 2 * LANES), jnp.float32)
        for f in range(2):
            for k in range(slots, half):
                uv_ref[f * half + k : f * half + k + 1, :] = jnp.zeros((1, padded), jnp.float32)
        for ref in (s_ref, u_ref):
            ref[:, :LANES] = jnp.zeros((slots, LANES), jnp.float32)
            ref[:, wide + LANES :] = jnp.zeros((slots, LANES), jnp.float32)
        w_ref[:, tail:] = jnp.zeros((slots, LANES), jnp.float32)
        d_ref[:, tail:] = jnp.zeros((slots, LANES), jnp.float32)
        rima_ref[...] = jnp.zeros(rima_ref.shape, jnp.float32)

        def per_level(read):
            level = lax.broadcasted_iota(jnp.int32, (levels, 1), 0)
            value = jnp.zeros((levels, 1), jnp.float32)
            for n in range(levels):
                value = jnp.where(level == n, read(n), value)
            return value

        for copy in small:
            copy.wait()
        thick_col = per_level(lambda n: thick[n])
        mix_col = per_level(lambda n: mixing[n])

        def choose(number, test, yes, no):
            return jnp.where(test(jnp.full(yes.shape, number, jnp.int32)), yes, no)

        sub = lax.broadcasted_iota(jnp.int32, (slots, LANES), 0)
        sub8 = lax.broadcasted_iota(jnp.int32, (8, LANES), 0)
        group, lane32 = lane >> 5, lane & 31
        own_k, own_e, own_n = lane32 >> 3, (lane32 >> 1) & 3, lane32 & 1

        def code_rows(e):
            value = jnp.zeros((slots, LANES), jnp.int32)
            for k in range(slots):
                value = jnp.where(sub == k, jnp.full(value.shape, links[k, e, 3], jnp.int32), value)
            return value

        codes = [code_rows(e) for e in range(4)]

        def turn(code):
            a = jnp.where(code == 0, 1.0, jnp.where(code == 2, -1.0, 0.0))
            b = jnp.where(code == 1, 1.0, jnp.where(code == 3, -1.0, 0.0))
            return a, b

        own_links = []
        for n in range(4):
            value = jnp.zeros((1, LANES), jnp.int32)
            for k in range(slots):
                for e in range(4):
                    value = jnp.where((lane32 >> 1) == 4 * k + e, jnp.full(value.shape, links[k, e, n], jnp.int32), value)
            own_links.append(value)

        copies[0].wait()
        copies[1].wait()
        spans = [(c * CHUNK, min(CHUNK, cells - c * CHUNK)) for c in range(chunks)]
        for k in range(slots):
            for at, size in spans:
                w_ref[k : k + 1, pl.ds(at, size)] = wbuf[k, :, pl.ds(at, size)].astype(jnp.float32)
                d_ref[k : k + 1, pl.ds(at, size)] = dbuf[k, :, pl.ds(at, size)] + 4.0

        q_rims = extract(
            lambda n: w_ref[:, pl.ds(LANES * n, LANES)] * d_ref[:, pl.ds(LANES * n, LANES)], slots, 2
        )
        w_rims = [[jnp.where(x > 0.0, 1.0, 0.0) for x in side] for side in q_rims]

        def pre_flip(e, value):
            return jnp.where(codes[e] != 0, flip(value), value)

        for e in range(4):
            value = pre_flip(e, q_rims[e][0])
            for k in range(slots):
                pack1[POS[e], k, 3:4, :] = value[k : k + 1]

        link_f = [x.astype(jnp.float32) for x in own_links]
        nothing = jnp.zeros((1, LANES), jnp.float32)
        ends_at = [jnp.where(own_n == 0, m, width - 1 - m) for m in range(2)]
        ends_w = jnp.where(group == 2, ends_at[1], ends_at[0])

        def mask_fields(k, wanted):
            for f in wanted:
                for at, size in spans:
                    masked = fbuf[k, f, :, pl.ds(at, size)] * w_ref[k : k + 1, pl.ds(at, size)]
                    kf = k * fields_n + f
                    m_ref[kf // 2, pl.ds(levels * (kf % 2), levels), pl.ds(LANES + at, size)] = masked
                    if f < 2:
                        uv_ref[f * half + k : f * half + k + 1, pl.ds(LANES + at, size)] = jnp.sum(
                            masked * thick_col, axis=0, keepdims=True
                        )

        for k in range(slots):
            copies[2 + k].wait()
            mask_fields(k, range(2))
        uv_rims = extract(lambda n: uv_ref[:, pl.ds(LANES * (n + 1), LANES)], 2 * half, 3)
        sent_rims, s_local = [], []
        ends_uv = [jnp.zeros((8, LANES), jnp.float32)] * 2
        ends_s = jnp.zeros((8, LANES), jnp.float32)
        for e in range(4):
            us = [x[0:slots] for x in uv_rims[e]]
            vs = [x[half : half + slots] for x in uv_rims[e]]
            normal, along = (us, vs) if e < 2 else (vs, us)
            sign = 0.5 if e in (0, 2) else -0.5
            w0, w1, q0 = w_rims[e][0], w_rims[e][1], q_rims[e][0]

            def slope(x):
                return 0.5 * (roll(x, -1) - roll(x, 1))

            s0 = w0 * (sign * normal[1] + slope(along[0]))
            s1 = w1 * (sign * (normal[2] - normal[0]) + slope(along[1]))
            u0 = q0 * s0 - w0 * (s1 + (roll(s0, -1) + roll(s0, 1)))
            a, b = turn(codes[e])
            rim = a * us[0] - b * vs[0] if e < 2 else a * vs[0] + b * us[0]
            for r, value in enumerate((rim, s0, u0)):
                value = pre_flip(e, value)
                for k in range(slots):
                    pack1[POS[e], k, r : r + 1, :] = value[k : k + 1]
            sent_rims.append(rim)
            s_local.append(s0)
            mine = own_e == e
            for m in range(2):
                ends_uv[m] = jnp.where(
                    mine & ((sub8 & 3) == own_k) & ((sub8 >> 2) == group), pick(uv_rims[e][0], ends_at[m]), ends_uv[m]
                )
            mine = mine & (sub8 == own_k)
            ends_s = jnp.where(mine & (group == 0), pick(s0, ends_at[0]), ends_s)
            ends_s = jnp.where(mine & ((group == 1) | (group == 2)), pick(w0, ends_w), ends_s)
        ends_uv = [jnp.sum(x, axis=0, keepdims=True) for x in ends_uv]
        cpack[0:1, :] = jnp.where(
            group == 0, link_f[0], jnp.where(group == 1, link_f[1], jnp.where(group == 2, link_f[2], 0.0))
        )
        cpack[1:2, :] = jnp.where(group == 2, link_f[3], ends_uv[0])
        cpack[2:3, :] = jnp.sum(ends_s, axis=0, keepdims=True)
        cpack[3:4, :] = ends_uv[1]
        record = cpack[...]
        for k in range(slots):
            carried = jnp.where(lane >= 96, roll(record, 96 - 32 * k), 0.0)
            for e in range(4):
                pack1[e, k] = pack1[e, k] + carried

        pl.semaphore_wait(barrier, peers)
        sent1, sentc = send_all()
        if relay:
            @pl.when((t == centre) & (s == 0))
            def _():
                for x in range(first):
                    if x != 2 * centre:
                        pl.semaphore_signal(
                            far_sem, inc=1, device_id=(x // 2, x % 2), device_id_type=pl.DeviceIdType.MESH
                        )

        cnear[self_far] = record
        if n_far_even > n_far:
            cnear[n_far] = jnp.zeros((4, LANES), jnp.float32)

        for k in range(slots):
            later[k].wait()
            mask_fields(k, range(2, fields_n))

        def slab_pack(kf, carry):
            rims = extract(lambda n: m_ref[kf, :, pl.ds(LANES * (n + 1), LANES)], 2 * levels, 1)
            for e, rim in enumerate(rims):
                packb[POS[e], 2 * kf] = rim[0][:levels]
                packb[POS[e], 2 * kf + 1] = rim[0][levels:]
            return carry

        lax.fori_loop(0, groups, slab_pack, 0)
        sentb = exchange(packb, nearb, sendb, recvb, t >= edge if relay else None)
        if relay:
            relay_on()

        def entry(k, e):
            dt, ds, p, code = (links[k, e, n] for n in range(4))
            source = place(dt, tiles) * n_s + place(ds, strips)
            return source, jnp.maximum(p, 0), p, code

        inner = slice(LANES, LANES + CHUNK)

        def image(x_ref, at):
            span = pl.ds(at, CHUNK)
            win = x_ref[:, pl.ds(at, CHUNK + 2 * LANES)]
            near = ne_ref[:, span] * roll(win, -1)[:, inner] + nw_ref[:, span] * roll(win, 1)[:, inner]
            near = near + (roll(win, -width)[:, inner] + roll(win, width)[:, inner])
            return w_ref[:, span] * (d_ref[:, span] * win[:, inner] - near)

        def whole(value):
            return jnp.sum(jnp.sum(value, axis=1, keepdims=True), axis=0, keepdims=True)

        for c in range(chunks):
            at = c * CHUNK
            span = pl.ds(at, CHUNK)
            u_win = uv_ref[0:slots, pl.ds(at, CHUNK + 2 * LANES)]
            v_win = uv_ref[half : half + slots, pl.ds(at, CHUNK + 2 * LANES)]
            flux = ne_ref[:, span] * roll(u_win, -1)[:, inner] - nw_ref[:, span] * roll(u_win, 1)[:, inner]
            flux = flux + (roll(v_win, -width)[:, inner] - roll(v_win, width)[:, inner])
            s_ref[:, pl.ds(LANES + at, CHUNK)] = w_ref[:, span] * (0.5 * flux)
        blank = jnp.zeros((slots, CHUNK), jnp.float32)
        ss = su = blank
        for c in range(chunks):
            x = s_ref[:, pl.ds(LANES + c * CHUNK, CHUNK)]
            y = image(s_ref, c * CHUNK)
            ss, su = ss + x * x, su + x * y
        ss, su = whole(ss), whole(su)
        ratio = jnp.where(su > 0.0, ss / su, 0.0)

        sub_l = lax.broadcasted_iota(jnp.int32, (2 * levels, 1), 0)
        lower = sub_l >= levels
        first_level = (sub_l == 0) | (sub_l == levels)
        last_level = (sub_l == levels - 1) | (sub_l == 2 * levels - 1)

        def pair_level(read_a, read_b):
            value = jnp.zeros((2 * levels, 1), jnp.float32)
            for n in range(levels):
                value = jnp.where(sub_l == n, read_a(n), value)
                value = jnp.where(sub_l == levels + n, read_b(n), value)
            return value

        mix_pair = pair_level(lambda n: mixing[n], lambda n: mixing[n])

        def slab_inner(g):
            ka, fa = (2 * g) // fields_n, (2 * g) % fields_n
            kb, fb = (2 * g + 1) // fields_n, (2 * g + 1) % fields_n
            alone = 2 * g + 1 >= slots * fields_n
            if alone:
                kb, fb = ka, fa
            spread_col = pair_level(lambda n: spread[fa, n], lambda n: spread[fb, n])
            keep = 1.0 - 4.0 * spread_col - 2.0 * mix_pair
            for at, size in spans:
                span = pl.ds(at, CHUNK)
                win = m_ref[g, :, pl.ds(at, CHUNK + 2 * LANES)]
                mid = win[:, inner]
                flat = ne_ref[:, span] * roll(win, -1)[:, inner] + nw_ref[:, span] * roll(win, 1)[:, inner]
                flat = flat + (roll(win, -width)[:, inner] + roll(win, width)[:, inner])
                above = jnp.where(last_level, mid, roll(mid, -1, 0))
                below = jnp.where(first_level, mid, roll(mid, 1, 0))
                new = keep * mid + spread_col * flat + mix_pair * (above + below)
                if ka == kb:
                    new = w_ref[ka : ka + 1, span] * new
                else:
                    new = jnp.where(lower, w_ref[kb : kb + 1, span], w_ref[ka : ka + 1, span]) * new
                out_f[0, 0, ka, fa, :, pl.ds(at, size)] = new[:levels, :size]
                if not alone:
                    out_f[0, 0, kb, fb, :, pl.ds(at, size)] = new[levels:, :size]

        def slab_rims(k):
            for e in range(4):
                source, slot, p, code = entry(k, e)
                a, b = turn(code)
                got = []
                for f in range(fields_n):
                    rim = nearb[source, POS[e ^ 1], slot * fields_n + f]
                    rim = choose(code, lambda x: x != 0, flip(rim), rim)
                    got.append(choose(p, lambda x: x >= 0, rim, jnp.zeros_like(rim)))
                rims_ref[e, 0] = a * got[0] + b * got[1]
                rims_ref[e, 1] = a * got[1] - b * got[0]
                for f in range(2, fields_n):
                    rims_ref[e, f] = got[f]

            def one(f, carry):
                def store(n, value):
                    ebs_ref[:, pl.ds(n * LANES, LANES)] = value

                insert(rims_ref[0, f], rims_ref[1, f], rims_ref[2, f], rims_ref[3, f], store)
                spread_col = per_level(lambda n: spread[f, n])
                for at, size in spans:
                    wet = w_ref[k : k + 1, pl.ds(at, size)]
                    old = out_f[0, 0, k, f, :, pl.ds(at, size)]
                    out_f[0, 0, k, f, :, pl.ds(at, size)] = old + wet * (spread_col * ebs_ref[:, pl.ds(at, size)])
                return carry

            lax.fori_loop(0, fields_n, one, 0)

        for g in range(2):
            slab_inner(g)
        if relay:
            @pl.when(early)
            def _():
                pl.semaphore_wait(far_sem, 1)
                for copy in sentb:
                    copy.start()

        for copy, _ in sent1:
            copy.wait_recv()
        for e in range(4):
            for k in range(slots):
                source, slot, p, code = entry(k, e)
                got = near1[source, POS[e ^ 1], slot]
                got = choose(p, lambda x: (x >= 0) & (lane < width), got, jnp.zeros_like(got))
                for r in range(4):
                    got_ref[r, e, k : k + 1, :] = got[r : r + 1]
        rho = [(0.5 if e in (1, 3) else -0.5) * got_ref[0, e] for e in range(4)]

        def store_r(n, value):
            ebr_ref[:, pl.ds(n * LANES, LANES)] = value

        insert(rho[0], rho[1], rho[2], rho[3], store_r)
        for c in range(chunks):
            span, shifted = pl.ds(c * CHUNK, CHUNK), pl.ds(LANES + c * CHUNK, CHUNK)
            s_ref[:, shifted] = s_ref[:, shifted] + w_ref[:, span] * ebr_ref[:, span]
        for dt in steps_t:
            for ds in steps_s:
                if dt == 0 and ds == 0:
                    continue
                at_side = 1
                if ds == 0:
                    at_side = 3 if dt == -1 else 0
                elif dt == 0 and strips >= 3:
                    at_side = 1 if ds == 1 else 2
                total = jnp.zeros((4, LANES), jnp.float32)
                for k in range(slots):
                    found = near1[place(dt, tiles) * n_s + place(ds, strips), at_side, k]
                    total = jnp.where(group == k, roll(found, 32 * k - 96), total)
                cnear[slot_of(dt, tiles) * far_s + slot_of(ds, strips)] = total

        for copy, _ in sentc:
            copy.wait_recv()

        def lookup(steps, at, target):
            at = 32 * group + at
            total = jnp.zeros((8, LANES), jnp.float32)
            wanted = target - (sub8 >> 2)
            near = reach(steps)
            for n in range(near[0] - near[0] % 2, near[-1] + 1, 2):
                pair = jnp.concatenate([cnear[n], cnear[n + 1]], 0)
                found = jnp.take_along_axis(pair, jnp.broadcast_to(at, pair.shape), axis=1)
                total = jnp.where(wanted == n, found, total)
            return total + roll(total, 4, 0)

        apart = lane32 + 32 * (sub8 & 3)

        def quantities(found, r):
            value = jnp.take_along_axis(jnp.broadcast_to(found[r : r + 1], (8, LANES)), apart, axis=1)
            return [value[n : n + 1] for n in range(4)]

        def far(dt, ds):
            if tiles >= 7:
                at_t = dt + 3
            else:
                at_t = dt - tiles * jnp.floor(dt * (1.0 / tiles) + 1e-3)
            if strips >= 7:
                at_s = ds + 3
            else:
                at_s = ds - strips * jnp.floor(ds * (1.0 / strips) + 1e-3)
            return at_t * far_s + at_s

        dt1, ds1, p1, c1 = link_f
        one_if = lambda test: jnp.where(test, 1, 0)
        end1 = own_n ^ one_if(c1 != 0.0)
        side_f = jnp.where(own_e < 2, 2, 0) + end1
        end_f = 1 - (own_e & 1)
        lane1 = jnp.maximum(p1, 0.0).astype(jnp.int32) * 8 + side_f * 2 + end_f
        found1 = lookup(1, lane1, far(dt1, ds1).astype(jnp.int32))
        dt2, ds2, p2, _ = quantities(found1, 0)
        u_c, v_c, c2, _ = quantities(found1, 1)
        _, w_c, w_n, _ = quantities(found1, 2)
        side_g = side_f ^ 1
        end2 = end_f ^ one_if(c2 != 0.0)
        side_h = jnp.where(side_g < 2, 2, 0) + end2
        end_h = side_g & 1
        slot2 = jnp.maximum(p2, 0.0).astype(jnp.int32) * 8
        dt12, ds12 = dt1 + dt2, ds1 + ds2
        lane2 = slot2 + side_g * 2 + end2
        lane2h = slot2 + side_h * 2 + end_h
        for_h = ((sub8 & 3) == 0) | (((sub8 & 3) == 1) & (group == 2))
        found2 = lookup(2, jnp.where(for_h, lane2h, lane2), far(dt12, ds12).astype(jnp.int32))
        dt3, ds3, p3, _ = quantities(found2, 0)
        u_g, v_g, c3, _ = quantities(found2, 1)
        s_g, w_g, _, _ = quantities(found2, 2)
        u_g1, v_g1, _, _ = quantities(found2, 3)
        lane3 = jnp.maximum(p3, 0.0).astype(jnp.int32) * 8 + (side_h ^ 1) * 2 + (end_h ^ one_if(c3 != 0.0))
        found3 = lookup(3, lane3, far(dt12 + dt3, ds12 + ds3).astype(jnp.int32))
        u_h, v_h, _, _ = quantities(found3, 1)

        def arriving(a, b, u, v, side):
            value = jnp.where(side < 2, a * u + b * v, a * v - b * u)
            return jnp.where((side & 1) == 0, -0.5, 0.5) * value

        a2, b2 = turn(c2)
        a3, b3 = turn(c3)
        live2 = (p1 >= 0.0) & (p2 >= 0.0)
        first_in = jnp.where(live2, w_c * arriving(a2, b2, u_g, v_g, side_f), 0.0)
        next_in = jnp.where(live2, w_n * arriving(a2, b2, u_g1, v_g1, side_f), 0.0)
        beyond = arriving(a2, -b2, u_c, v_c, side_g)
        beyond = beyond + jnp.where(p3 >= 0.0, arriving(a3, b3, u_h, v_h, side_h), 0.0)
        beyond = jnp.where(live2, s_g + w_g * beyond, 0.0)
        next_in = next_in + beyond
        first_in = jnp.broadcast_to(first_in, (8, LANES))
        next_in = jnp.broadcast_to(next_in, (8, LANES))

        def side_totals(west, east, south, north):
            end = slice(width - 1, width)

            def ends(at_first, at_last):
                return jnp.where(lane == 0, at_first, jnp.where(lane == width - 1, at_last, 0.0))

            return (
                west + ends(south[:, :1], north[:, :1]),
                east + ends(south[:, end], north[:, end]),
                south + ends(west[:, :1], east[:, :1]),
                north + ends(west[:, end], east[:, end]),
            )

        totals = side_totals(*rho)
        at_end = (lane == 0) | (lane == width - 1)
        by_end = (lane == 1) | (lane == width - 2)
        for e in range(4):
            mine = s_local[e] + w_rims[e][0] * totals[e]
            q = got_ref[3, e]
            wet = jnp.where(q > 0.0, 1.0, 0.0)
            delta = wet * ((-0.5 if e in (1, 3) else 0.5) * sent_rims[e])
            at = (sub8 & 3) * 8 + 2 * e + jnp.where(lane >= width // 2, 1, 0)
            at_first = jnp.take_along_axis(first_in, at, axis=1)[:slots]
            at_next = jnp.take_along_axis(next_in, at, axis=1)[:slots]
            delta = delta + jnp.where(at_end, at_first, 0.0)
            there = got_ref[1, e] + delta
            beside = (roll(delta, -1) + roll(delta, 1)) + mine
            beside = beside + jnp.where(at_end, at_next, 0.0)
            image_there = got_ref[2, e] + q * delta - wet * beside
            rima_ref[e, 0:slots, :] = there
            rima_ref[e, half : half + slots, :] = image_there

        def store_a(n, value):
            eba_ref[:, pl.ds(n * LANES, LANES)] = value

        insert(rima_ref[0], rima_ref[1], rima_ref[2], rima_ref[3], store_a)
        for c in range(chunks):
            span = pl.ds(c * CHUNK, CHUNK)
            u_ref[:, pl.ds(LANES + c * CHUNK, CHUNK)] = (
                image(s_ref, c * CHUNK) - w_ref[:, span] * eba_ref[0:slots, span]
            )
        uu = uv = ee = eu = ez = blank
        for c in range(chunks):
            span = pl.ds(c * CHUNK, CHUNK)
            x = s_ref[:, pl.ds(LANES + c * CHUNK, CHUNK)]
            y = u_ref[:, pl.ds(LANES + c * CHUNK, CHUNK)]
            z = image(u_ref, c * CHUNK) - w_ref[:, span] * eba_ref[half : half + slots, span]
            v_ref[:, span] = z
            left = x - ratio * y
            uu, uv = uu + y * y, uv + y * z
            ee, eu, ez = ee + left * left, eu + left * y, ez + left * z
        uu, uv, ee, eu, ez = (whole(x) for x in (uu, uv, ee, eu, ez))
        su = eu + ratio * uu
        ss = ee + ratio * (eu + su)
        ef = eu - ratio * ez
        uf = uu - ratio * uv + ez
        row = jnp.zeros((1, LANES), jnp.float32)
        for n, value in enumerate((ss, su, None, ee, eu, uu, ef, uf, uv)):
            row = jnp.where(lane == n, ratio if value is None else value, row)
        row_ref[...] = row
        red_ref[me_first] = row

        def target(j):
            return j - 1 + jnp.where(me_first <= j - 1, 1, 0)

        def first_copy(j):
            other = target(j)
            return pltpu.make_async_remote_copy(
                src_ref=row_ref,
                dst_ref=red_ref.at[me_first],
                send_sem=sendr.at[j],
                recv_sem=recvr.at[me_first],
                device_id=(base + other // strips, other % strips),
                device_id_type=pl.DeviceIdType.MESH,
            )

        def first_arrival(j):
            other = target(j)
            return pltpu.make_async_remote_copy(
                src_ref=row_ref,
                dst_ref=red_ref.at[other],
                send_sem=sendr.at[j],
                recv_sem=recvr.at[other],
                device_id=(base + other // strips, other % strips),
                device_id_type=pl.DeviceIdType.MESH,
            )

        if relay:
            @pl.when((t >= edge) & ((t != centre) | (s != 0)))
            def _():
                pl.semaphore_wait(far_sem, 1)

        for j in range(1, first):
            first_copy(j).start()
        for g in range(2, -(-slots * fields_n // 2)):
            slab_inner(g)

        for copy in sentb:
            copy.wait_recv()
        for k in range(slots):
            slab_rims(k)
        for j in range(1, first):
            first_arrival(j).wait_recv()

        if high > 1:
            mine = t // low
            copies2 = []
            for j in range(1, high):
                other = lax.rem(mine + j, high)
                copy = pltpu.make_async_remote_copy(
                    src_ref=red_ref,
                    dst_ref=red2_ref.at[mine],
                    send_sem=sendq.at[j],
                    recv_sem=recvq.at[mine],
                    device_id=(other * low + place_t, s),
                    device_id_type=pl.DeviceIdType.MESH,
                )
                copy.start()
                copies2.append(copy)
            red2_ref[mine] = red_ref[...]
            for j in range(1, high):
                other = lax.rem(mine + j, high)
                pltpu.make_async_remote_copy(
                    src_ref=red_ref,
                    dst_ref=red2_ref.at[other],
                    send_sem=sendq.at[j],
                    recv_sem=recvq.at[other],
                    device_id=(other * low + place_t, s),
                    device_id_type=pl.DeviceIdType.MESH,
                ).wait_recv()
            for copy in copies2:
                copy.wait_send()
            rows = [red2_ref[n] for n in range(high)]
        else:
            rows = [red_ref[...]]

        total = sum(jnp.sum(x, axis=0) for x in rows)
        rr0, sas = total[:, 0:1], total[:, 1:2]
        alpha0 = rr0 / sas
        moved = jnp.zeros((1, LANES), jnp.float32)
        lane3 = lax.broadcasted_iota(jnp.int32, (1, 1, LANES), 2)
        for x in rows:
            delta = jnp.broadcast_to(x[:, :, 2:3], x.shape) - alpha0[None]
            weight = jnp.where(
                (lane3 == 3) | (lane3 == 6), 1.0,
                jnp.where(lane3 == 4, 2.0 * delta, jnp.where(lane3 == 7, delta, delta * delta)),
            )
            moved = moved + jnp.sum(x * weight, axis=0)
        rr1 = jnp.sum(jnp.where((lane >= 3) & (lane <= 5), moved, 0.0), axis=1, keepdims=True)
        rar = jnp.sum(jnp.where((lane >= 6) & (lane <= 8), moved, 0.0), axis=1, keepdims=True)
        beta = rr1 / rr0
        alpha1 = rr1 / (rar - beta * rr1 / alpha0)
        for at, size in spans:
            x = s_ref[:, pl.ds(LANES + at, CHUNK)]
            y = u_ref[:, pl.ds(LANES + at, CHUNK)]
            z = v_ref[:, pl.ds(at, CHUNK)]
            r1 = x - alpha0 * y
            direction = r1 + beta * x
            direction_image = (y - alpha0 * z) + beta * y
            answer = alpha0 * x + alpha1 * direction
            left = r1 - alpha1 * direction_image
            for k in range(slots):
                out_x[0, k, :, pl.ds(at, size)] = answer[k : k + 1, :size]
                out_r[0, k, :, pl.ds(at, size)] = left[k : k + 1, :size]

        for pair in sent1 + sentc:
            sent(pair)
        if relay:
            relay_end()
        for copy in sentb:
            copy.wait_send()
        for j in range(1, first):
            first_copy(j).wait_send()

    f32 = jnp.float32
    any_space = pl.BlockSpec(memory_space=pl.ANY)
    hbm = pl.BlockSpec(memory_space=pltpu.HBM)
    vmem = pl.BlockSpec(memory_space=pltpu.VMEM)
    kf = slots * fields_n
    dma = pltpu.SemaphoreType.DMA
    return pl.pallas_call(
        kernel,
        out_shape=(
            pltpu.VMEM((1, 1, slots, fields_n, levels, cells), f32),
            pltpu.VMEM((1, slots, 1, cells), f32),
            pltpu.VMEM((1, slots, 1, cells), f32),
        ),
        in_specs=[hbm] * 7,
        out_specs=(vmem, vmem, vmem),
        scratch_shapes=[
            pltpu.SMEM((slots, 4, 4), jnp.int32),
            pltpu.SMEM((fields_n, levels), f32),
            pltpu.SMEM((levels,), f32),
            pltpu.SMEM((levels,), f32),
            pltpu.VMEM((slots, fields_n, levels, cells), f32),
            pltpu.VMEM((slots, 1, cells), jnp.int32),
            pltpu.VMEM((slots, 1, cells), f32),
            pltpu.VMEM((-(-kf // 2), 2 * levels, padded), f32),
            pltpu.VMEM((slots, wide), f32),
            pltpu.VMEM((slots, wide), f32),
            pltpu.VMEM((1, wide), f32),
            pltpu.VMEM((1, wide), f32),
            pltpu.VMEM((2 * half, padded), f32),
            pltpu.VMEM((slots, padded), f32),
            pltpu.VMEM((slots, padded), f32),
            pltpu.VMEM((slots, wide), f32),
            pltpu.VMEM((2 * half, wide), f32),
            pltpu.VMEM((slots, wide), f32),
            pltpu.VMEM((levels, wide), f32),
            pltpu.VMEM((4, 4, slots, LANES), f32),
            pltpu.VMEM((4, 2 * half, LANES), f32),
            pltpu.VMEM((4, fields_n, levels, LANES), f32),
            pltpu.VMEM((4, slots, 4, LANES), f32),
            pltpu.VMEM((n_dirs, 4, slots, 4, LANES), f32),
            pltpu.VMEM((4, kf + kf % 2, levels, LANES), f32),
            pltpu.VMEM((n_dirs, 4, kf + kf % 2, levels, LANES), f32),
            pltpu.VMEM((4, LANES), f32),
            pltpu.VMEM((n_far_even, 4, LANES), f32),
            pltpu.VMEM((3, slots, 4, LANES), f32),
            pltpu.VMEM((3, 4, LANES), f32),
            pltpu.VMEM((1, LANES), f32),
            pltpu.VMEM((first, 1, LANES), f32),
            pltpu.VMEM((high, first, 1, LANES) if high > 1 else (1, 1, 1, LANES), f32),
            dma((6 + 2 * slots,)),
            dma((n_dirs,)), dma((n_dirs,)), dma((n_dirs,)), dma((n_dirs,)),
            dma((n_far,)), dma((n_far,)), dma((4,)), dma((4,)), dma((8,)), pltpu.SemaphoreType.REGULAR,
            dma((first,)), dma((first,)), dma((high,)), dma((high,)),
        ],
        compiler_params=pltpu.CompilerParams(
            collective_id=0, has_side_effects=True, vmem_limit_bytes=58 << 20
        ),
    )


def put(*arrays):
    def kernel(*refs):
        count = len(arrays)
        sems = refs[-1]
        copies = [pltpu.make_async_copy(refs[n], refs[count + n], sems.at[n]) for n in range(count)]
        for copy in copies:
            copy.start()
        for copy in copies:
            copy.wait()

    return pl.pallas_call(
        kernel,
        out_shape=tuple(jax.ShapeDtypeStruct(x.shape, x.dtype) for x in arrays),
        in_specs=[pl.BlockSpec(memory_space=pl.ANY)] * len(arrays),
        out_specs=tuple(pl.BlockSpec(memory_space=pltpu.HBM) for _ in arrays),
        scratch_shapes=[pltpu.SemaphoreType.DMA((len(arrays),))],
        compiler_params=pltpu.CompilerParams(vmem_limit_bytes=1 << 20),
    )(*arrays)


def solution(mesh):
    tiles, strips = mesh.shape["tiles"], mesh.shape["strip"]

    def on_device(fields, wet_land, links, surface_diagonal, spread, mixing, thickness):
        slots, fields_n, levels, cells = fields.shape[2:]
        call = build(tiles, strips, slots, fields_n, levels, cells)
        wet_land, surface_diagonal = (jnp.swapaxes(x, 1, 2) for x in (wet_land, surface_diagonal))
        new, answer, left = call(fields, wet_land, links, surface_diagonal, spread, mixing, thickness)
        new, answer, left = put(new, answer, left)
        return new, jnp.swapaxes(answer, 1, 2), jnp.swapaxes(left, 1, 2)

    placed = (
        P("tiles", "strip", None, None, None, None),
        P("tiles", "strip", None, None),
        P("tiles", "strip", None, None, None),
        P("tiles", "strip", None, None),
        P(),
        P(),
        P(),
    )
    return jax.shard_map(
        on_device,
        mesh=mesh,
        in_specs=placed,
        out_specs=(
            P("tiles", "strip", None, None, None, None),
            P("tiles", "strip", None, None),
            P("tiles", "strip", None, None),
        ),
        check_vma=False,
    )
```

```python
import math

import jax
import jax.numpy as jnp
from jax import lax
from jax.experimental import pallas as pl
from jax.experimental.pallas import tpu as pltpu
from jax.sharding import PartitionSpec as P

LANES = 128
CHUNK = 1024
POS = (0, 3, 1, 2)
GROUP = 16


def offsets(size):
    return (-1, 0, 1) if size >= 3 else tuple(range(size))


def place(offset, size):
    if size >= 3:
        return offset + 1
    return offset * offset if size == 2 else 0 * offset


def roll(value, shift, axis=1):
    size = value.shape[axis]
    shift = shift % size
    return pltpu.roll(value, shift, axis) if shift else value


def window(size):
    return (-3, 3) if size >= 7 else (0, size - 1)


def slot_of(offset, size):
    return offset + 3 if size >= 7 else offset % size


def build(tiles, strips, slots, fields_n, levels, cells):
    width = math.isqrt(cells)
    n_tiles = -(-cells // CHUNK) * CHUNK // LANES
    wide = n_tiles * LANES
    padded = wide + 2 * LANES
    chunks = wide // CHUNK
    steps_t, steps_s = offsets(tiles), offsets(strips)
    n_s = len(steps_s)
    n_dirs = len(steps_t) * n_s
    low = min(GROUP, tiles)
    high = tiles // low
    first = low * strips
    half = 4
    span_t = window(tiles)
    span_s = window(strips)
    far_t = span_t[1] - span_t[0] + 1
    far_s = span_s[1] - span_s[0] + 1
    n_far = far_t * far_s
    n_far_even = n_far + n_far % 2
    directions = []
    for dt in steps_t:
        for ds in steps_s:
            if dt == 0 and ds == 0:
                continue
            sides = []
            if dt == -1 or (tiles == 2 and dt):
                sides.append(0)
            if ds == -1 or (strips == 2 and ds):
                sides.append(1)
            if ds == 1:
                sides.append(2)
            if dt == 1:
                sides.append(3)
            here = place(dt, tiles) * n_s + place(ds, strips)
            back = place(-dt if tiles >= 3 else dt, tiles) * n_s + place(-ds if strips >= 3 else ds, strips)
            directions.append((dt, ds, here, back, min(sides), max(sides) + 1))
    directions.sort(key=lambda d: -abs(d[0]) - abs(d[1]))
    self_far = slot_of(0, tiles) * far_s + slot_of(0, strips)
    beside_me = {slot_of(d[0], tiles) * far_s + slot_of(d[1], strips) for d in directions}
    around = []
    for dt in range(span_t[0], span_t[1] + 1):
        for ds in range(span_s[0], span_s[1] + 1):
            here = slot_of(dt, tiles) * far_s + slot_of(ds, strips)
            if here != self_far and here not in beside_me:
                around.append((dt, ds))
    around.sort(key=lambda a: -abs(a[0]))
    bits = first.bit_length() - 1
    paired = first == 1 << bits

    def hops(j):
        upper = j >> max(bits - 2, 0) if bits > 2 else j
        return upper + bin(j % (1 << max(bits - 2, 0))).count("1")

    relay = strips == 2 and high == 1 and tiles % 4 == 0 and tiles >= 12
    edge = 3
    relays = (tiles // 2 + 1, tiles // 2 + 3)
    centre = tiles // 2 - 1
    peer_order = sorted(range(1, first), key=lambda j: (-hops(j), -j))

    def reach(steps):
        if tiles < 7:
            return list(range(n_far))
        return [n for n in range(n_far) if abs(n // far_s - 3) <= steps]

    def kernel(
        fields, wet_in, links_in, diag_in, spread_in, mixing_in, thick_in, out_f, s_ref, u_ref, v_ref, out_c,
        links, spread, mixing, thick, fbuf, wbuf, dbuf, m_ref, w_ref, d_ref, nw_ref, ne_ref, uv_ref, eba_ref, ebr_ref, ebs_ref,
        got_ref, rima_ref, rims_ref, pack1, near1, packb, nearb, cpack, cnear, relay_rim, relay_c, row_ref, red_ref, red2_ref,
        in_sem, send1, recv1, sendb, recvb, sendc, recvc, sendm, recvm, sendf, far_sem, sendr, recvr, sendq, recvq,
    ):
        t = lax.axis_index("tiles")
        s = lax.axis_index("strip")
        copies = [
            pltpu.make_async_copy(wet_in.at[0], wbuf, in_sem.at[0]),
            pltpu.make_async_copy(diag_in.at[0], dbuf, in_sem.at[1]),
        ] + [
            pltpu.make_async_copy(fields.at[0, 0, k, pl.ds(0, 2)], fbuf.at[k, pl.ds(0, 2)], in_sem.at[2 + k])
            for k in range(slots)
        ]
        later = [
            pltpu.make_async_copy(
                fields.at[0, 0, k, pl.ds(2, fields_n - 2)], fbuf.at[k, pl.ds(2, fields_n - 2)], in_sem.at[6 + slots + k]
            )
            for k in range(slots)
        ]
        small = [
            pltpu.make_async_copy(thick_in, thick, in_sem.at[2 + slots]),
            pltpu.make_async_copy(mixing_in, mixing, in_sem.at[3 + slots]),
            pltpu.make_async_copy(spread_in, spread, in_sem.at[4 + slots]),
            pltpu.make_async_copy(links_in.at[0, 0], links, in_sem.at[5 + slots]),
        ]
        for copy in copies[:3] + small + copies[3:] + later:
            copy.start()

        barrier = pltpu.get_barrier_semaphore()
        base = (t // low) * low
        place_t = t % low
        me_first = place_t * strips + s
        deltas = [(1 << b) * (1 - 2 * ((me_first // (1 << b)) % 2)) for b in range(bits)]

        def peer(j):
            if not paired:
                return lax.rem(me_first + j, first)
            return me_first + sum(deltas[b] for b in range(bits) if j >> b & 1)

        early = t < edge
        peers = 0

        def greet(tx, sx):
            pl.semaphore_signal(barrier, inc=1, device_id=(tx, sx), device_id_type=pl.DeviceIdType.MESH)

        def greet_if(wanted, *targets):
            @pl.when(wanted)
            def _():
                for tx, sx in targets:
                    greet(tx, sx)

        if relay:
            other_s = 1 - s
            greet_if(t >= tiles - edge, (relays[0], s), (relays[0], other_s))
            greet_if(t == tiles - 1, (relays[1], s), (relays[1], other_s))
            greet_if(t == relays[0], (0, s))
            greet_if(t == relays[1], (1, s), (2, s))
            for dt in (-1, -2, -3):
                tx = lax.rem(t + dt + tiles, tiles)
                greet(tx, s)
                greet(tx, other_s)
            greet(t, other_s)
            for dt in (1, 2, 3):
                greet_if(t + dt < tiles, (t + dt, s), (t + dt, other_s))
            greet_if((t < centre - edge) | (t > centre + edge), (centre, 0))
            peers = 4 * edge + 1
            peers = peers + jnp.where(t == relays[0], 2 * edge, jnp.where(t == relays[1], 2, 0))
            peers = jnp.where(early, 2 * (t + edge + 1), peers)
            peers = jnp.where((t == centre) & (s == 0), first - 1, peers)
        for j in () if relay else peer_order:
            other = peer(j)
            pl.semaphore_signal(
                barrier, inc=1, device_id=(base + other // strips, other % strips),
                device_id_type=pl.DeviceIdType.MESH,
            )
            peers += 1
        for j in range(1, high):
            other = lax.rem(t // low + j, high)
            pl.semaphore_signal(
                barrier, inc=1, device_id=(other * low + place_t, s), device_id_type=pl.DeviceIdType.MESH
            )
            peers += 1
        if high > 1:
            for dt, ds in around + [d[:2] for d in directions]:
                pl.semaphore_signal(
                    barrier, inc=1,
                    device_id=(lax.rem(t + dt + tiles, tiles), lax.rem(s + ds + strips, strips)),
                    device_id_type=pl.DeviceIdType.MESH,
                )
                peers += 1

        def exchange(pack, near, send_sem, recv_sem, wanted):
            out = []
            for dt, ds, here, back, lo, hi in directions:
                copy = pltpu.make_async_remote_copy(
                    src_ref=pack.at[pl.ds(lo, hi - lo)],
                    dst_ref=near.at[back, pl.ds(lo, hi - lo)],
                    send_sem=send_sem.at[here],
                    recv_sem=recv_sem.at[back],
                    device_id=(lax.rem(t + dt + tiles, tiles), lax.rem(s + ds + strips, strips)),
                    device_id_type=pl.DeviceIdType.MESH,
                )
                if wanted is None:
                    copy.start()
                out.append(copy)
            if wanted is not None:
                @pl.when(wanted)
                def _():
                    for copy in out:
                        copy.start()
            return out

        lane = lax.broadcasted_iota(jnp.int32, (1, LANES), 1)
        flip_at = jnp.where(lane < width, width - 1 - lane, lane)

        def flip(value):
            rows = value.shape[0]
            if rows < 8:
                value = jnp.concatenate([value, jnp.zeros((8 - rows, LANES), jnp.float32)], 0)
            at = jnp.broadcast_to(flip_at, value.shape)
            return jnp.take_along_axis(value, at, axis=1)[:rows]

        outward = 2 * (t // (tiles // 2)) - 1 if tiles >= 7 and tiles % 2 == 0 else 1

        def to(dt, ds):
            return lax.rem(t + dt + tiles, tiles), lax.rem(s + ds + strips, strips)

        def start(copy, dt):
            if not relay:
                copy.start()
            else:
                pl.when(t + dt >= 0)(copy.start)

        def sent(pair):
            if not relay:
                pair[0].wait_send()
            else:
                pl.when(t + pair[1] >= 0)(pair[0].wait_send)

        def send_rim(dt, ds, lo, count):
            copy = pltpu.make_async_remote_copy(
                src_ref=pack1.at[pl.ds(lo, count)],
                dst_ref=near1.at[place(-dt if tiles >= 3 else dt, tiles) * n_s + place(-ds if strips >= 3 else ds, strips), pl.ds(lo, count)],
                send_sem=send1.at[place(dt, tiles) * n_s + place(ds, strips)],
                recv_sem=recv1.at[place(-dt if tiles >= 3 else dt, tiles) * n_s + place(-ds if strips >= 3 else ds, strips)],
                device_id=to(dt, ds),
                device_id_type=pl.DeviceIdType.MESH,
            )
            start(copy, dt)
            return copy, dt

        def send_corners(dt, ds):
            if tiles >= 7:
                here, back = (dt + 3) * far_s, (3 - dt) * far_s
            else:
                here, back = slot_of(dt, tiles) * far_s, slot_of(-dt, tiles) * far_s
            here, back = here + slot_of(ds, strips), back + slot_of(-ds, strips)
            copy = pltpu.make_async_remote_copy(
                src_ref=cpack,
                dst_ref=cnear.at[back],
                send_sem=sendc.at[here],
                recv_sem=recvc.at[back],
                device_id=to(dt, ds),
                device_id_type=pl.DeviceIdType.MESH,
            )
            start(copy, dt)
            return copy, dt

        def by_relay(index):
            if index == 0:
                pair = (pack1.at[pl.ds(0, 3)], relay_rim)
            else:
                pair = (cpack, relay_c.at[index - 1])
            return pltpu.make_async_remote_copy(
                src_ref=pair[0], dst_ref=pair[1], send_sem=sendm.at[index], recv_sem=recvm.at[index],
                device_id=(relays[0] if index < 2 else relays[1], s), device_id_type=pl.DeviceIdType.MESH,
            )

        def forwards(which):
            out = []
            for ds in range(2):
                def onward(src, dst, sem, tx, n):
                    return pltpu.make_async_remote_copy(
                        src_ref=src, dst_ref=dst, send_sem=sendf.at[n], recv_sem=sem,
                        device_id=(tx, lax.rem(s + ds, 2)), device_id_type=pl.DeviceIdType.MESH,
                    )

                if which == 0:
                    at = 2 * n_s + ds
                    count = 3 if ds else 1
                    out.append(onward(
                        relay_rim.at[pl.ds(0, count)], near1.at[at, pl.ds(0, count)], recv1.at[at],
                        tiles - 1, len(out),
                    ))
                for index, tx, dt in ((1, 2, 2), (1, 3, 3)) if which == 0 else ((2, 2, 3), (2, 1, 2), (3, 1, 3)):
                    at = (3 + dt) * far_s + ds
                    out.append(onward(relay_c.at[index - 1], cnear.at[at], recvc.at[at], tiles - tx, len(out)))
            return out

        def relay_on():
            for which in range(2):
                @pl.when(t == relays[which])
                def _():
                    for index in (0, 1) if which == 0 else (2, 3):
                        by_relay(index).wait_recv()
                    for copy in forwards(which):
                        copy.start()

        def relay_end():
            @pl.when(t == 0)
            def _():
                by_relay(0).wait_send()

            for tx in range(edge):
                @pl.when(t == tx)
                def _():
                    by_relay(tx + 1).wait_send()

            for which in range(2):
                @pl.when(t == relays[which])
                def _():
                    for copy in forwards(which):
                        copy.wait_send()

        def send_all():
            rims, corners = [], []
            if relay:
                @pl.when(t == 0)
                def _():
                    by_relay(0).start()

                for tx in range(edge):
                    @pl.when(t == tx)
                    def _():
                        by_relay(tx + 1).start()

            if tiles < 7 or tiles % 2:
                for dt, ds, here, back, lo, hi in directions:
                    rims.append(send_rim(dt, ds, lo, hi - lo))
                for dt, ds in around:
                    corners.append(send_corners(dt, ds))
                return rims, corners
            for sign in (1, -1):
                way = outward * sign
                right = (way + 1) // 2
                for dt, ds in around:
                    if dt > 0:
                        corners.append(send_corners(way * dt, ds))
                    elif dt == 0 and sign < 0:
                        corners.append(send_corners(dt, ds))
                for ds in sorted(steps_s, key=lambda d: -abs(d)):
                    rims.append(send_rim(way, ds, right if ds else 3 * right, 3 if ds else 1))
                if sign < 0:
                    for dt, ds, here, back, lo, hi in directions:
                        if dt == 0:
                            rims.append(send_rim(dt, ds, lo, hi - lo))
            return rims, corners

        def pick(value, at):
            rows = value.shape[0]
            if rows < 8:
                value = jnp.concatenate([value, jnp.zeros((8 - rows, LANES), jnp.float32)], 0)
            return jnp.take_along_axis(value, jnp.broadcast_to(at, value.shape), axis=1)

        def extract(tile, rows, depth):
            blank = jnp.zeros((rows, LANES), jnp.float32)
            period = 2 * depth
            parts = [blank] * period
            loaded = {}

            def at(n):
                if n not in loaded:
                    loaded[n] = tile(n)
                return loaded[n]

            for i in range(-1, width):
                pe = width * i + width - 1
                shift = (i - pe) % LANES
                reach_lo = pe - depth + 1 if i >= 0 else pe + 1
                reach_hi = pe + depth if i + 1 < width else pe
                for n in range(reach_lo // LANES, reach_hi // LANES + 1):
                    lo, hi = max(reach_lo, n * LANES), min(reach_hi, n * LANES + LANES - 1)
                    begin = (i + lo - pe) % LANES
                    mask = ((lane - begin) & (LANES - 1)) <= hi - lo if hi > lo else lane == begin
                    parts[i % period] = jnp.where(mask, roll(at(n), shift), parts[i % period])
            signed = jnp.where(lane >= LANES - depth, lane - LANES + period * LANES, lane)
            rest = signed - period * ((signed * ((1 << 12) // period + 1)) >> 12)

            def gather(offset, turn_by):
                total = parts[(0 + offset) % period]
                for m in range(1, period):
                    total = jnp.where(rest == m, parts[(m + offset) % period], total)
                total = roll(total, turn_by)
                return jnp.where(lane < width, total, 0.0)

            def line(start):
                a, n = start % LANES, start // LANES
                if a == 0:
                    return jnp.where(lane < width, at(n), 0.0)
                head = roll(at(n), -a)
                if a + width <= LANES:
                    return jnp.where(lane < width, head, 0.0)
                tail = roll(at(n + 1), -a)
                return jnp.where(lane < LANES - a, head, jnp.where(lane < width, tail, 0.0))

            west = [gather(-d - 1, -d) for d in range(depth)]
            east = [gather(d, d) for d in range(depth)]
            south = [line(width * d) for d in range(depth)]
            north = [line(width * (width - 1 - d)) for d in range(depth)]
            return west, east, south, north

        def insert(west, east, south, north, store):
            even = (lane & 1) == 0
            mixed = (jnp.where(even, east, west), jnp.where(even, west, east))
            tiles_of = {}

            def add(n, mask, value):
                tiles_of.setdefault(n, []).append((mask, value))

            for i in range(-1, width):
                pe = width * i + width - 1
                pw = pe + 1
                turned = roll(mixed[i % 2], (pe - i) % LANES)
                if i >= 0 and i + 1 < width and pe // LANES == pw // LANES:
                    mask = (lane == pe % LANES) | (lane == pw % LANES)
                    add(pe // LANES, mask, turned)
                else:
                    if i >= 0:
                        add(pe // LANES, lane == pe % LANES, turned)
                    if i + 1 < width:
                        add(pw // LANES, lane == pw % LANES, turned)
            extra = {}
            for start, rim in ((0, south), (width * (width - 1), north)):
                a, n = start % LANES, start // LANES
                turned = roll(rim, a)
                extra.setdefault(n, []).append(jnp.where(lane >= a, turned, 0.0) if a else turned)
                if a + width > LANES:
                    extra.setdefault(n + 1, []).append(jnp.where(lane < a + width - LANES, turned, 0.0))
            blank = jnp.zeros(west.shape, jnp.float32)
            for n in range(n_tiles):
                total = blank
                for mask, value in tiles_of.get(n, ()):
                    total = jnp.where(mask, value, total)
                for value in extra.get(n, ()):
                    total = total + value
                store(n, total)

        shift_bits = 22
        factor = (1 << shift_bits) // width + 1
        for c in range(chunks):
            index = lax.broadcasted_iota(jnp.int32, (1, CHUNK), 1) + c * CHUNK
            column = index - width * ((index * factor) >> shift_bits)
            nw_ref[:, pl.ds(c * CHUNK, CHUNK)] = jnp.where(column == 0, 0.0, 1.0)
            ne_ref[:, pl.ds(c * CHUNK, CHUNK)] = jnp.where(column == width - 1, 0.0, 1.0)
        tail = wide - LANES
        groups = -(-slots * fields_n // 2)
        m_ref[:, :, :LANES] = jnp.zeros((groups, 2 * levels, LANES), jnp.float32)
        m_ref[:, :, tail + LANES :] = jnp.zeros((groups, 2 * levels, 2 * LANES), jnp.float32)
        if (slots * fields_n) % 2:
            m_ref[groups - 1, levels:, :] = jnp.zeros((levels, padded), jnp.float32)
        uv_ref[:, :LANES] = jnp.zeros((2 * half, LANES), jnp.float32)
        uv_ref[:, tail + LANES :] = jnp.zeros((2 * half, 2 * LANES), jnp.float32)
        for f in range(2):
            for k in range(slots, half):
                uv_ref[f * half + k : f * half + k + 1, :] = jnp.zeros((1, padded), jnp.float32)
        for ref in (s_ref, u_ref):
            ref[:, :LANES] = jnp.zeros((slots, LANES), jnp.float32)
            ref[:, wide + LANES :] = jnp.zeros((slots, LANES), jnp.float32)
        w_ref[:, tail:] = jnp.zeros((slots, LANES), jnp.float32)
        d_ref[:, tail:] = jnp.zeros((slots, LANES), jnp.float32)
        rima_ref[...] = jnp.zeros(rima_ref.shape, jnp.float32)

        def per_level(read):
            level = lax.broadcasted_iota(jnp.int32, (levels, 1), 0)
            value = jnp.zeros((levels, 1), jnp.float32)
            for n in range(levels):
                value = jnp.where(level == n, read(n), value)
            return value

        for copy in small:
            copy.wait()
        thick_col = per_level(lambda n: thick[n])
        mix_col = per_level(lambda n: mixing[n])

        def choose(number, test, yes, no):
            return jnp.where(test(jnp.full(yes.shape, number, jnp.int32)), yes, no)

        sub = lax.broadcasted_iota(jnp.int32, (slots, LANES), 0)
        sub8 = lax.broadcasted_iota(jnp.int32, (8, LANES), 0)
        group, lane32 = lane >> 5, lane & 31
        own_k, own_e, own_n = lane32 >> 3, (lane32 >> 1) & 3, lane32 & 1

        def code_rows(e):
            value = jnp.zeros((slots, LANES), jnp.int32)
            for k in range(slots):
                value = jnp.where(sub == k, jnp.full(value.shape, links[k, e, 3], jnp.int32), value)
            return value

        codes = [code_rows(e) for e in range(4)]

        def turn(code):
            a = jnp.where(code == 0, 1.0, jnp.where(code == 2, -1.0, 0.0))
            b = jnp.where(code == 1, 1.0, jnp.where(code == 3, -1.0, 0.0))
            return a, b

        own_links = []
        for n in range(4):
            value = jnp.zeros((1, LANES), jnp.int32)
            for k in range(slots):
                for e in range(4):
                    value = jnp.where((lane32 >> 1) == 4 * k + e, jnp.full(value.shape, links[k, e, n], jnp.int32), value)
            own_links.append(value)

        copies[0].wait()
        copies[1].wait()
        spans = [(c * CHUNK, min(CHUNK, cells - c * CHUNK)) for c in range(chunks)]
        for k in range(slots):
            for at, size in spans:
                w_ref[k : k + 1, pl.ds(at, size)] = wbuf[k, :, pl.ds(at, size)].astype(jnp.float32)
                d_ref[k : k + 1, pl.ds(at, size)] = dbuf[k, :, pl.ds(at, size)] + 4.0

        q_rims = extract(
            lambda n: w_ref[:, pl.ds(LANES * n, LANES)] * d_ref[:, pl.ds(LANES * n, LANES)], slots, 2
        )
        w_rims = [[jnp.where(x > 0.0, 1.0, 0.0) for x in side] for side in q_rims]

        def pre_flip(e, value):
            return jnp.where(codes[e] != 0, flip(value), value)

        for e in range(4):
            value = pre_flip(e, q_rims[e][0])
            for k in range(slots):
                pack1[POS[e], k, 3:4, :] = value[k : k + 1]

        link_f = [x.astype(jnp.float32) for x in own_links]
        nothing = jnp.zeros((1, LANES), jnp.float32)
        ends_at = [jnp.where(own_n == 0, m, width - 1 - m) for m in range(2)]
        ends_w = jnp.where(group == 2, ends_at[1], ends_at[0])

        def mask_fields(k, wanted):
            for f in wanted:
                for at, size in spans:
                    masked = fbuf[k, f, :, pl.ds(at, size)] * w_ref[k : k + 1, pl.ds(at, size)]
                    kf = k * fields_n + f
                    m_ref[kf // 2, pl.ds(levels * (kf % 2), levels), pl.ds(LANES + at, size)] = masked
                    if f < 2:
                        uv_ref[f * half + k : f * half + k + 1, pl.ds(LANES + at, size)] = jnp.sum(
                            masked * thick_col, axis=0, keepdims=True
                        )

        for k in range(slots):
            copies[2 + k].wait()
            mask_fields(k, range(2))
        uv_rims = extract(lambda n: uv_ref[:, pl.ds(LANES * (n + 1), LANES)], 2 * half, 3)
        sent_rims, s_local = [], []
        ends_uv = [jnp.zeros((8, LANES), jnp.float32)] * 2
        ends_s = jnp.zeros((8, LANES), jnp.float32)
        for e in range(4):
            us = [x[0:slots] for x in uv_rims[e]]
            vs = [x[half : half + slots] for x in uv_rims[e]]
            normal, along = (us, vs) if e < 2 else (vs, us)
            sign = 0.5 if e in (0, 2) else -0.5
            w0, w1, q0 = w_rims[e][0], w_rims[e][1], q_rims[e][0]

            def slope(x):
                return 0.5 * (roll(x, -1) - roll(x, 1))

            s0 = w0 * (sign * normal[1] + slope(along[0]))
            s1 = w1 * (sign * (normal[2] - normal[0]) + slope(along[1]))
            u0 = q0 * s0 - w0 * (s1 + (roll(s0, -1) + roll(s0, 1)))
            a, b = turn(codes[e])
            rim = a * us[0] - b * vs[0] if e < 2 else a * vs[0] + b * us[0]
            for r, value in enumerate((rim, s0, u0)):
                value = pre_flip(e, value)
                for k in range(slots):
                    pack1[POS[e], k, r : r + 1, :] = value[k : k + 1]
            sent_rims.append(rim)
            s_local.append(s0)
            mine = own_e == e
            for m in range(2):
                ends_uv[m] = jnp.where(
                    mine & ((sub8 & 3) == own_k) & ((sub8 >> 2) == group), pick(uv_rims[e][0], ends_at[m]), ends_uv[m]
                )
            mine = mine & (sub8 == own_k)
            ends_s = jnp.where(mine & (group == 0), pick(s0, ends_at[0]), ends_s)
            ends_s = jnp.where(mine & ((group == 1) | (group == 2)), pick(w0, ends_w), ends_s)
        ends_uv = [jnp.sum(x, axis=0, keepdims=True) for x in ends_uv]
        cpack[0:1, :] = jnp.where(
            group == 0, link_f[0], jnp.where(group == 1, link_f[1], jnp.where(group == 2, link_f[2], 0.0))
        )
        cpack[1:2, :] = jnp.where(group == 2, link_f[3], ends_uv[0])
        cpack[2:3, :] = jnp.sum(ends_s, axis=0, keepdims=True)
        cpack[3:4, :] = ends_uv[1]
        record = cpack[...]
        for k in range(slots):
            carried = jnp.where(lane >= 96, roll(record, 96 - 32 * k), 0.0)
            for e in range(4):
                pack1[e, k] = pack1[e, k] + carried

        pl.semaphore_wait(barrier, peers)
        sent1, sentc = send_all()
        if relay:
            @pl.when((t == centre) & (s == 0))
            def _():
                for x in range(first):
                    if x != 2 * centre:
                        pl.semaphore_signal(
                            far_sem, inc=1, device_id=(x // 2, x % 2), device_id_type=pl.DeviceIdType.MESH
                        )

        cnear[self_far] = record
        if n_far_even > n_far:
            cnear[n_far] = jnp.zeros((4, LANES), jnp.float32)

        for k in range(slots):
            later[k].wait()
            mask_fields(k, range(2, fields_n))

        def slab_pack(kf, carry):
            rims = extract(lambda n: m_ref[kf, :, pl.ds(LANES * (n + 1), LANES)], 2 * levels, 1)
            for e, rim in enumerate(rims):
                packb[POS[e], 2 * kf] = rim[0][:levels]
                packb[POS[e], 2 * kf + 1] = rim[0][levels:]
            return carry

        lax.fori_loop(0, groups, slab_pack, 0)
        sentb = exchange(packb, nearb, sendb, recvb, t >= edge if relay else None)
        if relay:
            relay_on()

        def entry(k, e):
            dt, ds, p, code = (links[k, e, n] for n in range(4))
            source = place(dt, tiles) * n_s + place(ds, strips)
            return source, jnp.maximum(p, 0), p, code

        inner = slice(LANES, LANES + CHUNK)

        def image(x_ref, at):
            span = pl.ds(at, CHUNK)
            win = x_ref[:, pl.ds(at, CHUNK + 2 * LANES)]
            near = ne_ref[:, span] * roll(win, -1)[:, inner] + nw_ref[:, span] * roll(win, 1)[:, inner]
            near = near + (roll(win, -width)[:, inner] + roll(win, width)[:, inner])
            return w_ref[:, span] * (d_ref[:, span] * win[:, inner] - near)

        def whole(value):
            return jnp.sum(jnp.sum(value, axis=1, keepdims=True), axis=0, keepdims=True)

        for c in range(chunks):
            at = c * CHUNK
            span = pl.ds(at, CHUNK)
            u_win = uv_ref[0:slots, pl.ds(at, CHUNK + 2 * LANES)]
            v_win = uv_ref[half : half + slots, pl.ds(at, CHUNK + 2 * LANES)]
            flux = ne_ref[:, span] * roll(u_win, -1)[:, inner] - nw_ref[:, span] * roll(u_win, 1)[:, inner]
            flux = flux + (roll(v_win, -width)[:, inner] - roll(v_win, width)[:, inner])
            s_ref[:, pl.ds(LANES + at, CHUNK)] = w_ref[:, span] * (0.5 * flux)
        blank = jnp.zeros((slots, CHUNK), jnp.float32)
        ss = su = blank
        for c in range(chunks):
            x = s_ref[:, pl.ds(LANES + c * CHUNK, CHUNK)]
            y = image(s_ref, c * CHUNK)
            ss, su = ss + x * x, su + x * y
        ss, su = whole(ss), whole(su)
        ratio = jnp.where(su > 0.0, ss / su, 0.0)

        sub_l = lax.broadcasted_iota(jnp.int32, (2 * levels, 1), 0)
        lower = sub_l >= levels
        first_level = (sub_l == 0) | (sub_l == levels)
        last_level = (sub_l == levels - 1) | (sub_l == 2 * levels - 1)

        def pair_level(read_a, read_b):
            value = jnp.zeros((2 * levels, 1), jnp.float32)
            for n in range(levels):
                value = jnp.where(sub_l == n, read_a(n), value)
                value = jnp.where(sub_l == levels + n, read_b(n), value)
            return value

        mix_pair = pair_level(lambda n: mixing[n], lambda n: mixing[n])

        def slab_inner(g):
            ka, fa = (2 * g) // fields_n, (2 * g) % fields_n
            kb, fb = (2 * g + 1) // fields_n, (2 * g + 1) % fields_n
            alone = 2 * g + 1 >= slots * fields_n
            if alone:
                kb, fb = ka, fa
            spread_col = pair_level(lambda n: spread[fa, n], lambda n: spread[fb, n])
            keep = 1.0 - 4.0 * spread_col - 2.0 * mix_pair
            for at, size in spans:
                span = pl.ds(at, CHUNK)
                win = m_ref[g, :, pl.ds(at, CHUNK + 2 * LANES)]
                mid = win[:, inner]
                flat = ne_ref[:, span] * roll(win, -1)[:, inner] + nw_ref[:, span] * roll(win, 1)[:, inner]
                flat = flat + (roll(win, -width)[:, inner] + roll(win, width)[:, inner])
                above = jnp.where(last_level, mid, roll(mid, -1, 0))
                below = jnp.where(first_level, mid, roll(mid, 1, 0))
                new = keep * mid + spread_col * flat + mix_pair * (above + below)
                if ka == kb:
                    new = w_ref[ka : ka + 1, span] * new
                else:
                    new = jnp.where(lower, w_ref[kb : kb + 1, span], w_ref[ka : ka + 1, span]) * new
                out_f[0, 0, ka, fa, :, pl.ds(at, size)] = new[:levels, :size]
                if not alone:
                    out_f[0, 0, kb, fb, :, pl.ds(at, size)] = new[levels:, :size]

        def slab_rims(k):
            for e in range(4):
                source, slot, p, code = entry(k, e)
                a, b = turn(code)
                got = []
                for f in range(fields_n):
                    rim = nearb[source, POS[e ^ 1], slot * fields_n + f]
                    rim = choose(code, lambda x: x != 0, flip(rim), rim)
                    got.append(choose(p, lambda x: x >= 0, rim, jnp.zeros_like(rim)))
                rims_ref[e, 0] = a * got[0] + b * got[1]
                rims_ref[e, 1] = a * got[1] - b * got[0]
                for f in range(2, fields_n):
                    rims_ref[e, f] = got[f]

            def one(f, carry):
                def store(n, value):
                    ebs_ref[:, pl.ds(n * LANES, LANES)] = value

                insert(rims_ref[0, f], rims_ref[1, f], rims_ref[2, f], rims_ref[3, f], store)
                spread_col = per_level(lambda n: spread[f, n])
                for at, size in spans:
                    wet = w_ref[k : k + 1, pl.ds(at, size)]
                    old = out_f[0, 0, k, f, :, pl.ds(at, size)]
                    out_f[0, 0, k, f, :, pl.ds(at, size)] = old + wet * (spread_col * ebs_ref[:, pl.ds(at, size)])
                return carry

            lax.fori_loop(0, fields_n, one, 0)

        for g in range(2):
            slab_inner(g)
        if relay:
            @pl.when(early)
            def _():
                pl.semaphore_wait(far_sem, 1)
                for copy in sentb:
                    copy.start()

        for copy, _ in sent1:
            copy.wait_recv()
        for e in range(4):
            for k in range(slots):
                source, slot, p, code = entry(k, e)
                got = near1[source, POS[e ^ 1], slot]
                got = choose(p, lambda x: (x >= 0) & (lane < width), got, jnp.zeros_like(got))
                for r in range(4):
                    got_ref[r, e, k : k + 1, :] = got[r : r + 1]
        rho = [(0.5 if e in (1, 3) else -0.5) * got_ref[0, e] for e in range(4)]

        def store_r(n, value):
            ebr_ref[:, pl.ds(n * LANES, LANES)] = value

        insert(rho[0], rho[1], rho[2], rho[3], store_r)
        for c in range(chunks):
            span, shifted = pl.ds(c * CHUNK, CHUNK), pl.ds(LANES + c * CHUNK, CHUNK)
            s_ref[:, shifted] = s_ref[:, shifted] + w_ref[:, span] * ebr_ref[:, span]
        for dt in steps_t:
            for ds in steps_s:
                if dt == 0 and ds == 0:
                    continue
                at_side = 1
                if ds == 0:
                    at_side = 3 if dt == -1 else 0
                elif dt == 0 and strips >= 3:
                    at_side = 1 if ds == 1 else 2
                total = jnp.zeros((4, LANES), jnp.float32)
                for k in range(slots):
                    found = near1[place(dt, tiles) * n_s + place(ds, strips), at_side, k]
                    total = jnp.where(group == k, roll(found, 32 * k - 96), total)
                cnear[slot_of(dt, tiles) * far_s + slot_of(ds, strips)] = total

        for copy, _ in sentc:
            copy.wait_recv()

        def lookup(steps, at, target):
            at = 32 * group + at
            total = jnp.zeros((8, LANES), jnp.float32)
            wanted = target - (sub8 >> 2)
            near = reach(steps)
            for n in range(near[0] - near[0] % 2, near[-1] + 1, 2):
                pair = jnp.concatenate([cnear[n], cnear[n + 1]], 0)
                found = jnp.take_along_axis(pair, jnp.broadcast_to(at, pair.shape), axis=1)
                total = jnp.where(wanted == n, found, total)
            return total + roll(total, 4, 0)

        apart = lane32 + 32 * (sub8 & 3)

        def quantities(found, r):
            value = jnp.take_along_axis(jnp.broadcast_to(found[r : r + 1], (8, LANES)), apart, axis=1)
            return [value[n : n + 1] for n in range(4)]

        def far(dt, ds):
            if tiles >= 7:
                at_t = dt + 3
            else:
                at_t = dt - tiles * jnp.floor(dt * (1.0 / tiles) + 1e-3)
            if strips >= 7:
                at_s = ds + 3
            else:
                at_s = ds - strips * jnp.floor(ds * (1.0 / strips) + 1e-3)
            return at_t * far_s + at_s

        dt1, ds1, p1, c1 = link_f
        one_if = lambda test: jnp.where(test, 1, 0)
        end1 = own_n ^ one_if(c1 != 0.0)
        side_f = jnp.where(own_e < 2, 2, 0) + end1
        end_f = 1 - (own_e & 1)
        lane1 = jnp.maximum(p1, 0.0).astype(jnp.int32) * 8 + side_f * 2 + end_f
        found1 = lookup(1, lane1, far(dt1, ds1).astype(jnp.int32))
        dt2, ds2, p2, _ = quantities(found1, 0)
        u_c, v_c, c2, _ = quantities(found1, 1)
        _, w_c, w_n, _ = quantities(found1, 2)
        side_g = side_f ^ 1
        end2 = end_f ^ one_if(c2 != 0.0)
        side_h = jnp.where(side_g < 2, 2, 0) + end2
        end_h = side_g & 1
        slot2 = jnp.maximum(p2, 0.0).astype(jnp.int32) * 8
        dt12, ds12 = dt1 + dt2, ds1 + ds2
        lane2 = slot2 + side_g * 2 + end2
        lane2h = slot2 + side_h * 2 + end_h
        for_h = ((sub8 & 3) == 0) | (((sub8 & 3) == 1) & (group == 2))
        found2 = lookup(2, jnp.where(for_h, lane2h, lane2), far(dt12, ds12).astype(jnp.int32))
        dt3, ds3, p3, _ = quantities(found2, 0)
        u_g, v_g, c3, _ = quantities(found2, 1)
        s_g, w_g, _, _ = quantities(found2, 2)
        u_g1, v_g1, _, _ = quantities(found2, 3)
        lane3 = jnp.maximum(p3, 0.0).astype(jnp.int32) * 8 + (side_h ^ 1) * 2 + (end_h ^ one_if(c3 != 0.0))
        found3 = lookup(3, lane3, far(dt12 + dt3, ds12 + ds3).astype(jnp.int32))
        u_h, v_h, _, _ = quantities(found3, 1)

        def arriving(a, b, u, v, side):
            value = jnp.where(side < 2, a * u + b * v, a * v - b * u)
            return jnp.where((side & 1) == 0, -0.5, 0.5) * value

        a2, b2 = turn(c2)
        a3, b3 = turn(c3)
        live2 = (p1 >= 0.0) & (p2 >= 0.0)
        first_in = jnp.where(live2, w_c * arriving(a2, b2, u_g, v_g, side_f), 0.0)
        next_in = jnp.where(live2, w_n * arriving(a2, b2, u_g1, v_g1, side_f), 0.0)
        beyond = arriving(a2, -b2, u_c, v_c, side_g)
        beyond = beyond + jnp.where(p3 >= 0.0, arriving(a3, b3, u_h, v_h, side_h), 0.0)
        beyond = jnp.where(live2, s_g + w_g * beyond, 0.0)
        next_in = next_in + beyond
        first_in = jnp.broadcast_to(first_in, (8, LANES))
        next_in = jnp.broadcast_to(next_in, (8, LANES))

        def side_totals(west, east, south, north):
            end = slice(width - 1, width)

            def ends(at_first, at_last):
                return jnp.where(lane == 0, at_first, jnp.where(lane == width - 1, at_last, 0.0))

            return (
                west + ends(south[:, :1], north[:, :1]),
                east + ends(south[:, end], north[:, end]),
                south + ends(west[:, :1], east[:, :1]),
                north + ends(west[:, end], east[:, end]),
            )

        totals = side_totals(*rho)
        at_end = (lane == 0) | (lane == width - 1)
        by_end = (lane == 1) | (lane == width - 2)
        for e in range(4):
            mine = s_local[e] + w_rims[e][0] * totals[e]
            q = got_ref[3, e]
            wet = jnp.where(q > 0.0, 1.0, 0.0)
            delta = wet * ((-0.5 if e in (1, 3) else 0.5) * sent_rims[e])
            at = (sub8 & 3) * 8 + 2 * e + jnp.where(lane >= width // 2, 1, 0)
            at_first = jnp.take_along_axis(first_in, at, axis=1)[:slots]
            at_next = jnp.take_along_axis(next_in, at, axis=1)[:slots]
            delta = delta + jnp.where(at_end, at_first, 0.0)
            there = got_ref[1, e] + delta
            beside = (roll(delta, -1) + roll(delta, 1)) + mine
            beside = beside + jnp.where(at_end, at_next, 0.0)
            image_there = got_ref[2, e] + q * delta - wet * beside
            rima_ref[e, 0:slots, :] = there
            rima_ref[e, half : half + slots, :] = image_there

        def store_a(n, value):
            eba_ref[:, pl.ds(n * LANES, LANES)] = value

        insert(rima_ref[0], rima_ref[1], rima_ref[2], rima_ref[3], store_a)
        for c in range(chunks):
            span = pl.ds(c * CHUNK, CHUNK)
            u_ref[:, pl.ds(LANES + c * CHUNK, CHUNK)] = (
                image(s_ref, c * CHUNK) - w_ref[:, span] * eba_ref[0:slots, span]
            )
        uu = uv = ee = eu = ez = blank
        for c in range(chunks):
            span = pl.ds(c * CHUNK, CHUNK)
            x = s_ref[:, pl.ds(LANES + c * CHUNK, CHUNK)]
            y = u_ref[:, pl.ds(LANES + c * CHUNK, CHUNK)]
            z = image(u_ref, c * CHUNK) - w_ref[:, span] * eba_ref[half : half + slots, span]
            v_ref[:, span] = z
            left = x - ratio * y
            uu, uv = uu + y * y, uv + y * z
            ee, eu, ez = ee + left * left, eu + left * y, ez + left * z
        uu, uv, ee, eu, ez = (whole(x) for x in (uu, uv, ee, eu, ez))
        su = eu + ratio * uu
        ss = ee + ratio * (eu + su)
        ef = eu - ratio * ez
        uf = uu - ratio * uv + ez
        row = jnp.zeros((1, LANES), jnp.float32)
        for n, value in enumerate((ss, su, None, ee, eu, uu, ef, uf, uv)):
            row = jnp.where(lane == n, ratio if value is None else value, row)
        row_ref[...] = row
        red_ref[me_first] = row

        def target(j):
            return j - 1 + jnp.where(me_first <= j - 1, 1, 0)

        def first_copy(j):
            other = target(j)
            return pltpu.make_async_remote_copy(
                src_ref=row_ref,
                dst_ref=red_ref.at[me_first],
                send_sem=sendr.at[j],
                recv_sem=recvr.at[me_first],
                device_id=(base + other // strips, other % strips),
                device_id_type=pl.DeviceIdType.MESH,
            )

        def first_arrival(j):
            other = target(j)
            return pltpu.make_async_remote_copy(
                src_ref=row_ref,
                dst_ref=red_ref.at[other],
                send_sem=sendr.at[j],
                recv_sem=recvr.at[other],
                device_id=(base + other // strips, other % strips),
                device_id_type=pl.DeviceIdType.MESH,
            )

        if relay:
            @pl.when((t >= edge) & ((t != centre) | (s != 0)))
            def _():
                pl.semaphore_wait(far_sem, 1)

        for j in range(1, first):
            first_copy(j).start()
        for g in range(2, -(-slots * fields_n // 2)):
            slab_inner(g)

        for copy in sentb:
            copy.wait_recv()
        for k in range(slots):
            slab_rims(k)
        for j in range(1, first):
            first_arrival(j).wait_recv()

        if high > 1:
            mine = t // low
            copies2 = []
            for j in range(1, high):
                other = lax.rem(mine + j, high)
                copy = pltpu.make_async_remote_copy(
                    src_ref=red_ref,
                    dst_ref=red2_ref.at[mine],
                    send_sem=sendq.at[j],
                    recv_sem=recvq.at[mine],
                    device_id=(other * low + place_t, s),
                    device_id_type=pl.DeviceIdType.MESH,
                )
                copy.start()
                copies2.append(copy)
            red2_ref[mine] = red_ref[...]
            for j in range(1, high):
                other = lax.rem(mine + j, high)
                pltpu.make_async_remote_copy(
                    src_ref=red_ref,
                    dst_ref=red2_ref.at[other],
                    send_sem=sendq.at[j],
                    recv_sem=recvq.at[other],
                    device_id=(other * low + place_t, s),
                    device_id_type=pl.DeviceIdType.MESH,
                ).wait_recv()
            for copy in copies2:
                copy.wait_send()
            rows = [red2_ref[n] for n in range(high)]
        else:
            rows = [red_ref[...]]

        total = sum(jnp.sum(x, axis=0) for x in rows)
        rr0, sas = total[:, 0:1], total[:, 1:2]
        alpha0 = rr0 / sas
        moved = jnp.zeros((1, LANES), jnp.float32)
        lane3 = lax.broadcasted_iota(jnp.int32, (1, 1, LANES), 2)
        for x in rows:
            delta = jnp.broadcast_to(x[:, :, 2:3], x.shape) - alpha0[None]
            weight = jnp.where(
                (lane3 == 3) | (lane3 == 6), 1.0,
                jnp.where(lane3 == 4, 2.0 * delta, jnp.where(lane3 == 7, delta, delta * delta)),
            )
            moved = moved + jnp.sum(x * weight, axis=0)
        rr1 = jnp.sum(jnp.where((lane >= 3) & (lane <= 5), moved, 0.0), axis=1, keepdims=True)
        rar = jnp.sum(jnp.where((lane >= 6) & (lane <= 8), moved, 0.0), axis=1, keepdims=True)
        beta = rr1 / rr0
        alpha1 = rr1 / (rar - beta * rr1 / alpha0)
        out_c[...] = jnp.where(lane == 0, alpha0, jnp.where(lane == 1, alpha1, beta))

        for pair in sent1 + sentc:
            sent(pair)
        if relay:
            relay_end()
        for copy in sentb:
            copy.wait_send()
        for j in range(1, first):
            first_copy(j).wait_send()

    f32 = jnp.float32
    any_space = pl.BlockSpec(memory_space=pl.ANY)
    hbm = pl.BlockSpec(memory_space=pltpu.HBM)
    vmem = pl.BlockSpec(memory_space=pltpu.VMEM)
    kf = slots * fields_n
    dma = pltpu.SemaphoreType.DMA
    return pl.pallas_call(
        kernel,
        out_shape=(
            pltpu.VMEM((1, 1, slots, fields_n, levels, cells), f32),
            pltpu.VMEM((slots, padded), f32),
            pltpu.VMEM((slots, padded), f32),
            pltpu.VMEM((slots, wide), f32),
            pltpu.VMEM((1, LANES), f32),
        ),
        in_specs=[hbm] * 7,
        out_specs=(vmem,) * 5,
        scratch_shapes=[
            pltpu.SMEM((slots, 4, 4), jnp.int32),
            pltpu.SMEM((fields_n, levels), f32),
            pltpu.SMEM((levels,), f32),
            pltpu.SMEM((levels,), f32),
            pltpu.VMEM((slots, fields_n, levels, cells), f32),
            pltpu.VMEM((slots, 1, cells), jnp.int32),
            pltpu.VMEM((slots, 1, cells), f32),
            pltpu.VMEM((-(-kf // 2), 2 * levels, padded), f32),
            pltpu.VMEM((slots, wide), f32),
            pltpu.VMEM((slots, wide), f32),
            pltpu.VMEM((1, wide), f32),
            pltpu.VMEM((1, wide), f32),
            pltpu.VMEM((2 * half, padded), f32),
            pltpu.VMEM((2 * half, wide), f32),
            pltpu.VMEM((slots, wide), f32),
            pltpu.VMEM((levels, wide), f32),
            pltpu.VMEM((4, 4, slots, LANES), f32),
            pltpu.VMEM((4, 2 * half, LANES), f32),
            pltpu.VMEM((4, fields_n, levels, LANES), f32),
            pltpu.VMEM((4, slots, 4, LANES), f32),
            pltpu.VMEM((n_dirs, 4, slots, 4, LANES), f32),
            pltpu.VMEM((4, kf + kf % 2, levels, LANES), f32),
            pltpu.VMEM((n_dirs, 4, kf + kf % 2, levels, LANES), f32),
            pltpu.VMEM((4, LANES), f32),
            pltpu.VMEM((n_far_even, 4, LANES), f32),
            pltpu.VMEM((3, slots, 4, LANES), f32),
            pltpu.VMEM((3, 4, LANES), f32),
            pltpu.VMEM((1, LANES), f32),
            pltpu.VMEM((first, 1, LANES), f32),
            pltpu.VMEM((high, first, 1, LANES) if high > 1 else (1, 1, 1, LANES), f32),
            dma((6 + 2 * slots,)),
            dma((n_dirs,)), dma((n_dirs,)), dma((n_dirs,)), dma((n_dirs,)),
            dma((n_far,)), dma((n_far,)), dma((4,)), dma((4,)), dma((8,)), pltpu.SemaphoreType.REGULAR,
            dma((first,)), dma((first,)), dma((high,)), dma((high,)),
        ],
        compiler_params=pltpu.CompilerParams(
            collective_id=0, has_side_effects=True, vmem_limit_bytes=58 << 20
        ),
    )


def finish(new, s_in, u_in, v_in, scalars, cells):
    slots = s_in.shape[0]
    spans = [(at, min(CHUNK, cells - at)) for at in range(0, cells, CHUNK)]

    def kernel(new_ref, s_ref, u_ref, v_ref, c_ref, out_f, out_x, out_r, x_buf, r_buf, sems):
        whole = pltpu.make_async_copy(new_ref, out_f, sems.at[0])
        whole.start()
        alpha0, alpha1, beta = (c_ref[:, n : n + 1] for n in range(3))
        for at, size in spans:
            x = s_ref[:, pl.ds(LANES + at, CHUNK)]
            y = u_ref[:, pl.ds(LANES + at, CHUNK)]
            z = v_ref[:, pl.ds(at, CHUNK)]
            r1 = x - alpha0 * y
            direction = r1 + beta * x
            direction_image = (y - alpha0 * z) + beta * y
            answer = alpha0 * x + alpha1 * direction
            left = r1 - alpha1 * direction_image
            for k in range(slots):
                x_buf[0, k, :, pl.ds(at, size)] = answer[k : k + 1, :size]
                r_buf[0, k, :, pl.ds(at, size)] = left[k : k + 1, :size]
        copies = [
            pltpu.make_async_copy(x_buf, out_x, sems.at[1]),
            pltpu.make_async_copy(r_buf, out_r, sems.at[2]),
        ]
        for copy in copies:
            copy.start()
        for copy in [whole] + copies:
            copy.wait()

    surface = (1, slots, 1, cells)
    vmem = pl.BlockSpec(memory_space=pltpu.VMEM)
    return pl.pallas_call(
        kernel,
        out_shape=(
            jax.ShapeDtypeStruct(new.shape, new.dtype),
            jax.ShapeDtypeStruct(surface, jnp.float32),
            jax.ShapeDtypeStruct(surface, jnp.float32),
        ),
        in_specs=[pl.BlockSpec(memory_space=pl.ANY)] + [vmem] * 4,
        out_specs=tuple(pl.BlockSpec(memory_space=pltpu.HBM) for _ in range(3)),
        scratch_shapes=[
            pltpu.VMEM(surface, jnp.float32), pltpu.VMEM(surface, jnp.float32), pltpu.SemaphoreType.DMA((3,)),
        ],
        compiler_params=pltpu.CompilerParams(vmem_limit_bytes=2 << 20),
    )(new, s_in, u_in, v_in, scalars)


def solution(mesh):
    tiles, strips = mesh.shape["tiles"], mesh.shape["strip"]

    def on_device(fields, wet_land, links, surface_diagonal, spread, mixing, thickness):
        slots, fields_n, levels, cells = fields.shape[2:]
        call = build(tiles, strips, slots, fields_n, levels, cells)
        wet_land, surface_diagonal = (jnp.swapaxes(x, 1, 2) for x in (wet_land, surface_diagonal))
        parts = call(fields, wet_land, links, surface_diagonal, spread, mixing, thickness)
        new, answer, left = finish(*parts, cells)
        return new, jnp.swapaxes(answer, 1, 2), jnp.swapaxes(left, 1, 2)

    placed = (
        P("tiles", "strip", None, None, None, None),
        P("tiles", "strip", None, None),
        P("tiles", "strip", None, None, None),
        P("tiles", "strip", None, None),
        P(),
        P(),
        P(),
    )
    return jax.shard_map(
        on_device,
        mesh=mesh,
        in_specs=placed,
        out_specs=(
            P("tiles", "strip", None, None, None, None),
            P("tiles", "strip", None, None),
            P("tiles", "strip", None, None),
        ),
        check_vma=False,
    )
```

```python
import math

import jax
import jax.numpy as jnp
from jax import lax
from jax.experimental import pallas as pl
from jax.experimental.pallas import tpu as pltpu
from jax.sharding import PartitionSpec as P

LANES = 128
CHUNK = 1024
POS = (0, 3, 1, 2)
GROUP = 16


def offsets(size):
    return (-1, 0, 1) if size >= 3 else tuple(range(size))


def place(offset, size):
    if size >= 3:
        return offset + 1
    return offset * offset if size == 2 else 0 * offset


def roll(value, shift, axis=1):
    size = value.shape[axis]
    shift = shift % size
    return pltpu.roll(value, shift, axis) if shift else value


def window(size):
    return (-3, 3) if size >= 7 else (0, size - 1)


def slot_of(offset, size):
    return offset + 3 if size >= 7 else offset % size


def build(tiles, strips, slots, fields_n, levels, cells):
    width = math.isqrt(cells)
    n_tiles = -(-cells // CHUNK) * CHUNK // LANES
    wide = n_tiles * LANES
    padded = wide + 2 * LANES
    chunks = wide // CHUNK
    steps_t, steps_s = offsets(tiles), offsets(strips)
    n_s = len(steps_s)
    n_dirs = len(steps_t) * n_s
    low = min(GROUP, tiles)
    high = tiles // low
    first = low * strips
    half = 4
    span_t = window(tiles)
    span_s = window(strips)
    far_t = span_t[1] - span_t[0] + 1
    far_s = span_s[1] - span_s[0] + 1
    n_far = far_t * far_s
    n_far_even = n_far + n_far % 2
    directions = []
    for dt in steps_t:
        for ds in steps_s:
            if dt == 0 and ds == 0:
                continue
            sides = []
            if dt == -1 or (tiles == 2 and dt):
                sides.append(0)
            if ds == -1 or (strips == 2 and ds):
                sides.append(1)
            if ds == 1:
                sides.append(2)
            if dt == 1:
                sides.append(3)
            here = place(dt, tiles) * n_s + place(ds, strips)
            back = place(-dt if tiles >= 3 else dt, tiles) * n_s + place(-ds if strips >= 3 else ds, strips)
            directions.append((dt, ds, here, back, min(sides), max(sides) + 1))
    directions.sort(key=lambda d: -abs(d[0]) - abs(d[1]))
    self_far = slot_of(0, tiles) * far_s + slot_of(0, strips)
    beside_me = {slot_of(d[0], tiles) * far_s + slot_of(d[1], strips) for d in directions}
    around = []
    for dt in range(span_t[0], span_t[1] + 1):
        for ds in range(span_s[0], span_s[1] + 1):
            here = slot_of(dt, tiles) * far_s + slot_of(ds, strips)
            if here != self_far and here not in beside_me:
                around.append((dt, ds))
    around.sort(key=lambda a: -abs(a[0]))
    bits = first.bit_length() - 1
    paired = first == 1 << bits

    def hops(j):
        upper = j >> max(bits - 2, 0) if bits > 2 else j
        return upper + bin(j % (1 << max(bits - 2, 0))).count("1")

    relay = strips == 2 and high == 1 and tiles % 4 == 0 and tiles >= 12
    edge = 3
    relays = (tiles // 2 + 1, tiles // 2 + 3)
    centre = tiles // 2 - 1
    peer_order = sorted(range(1, first), key=lambda j: (-hops(j), -j))

    def reach(steps):
        if tiles < 7:
            return list(range(n_far))
        return [n for n in range(n_far) if abs(n // far_s - 3) <= steps]

    def kernel(
        fields, wet_in, links_in, diag_in, spread_in, mixing_in, thick_in, out_f, s_ref, u_ref, v_ref, out_c,
        links, spread, mixing, thick, fbuf, wbuf, dbuf, m_ref, w_ref, d_ref, nw_ref, ne_ref, uv_ref, eba_ref, ebr_ref, ebs_ref,
        got_ref, rima_ref, rims_ref, pack1, near1, packb, nearb, cpack, cnear, relay_rim, relay_c, row_ref, red_ref, red2_ref,
        in_sem, send1, recv1, sendb, recvb, sendc, recvc, sendm, recvm, sendf, far_sem, sendr, recvr, sendq, recvq,
    ):
        t = lax.axis_index("tiles")
        s = lax.axis_index("strip")
        copies = [
            pltpu.make_async_copy(wet_in.at[0], wbuf, in_sem.at[0]),
            pltpu.make_async_copy(diag_in.at[0], dbuf, in_sem.at[1]),
        ] + [
            pltpu.make_async_copy(fields.at[0, 0, k, pl.ds(0, 2)], fbuf.at[k, pl.ds(0, 2)], in_sem.at[2 + k])
            for k in range(slots)
        ]
        later = [
            pltpu.make_async_copy(
                fields.at[0, 0, k, pl.ds(2, fields_n - 2)], fbuf.at[k, pl.ds(2, fields_n - 2)], in_sem.at[6 + slots + k]
            )
            for k in range(slots)
        ]
        small = [
            pltpu.make_async_copy(thick_in, thick, in_sem.at[2 + slots]),
            pltpu.make_async_copy(mixing_in, mixing, in_sem.at[3 + slots]),
            pltpu.make_async_copy(spread_in, spread, in_sem.at[4 + slots]),
            pltpu.make_async_copy(links_in.at[0, 0], links, in_sem.at[5 + slots]),
        ]
        for copy in copies[:3] + small + copies[3:] + later:
            copy.start()

        barrier = pltpu.get_barrier_semaphore()
        base = (t // low) * low
        place_t = t % low
        me_first = place_t * strips + s
        deltas = [(1 << b) * (1 - 2 * ((me_first // (1 << b)) % 2)) for b in range(bits)]

        def peer(j):
            if not paired:
                return lax.rem(me_first + j, first)
            return me_first + sum(deltas[b] for b in range(bits) if j >> b & 1)

        early = t < edge
        peers = 0

        def greet(tx, sx):
            pl.semaphore_signal(barrier, inc=1, device_id=(tx, sx), device_id_type=pl.DeviceIdType.MESH)

        def greet_if(wanted, *targets):
            @pl.when(wanted)
            def _():
                for tx, sx in targets:
                    greet(tx, sx)

        if relay:
            other_s = 1 - s
            greet_if(t >= tiles - edge, (relays[0], s), (relays[0], other_s))
            greet_if(t == tiles - 1, (relays[1], s), (relays[1], other_s))
            greet_if(t == relays[0], (0, s))
            greet_if(t == relays[1], (1, s), (2, s))
            for dt in (-1, -2, -3):
                tx = lax.rem(t + dt + tiles, tiles)
                greet(tx, s)
                greet(tx, other_s)
            greet(t, other_s)
            for dt in (1, 2, 3):
                greet_if(t + dt < tiles, (t + dt, s), (t + dt, other_s))
            greet_if((t < centre - edge) | (t > centre + edge), (centre, 0))
            peers = 4 * edge + 1
            peers = peers + jnp.where(t == relays[0], 2 * edge, jnp.where(t == relays[1], 2, 0))
            peers = jnp.where(early, 2 * (t + edge + 1), peers)
            peers = jnp.where((t == centre) & (s == 0), first - 1, peers)
        for j in () if relay else peer_order:
            other = peer(j)
            pl.semaphore_signal(
                barrier, inc=1, device_id=(base + other // strips, other % strips),
                device_id_type=pl.DeviceIdType.MESH,
            )
            peers += 1
        for j in range(1, high):
            other = lax.rem(t // low + j, high)
            pl.semaphore_signal(
                barrier, inc=1, device_id=(other * low + place_t, s), device_id_type=pl.DeviceIdType.MESH
            )
            peers += 1
        if high > 1:
            for dt, ds in around + [d[:2] for d in directions]:
                pl.semaphore_signal(
                    barrier, inc=1,
                    device_id=(lax.rem(t + dt + tiles, tiles), lax.rem(s + ds + strips, strips)),
                    device_id_type=pl.DeviceIdType.MESH,
                )
                peers += 1

        def exchange(pack, near, send_sem, recv_sem, wanted):
            out = []
            for dt, ds, here, back, lo, hi in directions:
                copy = pltpu.make_async_remote_copy(
                    src_ref=pack.at[pl.ds(lo, hi - lo)],
                    dst_ref=near.at[back, pl.ds(lo, hi - lo)],
                    send_sem=send_sem.at[here],
                    recv_sem=recv_sem.at[back],
                    device_id=(lax.rem(t + dt + tiles, tiles), lax.rem(s + ds + strips, strips)),
                    device_id_type=pl.DeviceIdType.MESH,
                )
                if wanted is None:
                    copy.start()
                out.append(copy)
            if wanted is not None:
                @pl.when(wanted)
                def _():
                    for copy in out:
                        copy.start()
            return out

        lane = lax.broadcasted_iota(jnp.int32, (1, LANES), 1)
        flip_at = jnp.where(lane < width, width - 1 - lane, lane)

        def flip(value):
            rows = value.shape[0]
            if rows < 8:
                value = jnp.concatenate([value, jnp.zeros((8 - rows, LANES), jnp.float32)], 0)
            at = jnp.broadcast_to(flip_at, value.shape)
            return jnp.take_along_axis(value, at, axis=1)[:rows]

        outward = 2 * (t // (tiles // 2)) - 1 if tiles >= 7 and tiles % 2 == 0 else 1

        def to(dt, ds):
            return lax.rem(t + dt + tiles, tiles), lax.rem(s + ds + strips, strips)

        def start(copy, dt):
            if not relay:
                copy.start()
            else:
                pl.when(t + dt >= 0)(copy.start)

        def sent(pair):
            if not relay:
                pair[0].wait_send()
            else:
                pl.when(t + pair[1] >= 0)(pair[0].wait_send)

        def send_rim(dt, ds, lo, count):
            copy = pltpu.make_async_remote_copy(
                src_ref=pack1.at[pl.ds(lo, count)],
                dst_ref=near1.at[place(-dt if tiles >= 3 else dt, tiles) * n_s + place(-ds if strips >= 3 else ds, strips), pl.ds(lo, count)],
                send_sem=send1.at[place(dt, tiles) * n_s + place(ds, strips)],
                recv_sem=recv1.at[place(-dt if tiles >= 3 else dt, tiles) * n_s + place(-ds if strips >= 3 else ds, strips)],
                device_id=to(dt, ds),
                device_id_type=pl.DeviceIdType.MESH,
            )
            start(copy, dt)
            return copy, dt

        def send_corners(dt, ds):
            if tiles >= 7:
                here, back = (dt + 3) * far_s, (3 - dt) * far_s
            else:
                here, back = slot_of(dt, tiles) * far_s, slot_of(-dt, tiles) * far_s
            here, back = here + slot_of(ds, strips), back + slot_of(-ds, strips)
            copy = pltpu.make_async_remote_copy(
                src_ref=cpack,
                dst_ref=cnear.at[back],
                send_sem=sendc.at[here],
                recv_sem=recvc.at[back],
                device_id=to(dt, ds),
                device_id_type=pl.DeviceIdType.MESH,
            )
            start(copy, dt)
            return copy, dt

        def by_relay(index):
            if index == 0:
                pair = (pack1.at[pl.ds(0, 3)], relay_rim)
            else:
                pair = (cpack, relay_c.at[index - 1])
            return pltpu.make_async_remote_copy(
                src_ref=pair[0], dst_ref=pair[1], send_sem=sendm.at[index], recv_sem=recvm.at[index],
                device_id=(relays[0] if index < 2 else relays[1], s), device_id_type=pl.DeviceIdType.MESH,
            )

        def forwards(which):
            out = []
            for ds in range(2):
                def onward(src, dst, sem, tx, n):
                    return pltpu.make_async_remote_copy(
                        src_ref=src, dst_ref=dst, send_sem=sendf.at[n], recv_sem=sem,
                        device_id=(tx, lax.rem(s + ds, 2)), device_id_type=pl.DeviceIdType.MESH,
                    )

                if which == 0:
                    at = 2 * n_s + ds
                    count = 3 if ds else 1
                    out.append(onward(
                        relay_rim.at[pl.ds(0, count)], near1.at[at, pl.ds(0, count)], recv1.at[at],
                        tiles - 1, len(out),
                    ))
                for index, tx, dt in ((1, 2, 2), (1, 3, 3)) if which == 0 else ((2, 2, 3), (2, 1, 2), (3, 1, 3)):
                    at = (3 + dt) * far_s + ds
                    out.append(onward(relay_c.at[index - 1], cnear.at[at], recvc.at[at], tiles - tx, len(out)))
            return out

        def relay_on():
            for which in range(2):
                @pl.when(t == relays[which])
                def _():
                    for index in (0, 1) if which == 0 else (2, 3):
                        by_relay(index).wait_recv()
                    for copy in forwards(which):
                        copy.start()

        def relay_end():
            @pl.when(t == 0)
            def _():
                by_relay(0).wait_send()

            for tx in range(edge):
                @pl.when(t == tx)
                def _():
                    by_relay(tx + 1).wait_send()

            for which in range(2):
                @pl.when(t == relays[which])
                def _():
                    for copy in forwards(which):
                        copy.wait_send()

        def send_all():
            rims, corners = [], []
            if relay:
                @pl.when(t == 0)
                def _():
                    by_relay(0).start()

                for tx in range(edge):
                    @pl.when(t == tx)
                    def _():
                        by_relay(tx + 1).start()

            if tiles < 7 or tiles % 2:
                for dt, ds, here, back, lo, hi in directions:
                    rims.append(send_rim(dt, ds, lo, hi - lo))
                for dt, ds in around:
                    corners.append(send_corners(dt, ds))
                return rims, corners
            for sign in (1, -1):
                way = outward * sign
                right = (way + 1) // 2
                for dt, ds in around:
                    if dt > 0:
                        corners.append(send_corners(way * dt, ds))
                    elif dt == 0 and sign < 0:
                        corners.append(send_corners(dt, ds))
                for ds in sorted(steps_s, key=lambda d: -abs(d)):
                    rims.append(send_rim(way, ds, right if ds else 3 * right, 3 if ds else 1))
                if sign < 0:
                    for dt, ds, here, back, lo, hi in directions:
                        if dt == 0:
                            rims.append(send_rim(dt, ds, lo, hi - lo))
            return rims, corners

        def pick(value, at):
            rows = value.shape[0]
            if rows < 8:
                value = jnp.concatenate([value, jnp.zeros((8 - rows, LANES), jnp.float32)], 0)
            return jnp.take_along_axis(value, jnp.broadcast_to(at, value.shape), axis=1)

        def extract(tile, rows, depth):
            blank = jnp.zeros((rows, LANES), jnp.float32)
            period = 2 * depth
            parts = [blank] * period
            loaded = {}

            def at(n):
                if n not in loaded:
                    loaded[n] = tile(n)
                return loaded[n]

            for i in range(-1, width):
                pe = width * i + width - 1
                shift = (i - pe) % LANES
                reach_lo = pe - depth + 1 if i >= 0 else pe + 1
                reach_hi = pe + depth if i + 1 < width else pe
                for n in range(reach_lo // LANES, reach_hi // LANES + 1):
                    lo, hi = max(reach_lo, n * LANES), min(reach_hi, n * LANES + LANES - 1)
                    begin = (i + lo - pe) % LANES
                    mask = ((lane - begin) & (LANES - 1)) <= hi - lo if hi > lo else lane == begin
                    parts[i % period] = jnp.where(mask, roll(at(n), shift), parts[i % period])
            signed = jnp.where(lane >= LANES - depth, lane - LANES + period * LANES, lane)
            rest = signed - period * ((signed * ((1 << 12) // period + 1)) >> 12)

            def gather(offset, turn_by):
                total = parts[(0 + offset) % period]
                for m in range(1, period):
                    total = jnp.where(rest == m, parts[(m + offset) % period], total)
                total = roll(total, turn_by)
                return jnp.where(lane < width, total, 0.0)

            def line(start):
                a, n = start % LANES, start // LANES
                if a == 0:
                    return jnp.where(lane < width, at(n), 0.0)
                head = roll(at(n), -a)
                if a + width <= LANES:
                    return jnp.where(lane < width, head, 0.0)
                tail = roll(at(n + 1), -a)
                return jnp.where(lane < LANES - a, head, jnp.where(lane < width, tail, 0.0))

            west = [gather(-d - 1, -d) for d in range(depth)]
            east = [gather(d, d) for d in range(depth)]
            south = [line(width * d) for d in range(depth)]
            north = [line(width * (width - 1 - d)) for d in range(depth)]
            return west, east, south, north

        def insert(west, east, south, north, store):
            even = (lane & 1) == 0
            mixed = (jnp.where(even, east, west), jnp.where(even, west, east))
            tiles_of = {}

            def add(n, mask, value):
                tiles_of.setdefault(n, []).append((mask, value))

            for i in range(-1, width):
                pe = width * i + width - 1
                pw = pe + 1
                turned = roll(mixed[i % 2], (pe - i) % LANES)
                if i >= 0 and i + 1 < width and pe // LANES == pw // LANES:
                    mask = (lane == pe % LANES) | (lane == pw % LANES)
                    add(pe // LANES, mask, turned)
                else:
                    if i >= 0:
                        add(pe // LANES, lane == pe % LANES, turned)
                    if i + 1 < width:
                        add(pw // LANES, lane == pw % LANES, turned)
            extra = {}
            for start, rim in ((0, south), (width * (width - 1), north)):
                a, n = start % LANES, start // LANES
                turned = roll(rim, a)
                extra.setdefault(n, []).append(jnp.where(lane >= a, turned, 0.0) if a else turned)
                if a + width > LANES:
                    extra.setdefault(n + 1, []).append(jnp.where(lane < a + width - LANES, turned, 0.0))
            blank = jnp.zeros(west.shape, jnp.float32)
            for n in range(n_tiles):
                total = blank
                for mask, value in tiles_of.get(n, ()):
                    total = jnp.where(mask, value, total)
                for value in extra.get(n, ()):
                    total = total + value
                store(n, total)

        shift_bits = 22
        factor = (1 << shift_bits) // width + 1
        for c in range(chunks):
            index = lax.broadcasted_iota(jnp.int32, (1, CHUNK), 1) + c * CHUNK
            column = index - width * ((index * factor) >> shift_bits)
            nw_ref[:, pl.ds(c * CHUNK, CHUNK)] = jnp.where(column == 0, 0.0, 1.0)
            ne_ref[:, pl.ds(c * CHUNK, CHUNK)] = jnp.where(column == width - 1, 0.0, 1.0)
        tail = wide - LANES
        groups = -(-slots * fields_n // 2)
        m_ref[:, :, :LANES] = jnp.zeros((groups, 2 * levels, LANES), jnp.float32)
        m_ref[:, :, tail + LANES :] = jnp.zeros((groups, 2 * levels, 2 * LANES), jnp.float32)
        if (slots * fields_n) % 2:
            m_ref[groups - 1, levels:, :] = jnp.zeros((levels, padded), jnp.float32)
        uv_ref[:, :LANES] = jnp.zeros((2 * half, LANES), jnp.float32)
        uv_ref[:, tail + LANES :] = jnp.zeros((2 * half, 2 * LANES), jnp.float32)
        for f in range(2):
            for k in range(slots, half):
                uv_ref[f * half + k : f * half + k + 1, :] = jnp.zeros((1, padded), jnp.float32)
        for ref in (s_ref, u_ref):
            ref[:, :LANES] = jnp.zeros((slots, LANES), jnp.float32)
            ref[:, wide + LANES :] = jnp.zeros((slots, LANES), jnp.float32)
        w_ref[:, tail:] = jnp.zeros((slots, LANES), jnp.float32)
        d_ref[:, tail:] = jnp.zeros((slots, LANES), jnp.float32)
        rima_ref[...] = jnp.zeros(rima_ref.shape, jnp.float32)

        def per_level(read):
            level = lax.broadcasted_iota(jnp.int32, (levels, 1), 0)
            value = jnp.zeros((levels, 1), jnp.float32)
            for n in range(levels):
                value = jnp.where(level == n, read(n), value)
            return value

        for copy in small:
            copy.wait()
        thick_col = per_level(lambda n: thick[n])
        mix_col = per_level(lambda n: mixing[n])

        def choose(number, test, yes, no):
            return jnp.where(test(jnp.full(yes.shape, number, jnp.int32)), yes, no)

        sub = lax.broadcasted_iota(jnp.int32, (slots, LANES), 0)
        sub8 = lax.broadcasted_iota(jnp.int32, (8, LANES), 0)
        group, lane32 = lane >> 5, lane & 31
        own_k, own_e, own_n = lane32 >> 3, (lane32 >> 1) & 3, lane32 & 1

        def code_rows(e):
            value = jnp.zeros((slots, LANES), jnp.int32)
            for k in range(slots):
                value = jnp.where(sub == k, jnp.full(value.shape, links[k, e, 3], jnp.int32), value)
            return value

        codes = [code_rows(e) for e in range(4)]

        def turn(code):
            a = jnp.where(code == 0, 1.0, jnp.where(code == 2, -1.0, 0.0))
            b = jnp.where(code == 1, 1.0, jnp.where(code == 3, -1.0, 0.0))
            return a, b

        own_links = []
        for n in range(4):
            value = jnp.zeros((1, LANES), jnp.int32)
            for k in range(slots):
                for e in range(4):
                    value = jnp.where((lane32 >> 1) == 4 * k + e, jnp.full(value.shape, links[k, e, n], jnp.int32), value)
            own_links.append(value)

        copies[0].wait()
        copies[1].wait()
        spans = [(c * CHUNK, min(CHUNK, cells - c * CHUNK)) for c in range(chunks)]
        for k in range(slots):
            for at, size in spans:
                w_ref[k : k + 1, pl.ds(at, size)] = wbuf[k, :, pl.ds(at, size)].astype(jnp.float32)
                d_ref[k : k + 1, pl.ds(at, size)] = dbuf[k, :, pl.ds(at, size)] + 4.0

        q_rims = extract(
            lambda n: w_ref[:, pl.ds(LANES * n, LANES)] * d_ref[:, pl.ds(LANES * n, LANES)], slots, 2
        )
        w_rims = [[jnp.where(x > 0.0, 1.0, 0.0) for x in side] for side in q_rims]

        def pre_flip(e, value):
            return jnp.where(codes[e] != 0, flip(value), value)

        for e in range(4):
            value = pre_flip(e, q_rims[e][0])
            for k in range(slots):
                pack1[POS[e], k, 3:4, :] = value[k : k + 1]

        link_f = [x.astype(jnp.float32) for x in own_links]
        nothing = jnp.zeros((1, LANES), jnp.float32)
        ends_at = [jnp.where(own_n == 0, m, width - 1 - m) for m in range(2)]
        ends_w = jnp.where(group == 2, ends_at[1], ends_at[0])

        def mask_fields(k, wanted):
            for f in wanted:
                for at, size in spans:
                    masked = fbuf[k, f, :, pl.ds(at, size)] * w_ref[k : k + 1, pl.ds(at, size)]
                    kf = k * fields_n + f
                    m_ref[kf // 2, pl.ds(levels * (kf % 2), levels), pl.ds(LANES + at, size)] = masked
                    if f < 2:
                        uv_ref[f * half + k : f * half + k + 1, pl.ds(LANES + at, size)] = jnp.sum(
                            masked * thick_col, axis=0, keepdims=True
                        )

        for k in range(slots):
            copies[2 + k].wait()
            mask_fields(k, range(2))
        uv_rims = extract(lambda n: uv_ref[:, pl.ds(LANES * (n + 1), LANES)], 2 * half, 3)
        sent_rims, s_local = [], []
        ends_uv = [jnp.zeros((8, LANES), jnp.float32)] * 2
        ends_s = jnp.zeros((8, LANES), jnp.float32)
        for e in range(4):
            us = [x[0:slots] for x in uv_rims[e]]
            vs = [x[half : half + slots] for x in uv_rims[e]]
            normal, along = (us, vs) if e < 2 else (vs, us)
            sign = 0.5 if e in (0, 2) else -0.5
            w0, w1, q0 = w_rims[e][0], w_rims[e][1], q_rims[e][0]

            def slope(x):
                return 0.5 * (roll(x, -1) - roll(x, 1))

            s0 = w0 * (sign * normal[1] + slope(along[0]))
            s1 = w1 * (sign * (normal[2] - normal[0]) + slope(along[1]))
            u0 = q0 * s0 - w0 * (s1 + (roll(s0, -1) + roll(s0, 1)))
            a, b = turn(codes[e])
            rim = a * us[0] - b * vs[0] if e < 2 else a * vs[0] + b * us[0]
            for r, value in enumerate((rim, s0, u0)):
                value = pre_flip(e, value)
                for k in range(slots):
                    pack1[POS[e], k, r : r + 1, :] = value[k : k + 1]
            sent_rims.append(rim)
            s_local.append(s0)
            mine = own_e == e
            for m in range(2):
                ends_uv[m] = jnp.where(
                    mine & ((sub8 & 3) == own_k) & ((sub8 >> 2) == group), pick(uv_rims[e][0], ends_at[m]), ends_uv[m]
                )
            mine = mine & (sub8 == own_k)
            ends_s = jnp.where(mine & (group == 0), pick(s0, ends_at[0]), ends_s)
            ends_s = jnp.where(mine & ((group == 1) | (group == 2)), pick(w0, ends_w), ends_s)
        ends_uv = [jnp.sum(x, axis=0, keepdims=True) for x in ends_uv]
        cpack[0:1, :] = jnp.where(
            group == 0, link_f[0], jnp.where(group == 1, link_f[1], jnp.where(group == 2, link_f[2], 0.0))
        )
        cpack[1:2, :] = jnp.where(group == 2, link_f[3], ends_uv[0])
        cpack[2:3, :] = jnp.sum(ends_s, axis=0, keepdims=True)
        cpack[3:4, :] = ends_uv[1]
        record = cpack[...]
        for k in range(slots):
            carried = jnp.where(lane >= 96, roll(record, 96 - 32 * k), 0.0)
            for e in range(4):
                pack1[e, k] = pack1[e, k] + carried

        pl.semaphore_wait(barrier, peers)
        sent1, sentc = send_all()
        if relay:
            @pl.when((t == centre) & (s == 0))
            def _():
                for x in range(first):
                    if x != 2 * centre:
                        pl.semaphore_signal(
                            far_sem, inc=1, device_id=(x // 2, x % 2), device_id_type=pl.DeviceIdType.MESH
                        )

        cnear[self_far] = record
        if n_far_even > n_far:
            cnear[n_far] = jnp.zeros((4, LANES), jnp.float32)

        for k in range(slots):
            later[k].wait()
            mask_fields(k, range(2, fields_n))

        def slab_pack(kf, carry):
            rims = extract(lambda n: m_ref[kf, :, pl.ds(LANES * (n + 1), LANES)], 2 * levels, 1)
            for e, rim in enumerate(rims):
                packb[POS[e], 2 * kf] = rim[0][:levels]
                packb[POS[e], 2 * kf + 1] = rim[0][levels:]
            return carry

        lax.fori_loop(0, groups, slab_pack, 0)
        sentb = exchange(packb, nearb, sendb, recvb, t >= edge if relay else None)
        if relay:
            relay_on()

        def entry(k, e):
            dt, ds, p, code = (links[k, e, n] for n in range(4))
            source = place(dt, tiles) * n_s + place(ds, strips)
            return source, jnp.maximum(p, 0), p, code

        inner = slice(LANES, LANES + CHUNK)

        def image(x_ref, at):
            span = pl.ds(at, CHUNK)
            win = x_ref[:, pl.ds(at, CHUNK + 2 * LANES)]
            near = ne_ref[:, span] * roll(win, -1)[:, inner] + nw_ref[:, span] * roll(win, 1)[:, inner]
            near = near + (roll(win, -width)[:, inner] + roll(win, width)[:, inner])
            return w_ref[:, span] * (d_ref[:, span] * win[:, inner] - near)

        def whole(value):
            return jnp.sum(jnp.sum(value, axis=1, keepdims=True), axis=0, keepdims=True)

        for c in range(chunks):
            at = c * CHUNK
            span = pl.ds(at, CHUNK)
            u_win = uv_ref[0:slots, pl.ds(at, CHUNK + 2 * LANES)]
            v_win = uv_ref[half : half + slots, pl.ds(at, CHUNK + 2 * LANES)]
            flux = ne_ref[:, span] * roll(u_win, -1)[:, inner] - nw_ref[:, span] * roll(u_win, 1)[:, inner]
            flux = flux + (roll(v_win, -width)[:, inner] - roll(v_win, width)[:, inner])
            s_ref[:, pl.ds(LANES + at, CHUNK)] = w_ref[:, span] * (0.5 * flux)
        blank = jnp.zeros((slots, CHUNK), jnp.float32)
        ss = su = blank
        for c in range(chunks):
            x = s_ref[:, pl.ds(LANES + c * CHUNK, CHUNK)]
            y = image(s_ref, c * CHUNK)
            ss, su = ss + x * x, su + x * y
        ss, su = whole(ss), whole(su)
        ratio = jnp.where(su > 0.0, ss / su, 0.0)

        sub_l = lax.broadcasted_iota(jnp.int32, (2 * levels, 1), 0)
        lower = sub_l >= levels
        first_level = (sub_l == 0) | (sub_l == levels)
        last_level = (sub_l == levels - 1) | (sub_l == 2 * levels - 1)

        def pair_level(read_a, read_b):
            value = jnp.zeros((2 * levels, 1), jnp.float32)
            for n in range(levels):
                value = jnp.where(sub_l == n, read_a(n), value)
                value = jnp.where(sub_l == levels + n, read_b(n), value)
            return value

        mix_pair = pair_level(lambda n: mixing[n], lambda n: mixing[n])

        def slab_inner(g):
            ka, fa = (2 * g) // fields_n, (2 * g) % fields_n
            kb, fb = (2 * g + 1) // fields_n, (2 * g + 1) % fields_n
            alone = 2 * g + 1 >= slots * fields_n
            if alone:
                kb, fb = ka, fa
            spread_col = pair_level(lambda n: spread[fa, n], lambda n: spread[fb, n])
            keep = 1.0 - 4.0 * spread_col - 2.0 * mix_pair
            for at, size in spans:
                span = pl.ds(at, CHUNK)
                win = m_ref[g, :, pl.ds(at, CHUNK + 2 * LANES)]
                mid = win[:, inner]
                flat = ne_ref[:, span] * roll(win, -1)[:, inner] + nw_ref[:, span] * roll(win, 1)[:, inner]
                flat = flat + (roll(win, -width)[:, inner] + roll(win, width)[:, inner])
                above = jnp.where(last_level, mid, roll(mid, -1, 0))
                below = jnp.where(first_level, mid, roll(mid, 1, 0))
                new = keep * mid + spread_col * flat + mix_pair * (above + below)
                if ka == kb:
                    new = w_ref[ka : ka + 1, span] * new
                else:
                    new = jnp.where(lower, w_ref[kb : kb + 1, span], w_ref[ka : ka + 1, span]) * new
                out_f[0, 0, ka, fa, :, pl.ds(at, size)] = new[:levels, :size]
                if not alone:
                    out_f[0, 0, kb, fb, :, pl.ds(at, size)] = new[levels:, :size]

        def slab_rims(k):
            for e in range(4):
                source, slot, p, code = entry(k, e)
                a, b = turn(code)
                got = []
                for f in range(fields_n):
                    rim = nearb[source, POS[e ^ 1], slot * fields_n + f]
                    rim = choose(code, lambda x: x != 0, flip(rim), rim)
                    got.append(choose(p, lambda x: x >= 0, rim, jnp.zeros_like(rim)))
                rims_ref[e, 0] = a * got[0] + b * got[1]
                rims_ref[e, 1] = a * got[1] - b * got[0]
                for f in range(2, fields_n):
                    rims_ref[e, f] = got[f]

            def one(f, carry):
                def store(n, value):
                    ebs_ref[:, pl.ds(n * LANES, LANES)] = value

                insert(rims_ref[0, f], rims_ref[1, f], rims_ref[2, f], rims_ref[3, f], store)
                spread_col = per_level(lambda n: spread[f, n])
                for at, size in spans:
                    wet = w_ref[k : k + 1, pl.ds(at, size)]
                    old = out_f[0, 0, k, f, :, pl.ds(at, size)]
                    out_f[0, 0, k, f, :, pl.ds(at, size)] = old + wet * (spread_col * ebs_ref[:, pl.ds(at, size)])
                return carry

            lax.fori_loop(0, fields_n, one, 0)

        for g in range(2):
            slab_inner(g)
        if relay:
            @pl.when(early)
            def _():
                pl.semaphore_wait(far_sem, 1)
                for copy in sentb:
                    copy.start()

        for copy, _ in sent1:
            copy.wait_recv()
        for e in range(4):
            for k in range(slots):
                source, slot, p, code = entry(k, e)
                got = near1[source, POS[e ^ 1], slot]
                got = choose(p, lambda x: (x >= 0) & (lane < width), got, jnp.zeros_like(got))
                for r in range(4):
                    got_ref[r, e, k : k + 1, :] = got[r : r + 1]
        rho = [(0.5 if e in (1, 3) else -0.5) * got_ref[0, e] for e in range(4)]

        def store_r(n, value):
            ebr_ref[:, pl.ds(n * LANES, LANES)] = value

        insert(rho[0], rho[1], rho[2], rho[3], store_r)
        for c in range(chunks):
            span, shifted = pl.ds(c * CHUNK, CHUNK), pl.ds(LANES + c * CHUNK, CHUNK)
            s_ref[:, shifted] = s_ref[:, shifted] + w_ref[:, span] * ebr_ref[:, span]
        for dt in steps_t:
            for ds in steps_s:
                if dt == 0 and ds == 0:
                    continue
                at_side = 1
                if ds == 0:
                    at_side = 3 if dt == -1 else 0
                elif dt == 0 and strips >= 3:
                    at_side = 1 if ds == 1 else 2
                total = jnp.zeros((4, LANES), jnp.float32)
                for k in range(slots):
                    found = near1[place(dt, tiles) * n_s + place(ds, strips), at_side, k]
                    total = jnp.where(group == k, roll(found, 32 * k - 96), total)
                cnear[slot_of(dt, tiles) * far_s + slot_of(ds, strips)] = total

        for copy, _ in sentc:
            copy.wait_recv()

        def lookup(steps, at, target):
            at = 32 * group + at
            total = jnp.zeros((8, LANES), jnp.float32)
            wanted = target - (sub8 >> 2)
            near = reach(steps)
            for n in range(near[0] - near[0] % 2, near[-1] + 1, 2):
                pair = jnp.concatenate([cnear[n], cnear[n + 1]], 0)
                found = jnp.take_along_axis(pair, jnp.broadcast_to(at, pair.shape), axis=1)
                total = jnp.where(wanted == n, found, total)
            return total + roll(total, 4, 0)

        apart = lane32 + 32 * (sub8 & 3)

        def quantities(found, r):
            value = jnp.take_along_axis(jnp.broadcast_to(found[r : r + 1], (8, LANES)), apart, axis=1)
            return [value[n : n + 1] for n in range(4)]

        def far(dt, ds):
            if tiles >= 7:
                at_t = dt + 3
            else:
                at_t = dt - tiles * jnp.floor(dt * (1.0 / tiles) + 1e-3)
            if strips >= 7:
                at_s = ds + 3
            else:
                at_s = ds - strips * jnp.floor(ds * (1.0 / strips) + 1e-3)
            return at_t * far_s + at_s

        dt1, ds1, p1, c1 = link_f
        one_if = lambda test: jnp.where(test, 1, 0)
        end1 = own_n ^ one_if(c1 != 0.0)
        side_f = jnp.where(own_e < 2, 2, 0) + end1
        end_f = 1 - (own_e & 1)
        lane1 = jnp.maximum(p1, 0.0).astype(jnp.int32) * 8 + side_f * 2 + end_f
        found1 = lookup(1, lane1, far(dt1, ds1).astype(jnp.int32))
        dt2, ds2, p2, _ = quantities(found1, 0)
        u_c, v_c, c2, _ = quantities(found1, 1)
        _, w_c, w_n, _ = quantities(found1, 2)
        side_g = side_f ^ 1
        end2 = end_f ^ one_if(c2 != 0.0)
        side_h = jnp.where(side_g < 2, 2, 0) + end2
        end_h = side_g & 1
        slot2 = jnp.maximum(p2, 0.0).astype(jnp.int32) * 8
        dt12, ds12 = dt1 + dt2, ds1 + ds2
        lane2 = slot2 + side_g * 2 + end2
        lane2h = slot2 + side_h * 2 + end_h
        for_h = ((sub8 & 3) == 0) | (((sub8 & 3) == 1) & (group == 2))
        found2 = lookup(2, jnp.where(for_h, lane2h, lane2), far(dt12, ds12).astype(jnp.int32))
        dt3, ds3, p3, _ = quantities(found2, 0)
        u_g, v_g, c3, _ = quantities(found2, 1)
        s_g, w_g, _, _ = quantities(found2, 2)
        u_g1, v_g1, _, _ = quantities(found2, 3)
        lane3 = jnp.maximum(p3, 0.0).astype(jnp.int32) * 8 + (side_h ^ 1) * 2 + (end_h ^ one_if(c3 != 0.0))
        found3 = lookup(3, lane3, far(dt12 + dt3, ds12 + ds3).astype(jnp.int32))
        u_h, v_h, _, _ = quantities(found3, 1)

        def arriving(a, b, u, v, side):
            value = jnp.where(side < 2, a * u + b * v, a * v - b * u)
            return jnp.where((side & 1) == 0, -0.5, 0.5) * value

        a2, b2 = turn(c2)
        a3, b3 = turn(c3)
        live2 = (p1 >= 0.0) & (p2 >= 0.0)
        first_in = jnp.where(live2, w_c * arriving(a2, b2, u_g, v_g, side_f), 0.0)
        next_in = jnp.where(live2, w_n * arriving(a2, b2, u_g1, v_g1, side_f), 0.0)
        beyond = arriving(a2, -b2, u_c, v_c, side_g)
        beyond = beyond + jnp.where(p3 >= 0.0, arriving(a3, b3, u_h, v_h, side_h), 0.0)
        beyond = jnp.where(live2, s_g + w_g * beyond, 0.0)
        next_in = next_in + beyond
        first_in = jnp.broadcast_to(first_in, (8, LANES))
        next_in = jnp.broadcast_to(next_in, (8, LANES))

        def side_totals(west, east, south, north):
            end = slice(width - 1, width)

            def ends(at_first, at_last):
                return jnp.where(lane == 0, at_first, jnp.where(lane == width - 1, at_last, 0.0))

            return (
                west + ends(south[:, :1], north[:, :1]),
                east + ends(south[:, end], north[:, end]),
                south + ends(west[:, :1], east[:, :1]),
                north + ends(west[:, end], east[:, end]),
            )

        totals = side_totals(*rho)
        at_end = (lane == 0) | (lane == width - 1)
        by_end = (lane == 1) | (lane == width - 2)
        for e in range(4):
            mine = s_local[e] + w_rims[e][0] * totals[e]
            q = got_ref[3, e]
            wet = jnp.where(q > 0.0, 1.0, 0.0)
            delta = wet * ((-0.5 if e in (1, 3) else 0.5) * sent_rims[e])
            at = (sub8 & 3) * 8 + 2 * e + jnp.where(lane >= width // 2, 1, 0)
            at_first = jnp.take_along_axis(first_in, at, axis=1)[:slots]
            at_next = jnp.take_along_axis(next_in, at, axis=1)[:slots]
            delta = delta + jnp.where(at_end, at_first, 0.0)
            there = got_ref[1, e] + delta
            beside = (roll(delta, -1) + roll(delta, 1)) + mine
            beside = beside + jnp.where(at_end, at_next, 0.0)
            image_there = got_ref[2, e] + q * delta - wet * beside
            rima_ref[e, 0:slots, :] = there
            rima_ref[e, half : half + slots, :] = image_there

        def store_a(n, value):
            eba_ref[:, pl.ds(n * LANES, LANES)] = value

        insert(rima_ref[0], rima_ref[1], rima_ref[2], rima_ref[3], store_a)
        for c in range(chunks):
            span = pl.ds(c * CHUNK, CHUNK)
            u_ref[:, pl.ds(LANES + c * CHUNK, CHUNK)] = (
                image(s_ref, c * CHUNK) - w_ref[:, span] * eba_ref[0:slots, span]
            )
        uu = uv = ee = eu = ez = blank
        for c in range(chunks):
            span = pl.ds(c * CHUNK, CHUNK)
            x = s_ref[:, pl.ds(LANES + c * CHUNK, CHUNK)]
            y = u_ref[:, pl.ds(LANES + c * CHUNK, CHUNK)]
            z = image(u_ref, c * CHUNK) - w_ref[:, span] * eba_ref[half : half + slots, span]
            v_ref[:, span] = z
            left = x - ratio * y
            uu, uv = uu + y * y, uv + y * z
            ee, eu, ez = ee + left * left, eu + left * y, ez + left * z
        uu, uv, ee, eu, ez = (whole(x) for x in (uu, uv, ee, eu, ez))
        su = eu + ratio * uu
        ss = ee + ratio * (eu + su)
        ef = eu - ratio * ez
        uf = uu - ratio * uv + ez
        row = jnp.zeros((1, LANES), jnp.float32)
        for n, value in enumerate((ss, su, None, ee, eu, uu, ef, uf, uv)):
            row = jnp.where(lane == n, ratio if value is None else value, row)
        row_ref[...] = row
        red_ref[me_first] = row

        def target(j):
            return j - 1 + jnp.where(me_first <= j - 1, 1, 0)

        def first_copy(j):
            other = target(j)
            return pltpu.make_async_remote_copy(
                src_ref=row_ref,
                dst_ref=red_ref.at[me_first],
                send_sem=sendr.at[j],
                recv_sem=recvr.at[me_first],
                device_id=(base + other // strips, other % strips),
                device_id_type=pl.DeviceIdType.MESH,
            )

        def first_arrival(j):
            other = target(j)
            return pltpu.make_async_remote_copy(
                src_ref=row_ref,
                dst_ref=red_ref.at[other],
                send_sem=sendr.at[j],
                recv_sem=recvr.at[other],
                device_id=(base + other // strips, other % strips),
                device_id_type=pl.DeviceIdType.MESH,
            )

        if relay:
            @pl.when((t >= edge) & ((t != centre) | (s != 0)))
            def _():
                pl.semaphore_wait(far_sem, 1)

        for j in range(1, first):
            first_copy(j).start()
        for g in range(2, -(-slots * fields_n // 2)):
            slab_inner(g)

        for copy in sentb:
            copy.wait_recv()
        for k in range(slots):
            slab_rims(k)
        for pair in sent1 + sentc:
            sent(pair)
        if relay:
            relay_end()
        for copy in sentb:
            copy.wait_send()
        for j in range(1, first):
            first_copy(j).wait_send()
        for j in range(1, first):
            first_arrival(j).wait_recv()

        if high > 1:
            mine = t // low
            copies2 = []
            for j in range(1, high):
                other = lax.rem(mine + j, high)
                copy = pltpu.make_async_remote_copy(
                    src_ref=red_ref,
                    dst_ref=red2_ref.at[mine],
                    send_sem=sendq.at[j],
                    recv_sem=recvq.at[mine],
                    device_id=(other * low + place_t, s),
                    device_id_type=pl.DeviceIdType.MESH,
                )
                copy.start()
                copies2.append(copy)
            red2_ref[mine] = red_ref[...]
            for j in range(1, high):
                other = lax.rem(mine + j, high)
                pltpu.make_async_remote_copy(
                    src_ref=red_ref,
                    dst_ref=red2_ref.at[other],
                    send_sem=sendq.at[j],
                    recv_sem=recvq.at[other],
                    device_id=(other * low + place_t, s),
                    device_id_type=pl.DeviceIdType.MESH,
                ).wait_recv()
            for copy in copies2:
                copy.wait_send()
            rows = [red2_ref[n] for n in range(high)]
        else:
            rows = [red_ref[...]]

        total = sum(jnp.sum(x, axis=0) for x in rows)
        rr0, sas = total[:, 0:1], total[:, 1:2]
        alpha0 = rr0 / sas
        moved = jnp.zeros((1, LANES), jnp.float32)
        lane3 = lax.broadcasted_iota(jnp.int32, (1, 1, LANES), 2)
        for x in rows:
            delta = jnp.broadcast_to(x[:, :, 2:3], x.shape) - alpha0[None]
            weight = jnp.where(
                (lane3 == 3) | (lane3 == 6), 1.0,
                jnp.where(lane3 == 4, 2.0 * delta, jnp.where(lane3 == 7, delta, delta * delta)),
            )
            moved = moved + jnp.sum(x * weight, axis=0)
        rr1 = jnp.sum(jnp.where((lane >= 3) & (lane <= 5), moved, 0.0), axis=1, keepdims=True)
        rar = jnp.sum(jnp.where((lane >= 6) & (lane <= 8), moved, 0.0), axis=1, keepdims=True)
        beta = rr1 / rr0
        alpha1 = rr1 / (rar - beta * rr1 / alpha0)
        out_c[...] = jnp.where(lane == 0, alpha0, jnp.where(lane == 1, alpha1, beta))

    f32 = jnp.float32
    any_space = pl.BlockSpec(memory_space=pl.ANY)
    hbm = pl.BlockSpec(memory_space=pltpu.HBM)
    vmem = pl.BlockSpec(memory_space=pltpu.VMEM)
    kf = slots * fields_n
    dma = pltpu.SemaphoreType.DMA
    return pl.pallas_call(
        kernel,
        out_shape=(
            pltpu.VMEM((1, 1, slots, fields_n, levels, cells), f32),
            pltpu.VMEM((slots, padded), f32),
            pltpu.VMEM((slots, padded), f32),
            pltpu.VMEM((slots, wide), f32),
            pltpu.VMEM((1, LANES), f32),
        ),
        in_specs=[hbm] * 7,
        out_specs=(vmem,) * 5,
        scratch_shapes=[
            pltpu.SMEM((slots, 4, 4), jnp.int32),
            pltpu.SMEM((fields_n, levels), f32),
            pltpu.SMEM((levels,), f32),
            pltpu.SMEM((levels,), f32),
            pltpu.VMEM((slots, fields_n, levels, cells), f32),
            pltpu.VMEM((slots, 1, cells), jnp.int32),
            pltpu.VMEM((slots, 1, cells), f32),
            pltpu.VMEM((-(-kf // 2), 2 * levels, padded), f32),
            pltpu.VMEM((slots, wide), f32),
            pltpu.VMEM((slots, wide), f32),
            pltpu.VMEM((1, wide), f32),
            pltpu.VMEM((1, wide), f32),
            pltpu.VMEM((2 * half, padded), f32),
            pltpu.VMEM((2 * half, wide), f32),
            pltpu.VMEM((slots, wide), f32),
            pltpu.VMEM((levels, wide), f32),
            pltpu.VMEM((4, 4, slots, LANES), f32),
            pltpu.VMEM((4, 2 * half, LANES), f32),
            pltpu.VMEM((4, fields_n, levels, LANES), f32),
            pltpu.VMEM((4, slots, 4, LANES), f32),
            pltpu.VMEM((n_dirs, 4, slots, 4, LANES), f32),
            pltpu.VMEM((4, kf + kf % 2, levels, LANES), f32),
            pltpu.VMEM((n_dirs, 4, kf + kf % 2, levels, LANES), f32),
            pltpu.VMEM((4, LANES), f32),
            pltpu.VMEM((n_far_even, 4, LANES), f32),
            pltpu.VMEM((3, slots, 4, LANES), f32),
            pltpu.VMEM((3, 4, LANES), f32),
            pltpu.VMEM((1, LANES), f32),
            pltpu.VMEM((first, 1, LANES), f32),
            pltpu.VMEM((high, first, 1, LANES) if high > 1 else (1, 1, 1, LANES), f32),
            dma((6 + 2 * slots,)),
            dma((n_dirs,)), dma((n_dirs,)), dma((n_dirs,)), dma((n_dirs,)),
            dma((n_far,)), dma((n_far,)), dma((4,)), dma((4,)), dma((8,)), pltpu.SemaphoreType.REGULAR,
            dma((first,)), dma((first,)), dma((high,)), dma((high,)),
        ],
        compiler_params=pltpu.CompilerParams(
            collective_id=0, has_side_effects=True, vmem_limit_bytes=58 << 20
        ),
    )


def finish(new, s_in, u_in, v_in, scalars, cells):
    slots = s_in.shape[0]
    spans = [(at, min(CHUNK, cells - at)) for at in range(0, cells, CHUNK)]

    def kernel(new_ref, s_ref, u_ref, v_ref, c_ref, out_f, out_x, out_r, x_buf, r_buf, sems):
        whole = pltpu.make_async_copy(new_ref, out_f, sems.at[0])
        whole.start()
        alpha0, alpha1, beta = (c_ref[:, n : n + 1] for n in range(3))
        for at, size in spans:
            x = s_ref[:, pl.ds(LANES + at, CHUNK)]
            y = u_ref[:, pl.ds(LANES + at, CHUNK)]
            z = v_ref[:, pl.ds(at, CHUNK)]
            r1 = x - alpha0 * y
            direction = r1 + beta * x
            direction_image = (y - alpha0 * z) + beta * y
            answer = alpha0 * x + alpha1 * direction
            left = r1 - alpha1 * direction_image
            for k in range(slots):
                x_buf[0, k, :, pl.ds(at, size)] = answer[k : k + 1, :size]
                r_buf[0, k, :, pl.ds(at, size)] = left[k : k + 1, :size]
        copies = [
            pltpu.make_async_copy(x_buf, out_x, sems.at[1]),
            pltpu.make_async_copy(r_buf, out_r, sems.at[2]),
        ]
        for copy in copies:
            copy.start()
        for copy in [whole] + copies:
            copy.wait()

    surface = (1, slots, 1, cells)
    vmem = pl.BlockSpec(memory_space=pltpu.VMEM)
    return pl.pallas_call(
        kernel,
        out_shape=(
            jax.ShapeDtypeStruct(new.shape, new.dtype),
            jax.ShapeDtypeStruct(surface, jnp.float32),
            jax.ShapeDtypeStruct(surface, jnp.float32),
        ),
        in_specs=[pl.BlockSpec(memory_space=pl.ANY)] + [vmem] * 4,
        out_specs=tuple(pl.BlockSpec(memory_space=pltpu.HBM) for _ in range(3)),
        scratch_shapes=[
            pltpu.VMEM(surface, jnp.float32), pltpu.VMEM(surface, jnp.float32), pltpu.SemaphoreType.DMA((3,)),
        ],
        compiler_params=pltpu.CompilerParams(vmem_limit_bytes=2 << 20),
    )(new, s_in, u_in, v_in, scalars)


def solution(mesh):
    tiles, strips = mesh.shape["tiles"], mesh.shape["strip"]

    def on_device(fields, wet_land, links, surface_diagonal, spread, mixing, thickness):
        slots, fields_n, levels, cells = fields.shape[2:]
        call = build(tiles, strips, slots, fields_n, levels, cells)
        wet_land, surface_diagonal = (jnp.swapaxes(x, 1, 2) for x in (wet_land, surface_diagonal))
        parts = call(fields, wet_land, links, surface_diagonal, spread, mixing, thickness)
        new, answer, left = finish(*parts, cells)
        return new, jnp.swapaxes(answer, 1, 2), jnp.swapaxes(left, 1, 2)

    placed = (
        P("tiles", "strip", None, None, None, None),
        P("tiles", "strip", None, None),
        P("tiles", "strip", None, None, None),
        P("tiles", "strip", None, None),
        P(),
        P(),
        P(),
    )
    return jax.shard_map(
        on_device,
        mesh=mesh,
        in_specs=placed,
        out_specs=(
            P("tiles", "strip", None, None, None, None),
            P("tiles", "strip", None, None),
            P("tiles", "strip", None, None),
        ),
        check_vma=False,
    )
```
